32 devices in a mesh: tri: 16 (over z, y, x), sub: 2 (over core).
Axes of the slice: x: 2, y: 2, z: 4, core: 2. Of those that a mesh axis runs over, the one named last changes fastest.
Arguments:
- stored_tiles: float32 [16, 36, 512, 512], P('tri', None, 'sub'), may hold values from -190 to 190, as said below
- cell_owner: int32 [16], replicated, may hold values from 0 to 15, as said below
Outputs:
- updated: float32 [16, 36, 512, 512], P('tri', None, 'sub')
The draws below stay inside these ranges and needn't reach their ends.
Inputs may be any that keep to these rules, and one draw needn't show every extreme that they name: `cell_owner`: a permutation of the indices of tri. `stored_tiles`: every tile whose row and column blocks are equal is skew-symmetric, every pivot met is invertible, and slots that hold no tile are zero.
All inputs are finite; a program needn't handle non-finite values.
Results may differ from the reference program's by a relative error of at most 0.00035.
Values may be sent and summed in bfloat16 or wider, within the bound.
No kernel may reach another device: no remote copies, remote signals or barrier semaphores. Data moves between devices by JAX's collectives and lax.ppermute only.
A program may use at most 128 MiB of HBM per device.

```python
import math
import jax
import jax.numpy as jnp
import numpy as np
from jax import lax

NB = 32
BS = 512
STEPS = 1
N_TRI = 16


def layout_drawn(groups, per_group):
    half_group = per_group // 2
    slot_count = per_group * (per_group + 1) // 2
    row_table = np.full((groups * groups, slot_count), -1, np.int32)
    col_table = np.full((groups * groups, slot_count), -1, np.int32)
    for first_group in range(groups):
        for second_group in range(groups):
            cell_index = first_group * groups + second_group
            for inner_row in range(per_group):
                if first_group == second_group:
                    for inner_column in range(inner_row + 1):
                        slot_index = inner_row * (inner_row + 1) // 2 + inner_column
                        row_table[cell_index, slot_index] = first_group * per_group + inner_row
                        col_table[cell_index, slot_index] = first_group * per_group + inner_column
                else:
                    for inner_column in range(half_group):
                        slot_index = inner_row * half_group + inner_column
                        if first_group > second_group:
                            row_table[cell_index, slot_index] = first_group * per_group + inner_row
                            col_table[cell_index, slot_index] = second_group * per_group + inner_column
                        else:
                            row_table[cell_index, slot_index] = second_group * per_group + inner_row
                            col_table[cell_index, slot_index] = first_group * per_group + half_group + inner_column
    return (row_table, col_table)


def cell_draw(key):
    return jax.random.permutation(jax.random.fold_in(key, 11), N_TRI).astype(jnp.int32)


def draw_cell_owner(key, part):
    return cell_draw(key)


def draw_stored_tiles(key, part):
    owners = cell_draw(key)
    cell_of = jnp.zeros((N_TRI,), jnp.int32).at[owners].set(jnp.arange(N_TRI, dtype=jnp.int32))
    groups = math.isqrt(N_TRI)
    per_group = NB // groups
    row_table, col_table = layout_drawn(groups, per_group)
    row_ids = jnp.asarray(row_table)[cell_of]
    col_ids = jnp.asarray(col_table)[cell_of]
    slot_count = row_table.shape[1]
    tile_shape = (N_TRI, slot_count, BS, BS)
    first_key = jax.random.fold_in(key, 1)
    second_key = jax.random.fold_in(key, 2)
    noise_draw = jnp.clip(jax.random.normal(first_key, tile_shape, jnp.float32), -4.0, 4.0)
    skew_part = 1.2 * (noise_draw - jnp.swapaxes(noise_draw, 2, 3)) / math.sqrt(2.0)
    pair_values = 90.0 * jnp.exp(jax.random.uniform(second_key, (N_TRI, slot_count, BS // 2), jnp.float32, 0.0, math.log(2.0)))
    spread_values = jnp.repeat(pair_values, 2, axis=2)
    row_index = jnp.arange(BS)
    partner_index = row_index + 1 - 2 * (row_index % 2)
    sign_of_row = (1 - 2 * (row_index % 2)).astype(jnp.float32)
    pair_mask = row_index[None, :] == partner_index[:, None]
    pair_part = jnp.where(pair_mask, sign_of_row[:, None] * spread_values[..., :, None], 0.0)
    diagonal = (row_ids == col_ids) & (row_ids >= 0)
    empty_slot = row_ids < 0
    drawn_part = jnp.where(empty_slot[..., None, None], 0.0, 0.5 * noise_draw)
    return jnp.where(diagonal[..., None, None], skew_part + pair_part, drawn_part)


def setup_inputs(seed: int = 0) -> dict:
    key_list = jax.random.split(jax.random.key(seed), 3)
    return {
        "stored_tiles": draw_stored_tiles(jax.random.fold_in(key_list[2], 71), 0),
        "cell_owner": draw_cell_owner(jax.random.fold_in(key_list[2], 71), 0),
    }


def layout(groups, per_group):
    half_group = per_group // 2
    slot_count = per_group * (per_group + 1) // 2
    row_table = np.full((groups * groups, slot_count), -1, np.int32)
    col_table = np.full((groups * groups, slot_count), -1, np.int32)
    for first_group in range(groups):
        for second_group in range(groups):
            cell_index = first_group * groups + second_group
            for inner_row in range(per_group):
                if first_group == second_group:
                    for inner_column in range(inner_row + 1):
                        slot_index = inner_row * (inner_row + 1) // 2 + inner_column
                        row_table[cell_index, slot_index] = first_group * per_group + inner_row
                        col_table[cell_index, slot_index] = first_group * per_group + inner_column
                else:
                    for inner_column in range(half_group):
                        slot_index = inner_row * half_group + inner_column
                        if first_group > second_group:
                            row_table[cell_index, slot_index] = first_group * per_group + inner_row
                            col_table[cell_index, slot_index] = second_group * per_group + inner_column
                        else:
                            row_table[cell_index, slot_index] = second_group * per_group + inner_row
                            col_table[cell_index, slot_index] = first_group * per_group + half_group + inner_column
    return (row_table, col_table)

def reference(stored_tiles, cell_owner):
    groups = math.isqrt(N_TRI)
    per_group = NB // groups
    row_table, col_table = layout(groups, per_group)
    locate = {}
    for cell_index in range(row_table.shape[0]):
        for slot_index in range(row_table.shape[1]):
            if row_table[cell_index, slot_index] >= 0:
                locate[int(row_table[cell_index, slot_index]), int(col_table[cell_index, slot_index])] = (cell_index, slot_index)
    highest = lax.Precision.HIGHEST
    by_cell = stored_tiles[cell_owner]
    row_ids = jnp.asarray(row_table)
    col_ids = jnp.asarray(col_table)
    for step_index in range(STEPS):
        source_cells = np.array([locate[member, step_index][0] for member in range(step_index + 1, NB)], np.int32)
        source_slots = np.array([locate[member, step_index][1] for member in range(step_index + 1, NB)], np.int32)
        column_tiles = by_cell[source_cells, source_slots].astype(jnp.bfloat16)
        pivot_cell, pivot_slot = locate[step_index, step_index]
        pivot_block = by_cell[pivot_cell, pivot_slot]
        inverse = jnp.linalg.inv(pivot_block)
        padded = jnp.concatenate([jnp.zeros((step_index + 1, BS, BS), jnp.bfloat16), column_tiles], axis=0)
        scaled = jnp.einsum('nrk,kc->nrc', padded.astype(jnp.float32), inverse, precision=highest).astype(jnp.bfloat16)

        def cell_update(operands):
            cell_tiles, cell_rows, cell_cols = operands
            live_slots = (cell_rows > step_index) & (cell_cols > step_index)
            left_side = scaled[jnp.maximum(cell_rows, 0)].astype(jnp.float32)
            right_side = padded[jnp.maximum(cell_cols, 0)].astype(jnp.float32)
            product = jnp.einsum('qrk,qck->qrc', left_side, right_side, precision=highest)
            return cell_tiles + jnp.where(live_slots[:, None, None], product, 0.0)
        by_cell = lax.map(cell_update, (by_cell, row_ids, col_ids))
    return jnp.zeros_like(stored_tiles).at[cell_owner].set(by_cell)
```

```python
import math

import jax
import jax.numpy as jnp
import numpy as np
from jax import lax
from jax.experimental import pallas as pl
from jax.experimental.pallas import tpu as pltpu
from jax.sharding import PartitionSpec as P

NB = 32


def shortened(x):

    def short(part):
        return part.astype(jnp.bfloat16) if part.dtype == jnp.float32 else part

    return jax.tree.map(short, x)


def layout(groups, per_group):
    half_group = per_group // 2
    slot_count = per_group * (per_group + 1) // 2
    row_table = np.full((groups * groups, slot_count), -1, np.int32)
    col_table = np.full((groups * groups, slot_count), -1, np.int32)
    for first_group in range(groups):
        for second_group in range(groups):
            cell_index = first_group * groups + second_group
            for inner_row in range(per_group):
                if first_group == second_group:
                    for inner_column in range(inner_row + 1):
                        slot_index = inner_row * (inner_row + 1) // 2 + inner_column
                        row_table[cell_index, slot_index] = first_group * per_group + inner_row
                        col_table[cell_index, slot_index] = first_group * per_group + inner_column
                else:
                    for inner_column in range(half_group):
                        slot_index = inner_row * half_group + inner_column
                        if first_group > second_group:
                            row_table[cell_index, slot_index] = first_group * per_group + inner_row
                            col_table[cell_index, slot_index] = (
                                second_group * per_group + inner_column
                            )
                        else:
                            row_table[cell_index, slot_index] = second_group * per_group + inner_row
                            col_table[cell_index, slot_index] = (
                                first_group * per_group + half_group + inner_column
                            )
    return (row_table, col_table)


def untiled(stored_tiles, cell_owner):
    tri_count = lax.axis_size("tri")
    groups = math.isqrt(tri_count)
    per_group = NB // groups
    half_group = per_group // 2
    strip_rows = stored_tiles.shape[2]
    block_order = stored_tiles.shape[3]
    row_table, col_table = layout(groups, per_group)
    position = lax.axis_index("tri")
    my_cell = jnp.sum(jnp.where(cell_owner == position, jnp.arange(tri_count, dtype=jnp.int32), 0))
    cell_down = my_cell // groups
    cell_across = my_cell % groups
    row_group = jnp.maximum(cell_down, cell_across)
    col_group = jnp.minimum(cell_down, cell_across)
    my_rows = jnp.asarray(row_table)[my_cell]
    my_cols = jnp.asarray(col_table)[my_cell]
    row_local = jnp.clip(my_rows - row_group * per_group, 0, per_group - 1)
    col_local = jnp.clip(my_cols - col_group * per_group, 0, per_group - 1)
    holders = cell_owner[jnp.arange(groups) * groups]
    highest = lax.Precision.HIGHEST
    current = stored_tiles[0]
    lower_slots = np.array([member * half_group for member in range(per_group)], np.int32)
    first_slots = np.array(
        [member * (member + 1) // 2 if member > 0 else 0 for member in range(per_group)], np.int32
    )
    keep_first = np.array([1.0 if member > 0 else 0.0 for member in range(per_group)], np.float32)
    from_lower = current[lower_slots]
    from_first = current[first_slots] * keep_first[:, None, None]
    holder_part = jnp.where(cell_down > 0, from_lower, from_first)
    holder_part = jnp.where(cell_across == 0, holder_part, 0.0).astype(jnp.bfloat16)
    pivot_slot = 0 // 2
    pivot_part = jnp.where(my_cell == 0, current[pivot_slot], 0.0)
    piece_size = holder_part.size // tri_count
    pivot_piece = pivot_part.size // tri_count
    spread_panel = lax.all_to_all(
        holder_part.reshape(tri_count, piece_size), "tri", split_axis=0, concat_axis=0, tiled=True
    )
    spread_pivot = lax.all_to_all(
        pivot_part.reshape(tri_count, pivot_piece).astype(jnp.bfloat16),
        "tri",
        split_axis=0,
        concat_axis=0,
        tiled=True,
    ).astype(jnp.float32)
    picked_panel = spread_panel[holders][:, None, :]
    picked_pivot = spread_pivot[holders[0]][None, :]
    whole_panel = lax.all_gather(picked_panel, "tri", axis=1, tiled=True)
    whole_pivot = lax.all_gather(
        picked_pivot.astype(jnp.bfloat16), "tri", axis=0, tiled=True
    ).astype(picked_pivot.dtype)
    panels = whole_panel.reshape(groups, per_group, strip_rows, block_order)
    pivot_strip = whole_pivot.reshape(strip_rows, block_order)
    own_strips = panels[row_group]
    other_strips = panels[col_group]
    pivot_block = lax.all_gather(
        pivot_strip.astype(jnp.bfloat16), "sub", axis=0, tiled=True
    ).astype(pivot_strip.dtype)
    partner = lax.all_gather(other_strips, "sub", axis=1, tiled=True)
    gram_matrix = jnp.dot(pivot_block.T, pivot_block, precision=highest)
    factor = jnp.linalg.cholesky(gram_matrix)
    column_count = block_order // lax.axis_size("sub")
    first_column = lax.axis_index("sub") * column_count
    columns = lax.dynamic_slice_in_dim(pivot_block.T, first_column, column_count, 1)
    column_part = jax.scipy.linalg.cho_solve((factor, True), columns)
    inverse = lax.all_gather(shortened(column_part), "sub", axis=1, tiled=True).astype(
        column_part.dtype
    )
    scaled = jnp.einsum(
        "irk,kc->irc", own_strips.astype(jnp.float32), inverse, precision=highest
    ).astype(jnp.bfloat16)
    left_slots = scaled[row_local]
    right_slots = partner[col_local]
    update = jnp.einsum("qrk,qck->qrc", left_slots, right_slots, preferred_element_type=jnp.float32)
    live_slots = (my_rows > 0) & (my_cols > 0)
    current = current + jnp.where(live_slots[:, None, None], update, 0.0)
    return current[None]


class Plan:
    def __init__(self, tri, subs, slots, strip, order, chunks):
        self.tri, self.subs, self.slots, self.strip, self.order = tri, subs, slots, strip, order
        self.chunks = chunks
        self.groups = math.isqrt(tri)
        self.per_group = NB // self.groups
        self.half_group = self.per_group // 2
        self.half_tri = tri // 2
        self.piece = strip // self.half_tri
        self.wide = self.half_group // chunks
        self.in_chunk = 2 * self.wide
        self.o_sub = 0
        self.o_diag = 1
        self.o_slot = 2
        self.o_src = self.o_slot + self.per_group
        self.o_here = self.o_src + self.groups
        self.o_rg = self.o_here + self.groups
        self.o_cg = self.o_rg + self.half_tri
        self.o_hf = self.o_cg + self.half_tri
        self.o_i = self.o_hf + self.half_tri
        self.o_j = self.o_i + slots
        self.o_live = self.o_j + slots
        self.o_new = self.o_live + slots
        self.size = self.o_new + slots

    def tiled(self):
        return (
            self.piece % 16 == 0
            and self.order % 128 == 0
            and self.half_group % self.chunks == 0
            and self.groups * self.groups == self.tri
            and self.subs * self.strip == self.order
        )

    def tile_of(self, chunk, place):
        half, inner = divmod(place, self.wide)
        return half * self.half_group + chunk * self.wide + inner


def table_call(p, cell_owner):
    def kernel(owner, out, cell_of):
        position = lax.axis_index("tri")
        for cell in range(p.tri):
            cell_of[owner[cell]] = cell

        def split(cell):
            down = cell // p.groups
            across = cell - down * p.groups
            return down, across

        down, across = split(cell_of[position])
        row_group = jnp.maximum(down, across)
        col_group = jnp.minimum(down, across)
        diag = down == across
        my_half = position // p.half_tri
        out[p.o_sub] = lax.axis_index("sub")
        out[p.o_diag] = jnp.where(diag, 1, 0)
        for chunk in range(p.chunks):
            for place in range(p.in_chunk):
                member = p.tile_of(chunk, place)
                out[p.o_slot + chunk * p.in_chunk + place] = jnp.where(
                    down > 0, member * p.half_group, member * (member + 1) // 2
                )
        for group in range(p.groups):
            holder = owner[group * p.groups]
            half = holder // p.half_tri
            out[p.o_src + group] = holder - half * p.half_tri
            out[p.o_here + group] = jnp.where(half == my_half, 1, 0)
        for end in range(p.half_tri):
            there_down, there_across = split(cell_of[my_half * p.half_tri + end])
            out[p.o_rg + end] = jnp.maximum(there_down, there_across)
            out[p.o_cg + end] = jnp.minimum(there_down, there_across)
            out[p.o_hf + end] = jnp.where(there_down < there_across, 1, 0)
        col_shift = jnp.where(down < across, p.half_group, 0)
        triangle = [(i, j) for i in range(p.per_group) for j in range(i + 1)]
        for slot in range(p.slots):
            tri_i, tri_j = triangle[slot] if slot < len(triangle) else (0, -1)
            box_i, box_j = divmod(slot, p.half_group)
            if box_i >= p.per_group:
                box_i, box_j = 0, -1
            inner_i = jnp.where(diag, tri_i, box_i)
            inner_j = jnp.where(diag, tri_j, box_j)
            row = row_group * p.per_group + inner_i
            col = col_group * p.per_group + jnp.where(diag, 0, col_shift) + inner_j
            live = (inner_j >= 0) & (row > 0) & (col > 0)
            out[p.o_i + slot] = inner_i
            out[p.o_j + slot] = jnp.maximum(inner_j, 0)
            out[p.o_live + slot] = jnp.where(live, 1, 0)
            new_tri = 1 if tri_j == 0 else 0
            new_box = 1 if box_j == 0 else 0
            out[p.o_new + slot] = jnp.where(diag, new_tri, new_box)

    return pl.pallas_call(
        kernel,
        out_shape=jax.ShapeDtypeStruct((p.size,), jnp.int32),
        in_specs=[pl.BlockSpec(memory_space=pltpu.SMEM)],
        out_specs=pl.BlockSpec(memory_space=pltpu.SMEM),
        scratch_shapes=[pltpu.SMEM((p.tri,), jnp.int32)],
        name="table",
    )(cell_owner)


def extract_call(p, table, current, chunk):
    def kernel(t, tile, out):
        out[...] = tile[...].reshape(p.half_tri, 1, p.piece, p.order).astype(jnp.bfloat16)

    return pl.pallas_call(
        kernel,
        out_shape=jax.ShapeDtypeStruct((p.half_tri, p.in_chunk, p.piece, p.order), jnp.bfloat16),
        grid_spec=pltpu.PrefetchScalarGridSpec(
            num_scalar_prefetch=1,
            grid=(p.in_chunk,),
            in_specs=[
                pl.BlockSpec(
                    (1, p.strip, p.order),
                    lambda i, t: (t[p.o_slot + chunk * p.in_chunk + i], 0, 0),
                )
            ],
            out_specs=pl.BlockSpec(
                (p.half_tri, 1, p.piece, p.order), lambda i, t: (0, i, 0, 0)
            ),
        ),
        name=f"extract{chunk}",
    )(table, current)


def pick_call(p, table, spread):
    def kernel(t, spread_ref, out, sems):
        copies = [
            pltpu.make_async_copy(spread_ref.at[t[p.o_src + g]], out.at[g], sems.at[g])
            for g in range(p.groups)
        ]
        for copy in copies:
            copy.start()
        for copy in copies:
            copy.wait()

    any_space = pl.BlockSpec(memory_space=pl.ANY)
    return pl.pallas_call(
        kernel,
        out_shape=jax.ShapeDtypeStruct((p.groups,) + spread.shape[1:], jnp.bfloat16),
        grid_spec=pltpu.PrefetchScalarGridSpec(
            num_scalar_prefetch=1,
            grid=(),
            in_specs=[any_space],
            out_specs=any_space,
            scratch_shapes=[pltpu.SemaphoreType.DMA((p.groups,))],
        ),
        name="pick",
    )(table, spread)


def build_call(p, table, near, far, with_pivot):
    rows = p.in_chunk + p.wide + (1 if with_pivot else 0)

    def kernel(t, near_ref, far_ref, out, sems):
        def part(group, first, count, end, place, sem):
            here = t[p.o_here + group] == 1
            target = out.at[end, pl.ds(place, count)]

            @pl.when(here)
            def _():
                pltpu.make_async_copy(near_ref.at[group, pl.ds(first, count)], target, sem).start()

            @pl.when(jnp.logical_not(here))
            def _():
                pltpu.make_async_copy(far_ref.at[group, pl.ds(first, count)], target, sem).start()

        for end in range(p.half_tri):
            part(t[p.o_rg + end], 0, p.in_chunk, end, 0, sems.at[end, 0])
            part(
                t[p.o_cg + end],
                t[p.o_hf + end] * p.wide,
                p.wide,
                end,
                p.in_chunk,
                sems.at[end, 1],
            )
            if with_pivot:
                part(0, 0, 1, end, p.in_chunk + p.wide, sems.at[end, 2])

        def await_part(end, place, count, sem):
            target = out.at[end, pl.ds(place, count)]
            pltpu.make_async_copy(near_ref.at[0, pl.ds(0, count)], target, sem).wait()

        for end in range(p.half_tri):
            await_part(end, 0, p.in_chunk, sems.at[end, 0])
            await_part(end, p.in_chunk, p.wide, sems.at[end, 1])
            if with_pivot:
                await_part(end, p.in_chunk + p.wide, 1, sems.at[end, 2])

    any_space = pl.BlockSpec(memory_space=pl.ANY)
    return pl.pallas_call(
        kernel,
        out_shape=jax.ShapeDtypeStruct((p.half_tri, rows, p.piece, p.order), jnp.bfloat16),
        grid_spec=pltpu.PrefetchScalarGridSpec(
            num_scalar_prefetch=1,
            grid=(),
            in_specs=[any_space, any_space],
            out_specs=any_space,
            scratch_shapes=[pltpu.SemaphoreType.DMA((p.half_tri, 3))],
        ),
        name="build",
    )(table, near, far)


def inverse_call(p, table, arrived):
    place = p.in_chunk + p.wide
    order = p.order

    def kernel(t, *refs):
        sources = refs[: p.subs]
        high, low, pivot, x_wide, x_half, e_ref, sem = refs[p.subs :]
        for shift in range(p.subs):
            strip = lax.rem(t[p.o_sub] + shift, p.subs) * p.strip
            for s in range(p.half_tri):
                at = pl.multiple_of(strip + s * p.piece, p.piece)
                pltpu.make_async_copy(
                    sources[shift].at[s, place], pivot.at[pl.ds(at, p.piece)], sem
                ).start()
        pltpu.make_async_copy(pivot, pivot, sem).wait()

        def dot(a, b):
            return lax.dot_general(
                a, b, (((1,), (0,)), ((), ())), preferred_element_type=jnp.float32
            )

        def eye():
            r = lax.broadcasted_iota(jnp.int32, (order, order), 0)
            c = lax.broadcasted_iota(jnp.int32, (order, order), 1)
            return jnp.where(r == c, 1.0, 0.0)

        square = dot(pivot[...], pivot[...])
        bound = jnp.max(jnp.sum(jnp.abs(square), axis=1))
        start = pivot[...].astype(jnp.float32) * (-1.0 / bound)
        x_wide[...] = start
        x_half[...] = start.astype(jnp.bfloat16)

        def coarse_on(carry):
            step, error, noise = carry
            return (step < 40) & (error > 0.01) & (noise < 0.1)

        def coarse(carry):
            step, _, _ = carry
            x = x_half[...]
            residual = eye() - dot(pivot[...], x)
            e_ref[...] = residual.astype(jnp.bfloat16)
            error = jnp.sum(residual * residual)
            new = x.astype(jnp.float32) + dot(x, e_ref[...])
            x_wide[...] = new
            x_half[...] = new.astype(jnp.bfloat16)
            noise = jnp.sum(new * new) * bound * 2.0**-18
            return step + 1, error, noise

        lax.while_loop(coarse_on, coarse, (jnp.int32(0), jnp.float32(1e30), jnp.float32(0.0)))

        def fine_on(carry):
            step, error, before = carry
            stuck = (before < 0.5) & (error > 0.5 * before)
            return (step < 100) & (error > 1e-4) & jnp.logical_not(stuck)

        def fine(carry):
            step, before, _ = carry
            x = x_wide[...]
            x_high = x.astype(jnp.bfloat16)
            x_low = (x - x_high.astype(jnp.float32)).astype(jnp.bfloat16)
            residual = eye() - (dot(pivot[...], x_high) + dot(pivot[...], x_low))
            error = jnp.sum(residual * residual)
            e_high = residual.astype(jnp.bfloat16)
            e_low = (residual - e_high.astype(jnp.float32)).astype(jnp.bfloat16)
            x_wide[...] = x + (dot(x_high, e_high) + (dot(x_high, e_low) + dot(x_low, e_high)))
            return step + 1, error, before

        lax.while_loop(fine_on, fine, (jnp.int32(0), jnp.float32(1e30), jnp.float32(1e30)))
        x = x_wide[...]
        rounded = x.astype(jnp.bfloat16)
        high[...] = rounded
        low[...] = (x - rounded.astype(jnp.float32)).astype(jnp.bfloat16)

    any_space = pl.BlockSpec(memory_space=pl.ANY)
    whole = pl.BlockSpec((order, order), lambda t: (0, 0))
    square_shape = jax.ShapeDtypeStruct((order, order), jnp.bfloat16)
    return pl.pallas_call(
        kernel,
        out_shape=(square_shape, square_shape),
        grid_spec=pltpu.PrefetchScalarGridSpec(
            num_scalar_prefetch=1,
            grid=(),
            in_specs=[any_space] * p.subs,
            out_specs=(pl.BlockSpec(memory_space=pltpu.VMEM),) * 2,
            scratch_shapes=[
                pltpu.VMEM((order, order), jnp.bfloat16),
                pltpu.VMEM((order, order), jnp.float32),
                pltpu.VMEM((order, order), jnp.bfloat16),
                pltpu.VMEM((order, order), jnp.bfloat16),
                pltpu.SemaphoreType.DMA,
            ],
        ),
        name="inverse",
    )(table, *arrived)


def update_call(p, table, current, arrived, inverse):
    per_step = 2 if p.slots % 2 == 0 else 1

    def kernel(t, tiles, high, low, *refs):
        sources = [refs[k * p.subs : (k + 1) * p.subs] for k in range(p.chunks)]
        out, left, right, scaled, left_sem, right_sem = refs[p.chunks * p.subs :]
        step = pl.program_id(0)
        diag = t[p.o_diag] == 1

        @pl.when(step == 0)
        def _():
            for k in range(p.chunks):
                for shift in range(p.subs):
                    ref = sources[k][shift]
                    strip = lax.rem(t[p.o_sub] + shift, p.subs) * p.strip
                    for s in range(p.half_tri):
                        at = pl.multiple_of(strip + s * p.piece, p.piece)
                        for half in range(2):
                            tiles_at = pl.ds(half * p.half_group + k * p.wide, p.wide)
                            part = ref.at[s, pl.ds(half * p.wide, p.wide)]
                            if shift == 0:
                                pltpu.make_async_copy(
                                    part, left.at[tiles_at, pl.ds(s * p.piece, p.piece)], left_sem
                                ).start()

                            @pl.when(diag)
                            def _():
                                pltpu.make_async_copy(
                                    part, right.at[tiles_at, pl.ds(at, p.piece)], right_sem
                                ).start()

                        @pl.when(jnp.logical_not(diag))
                        def _():
                            pltpu.make_async_copy(
                                ref.at[s, pl.ds(p.in_chunk, p.wide)],
                                right.at[pl.ds(k * p.wide, p.wide), pl.ds(at, p.piece)],
                                right_sem,
                            ).start()

            pltpu.make_async_copy(left, left, left_sem).wait()

            @pl.when(diag)
            def _():
                pltpu.make_async_copy(right, right, right_sem).wait()

            @pl.when(jnp.logical_not(diag))
            def _():
                some = right.at[pl.ds(0, p.half_group)]
                pltpu.make_async_copy(some, some, right_sem).wait()

        for u in range(per_step):
            slot = step * per_step + u

            @pl.when(t[p.o_new + slot] == 1)
            def _():
                strip = left[t[p.o_i + slot]]
                dims = (((1,), (0,)), ((), ()))
                product = lax.dot_general(
                    strip, high[...], dims, preferred_element_type=jnp.float32
                ) + lax.dot_general(strip, low[...], dims, preferred_element_type=jnp.float32)
                scaled[...] = product.astype(jnp.bfloat16)

            live = t[p.o_live + slot] == 1

            @pl.when(live)
            def _():
                out[u] = tiles[u] + lax.dot_general(
                    scaled[...],
                    right[t[p.o_j + slot]],
                    (((1,), (1,)), ((), ())),
                    preferred_element_type=jnp.float32,
                )

            @pl.when(jnp.logical_not(live))
            def _():
                out[u] = tiles[u]

    any_space = pl.BlockSpec(memory_space=pl.ANY)
    block = pl.BlockSpec((per_step, p.strip, p.order), lambda i, t: (i, 0, 0))
    square = pl.BlockSpec((p.order, p.order), lambda i, t: (0, 0))
    return pl.pallas_call(
        kernel,
        out_shape=jax.ShapeDtypeStruct(current.shape, jnp.float32),
        grid_spec=pltpu.PrefetchScalarGridSpec(
            num_scalar_prefetch=1,
            grid=(p.slots // per_step,),
            in_specs=[block, square, square] + [any_space] * (p.chunks * p.subs),
            out_specs=block,
            scratch_shapes=[
                pltpu.VMEM((p.per_group, p.strip, p.order), jnp.bfloat16),
                pltpu.VMEM((p.per_group, p.order, p.order), jnp.bfloat16),
                pltpu.VMEM((p.strip, p.order), jnp.bfloat16),
                pltpu.SemaphoreType.DMA,
                pltpu.SemaphoreType.DMA,
            ],
        ),
        compiler_params=pltpu.CompilerParams(dimension_semantics=("arbitrary",)),
        name="update",
    )(table, current, *inverse, *[ref for chunk in arrived for ref in chunk])


def planned(p, stored_tiles, cell_owner):
    table = table_call(p, cell_owner)
    current = stored_tiles[0]
    halves = [list(range(h * p.half_tri, (h + 1) * p.half_tri)) for h in range(2)]
    swap = [(i, (i + p.half_tri) % p.tri) for i in range(p.tri)]

    def exchange(x):
        return lax.all_to_all(
            x, "tri", split_axis=0, concat_axis=0, tiled=True, axis_index_groups=halves
        )

    def arrivals(x):
        return [x] + [
            lax.ppermute(x, "sub", [((i + shift) % p.subs, i) for i in range(p.subs)])
            for shift in range(1, p.subs)
        ]

    near = []
    for chunk in range(p.chunks):
        spread = exchange(extract_call(p, table, current, chunk))
        near.append(pick_call(p, table, spread))
    far = [lax.ppermute(x, "tri", swap) for x in near]
    arrived = []
    for chunk in range(p.chunks):
        built = build_call(p, table, near[chunk], far[chunk], chunk == 0)
        arrived.append(arrivals(exchange(built)))
    inverse = inverse_call(p, table, arrived[0])
    return update_call(p, table, current, arrived, inverse)[None]


def shards(stored_tiles, cell_owner):
    p = Plan(
        lax.axis_size("tri"),
        lax.axis_size("sub"),
        stored_tiles.shape[1],
        stored_tiles.shape[2],
        stored_tiles.shape[3],
        2,
    )
    if p.tiled():
        return planned(p, stored_tiles, cell_owner)
    return untiled(stored_tiles, cell_owner)


def solution(mesh):
    placed = (P("tri", None, "sub", None), P())
    return jax.shard_map(
        shards, mesh=mesh, in_specs=placed, out_specs=P("tri", None, "sub", None), check_vma=False
    )
```

```python
import math

import jax
import jax.numpy as jnp
import numpy as np
from jax import lax
from jax.experimental import pallas as pl
from jax.experimental.pallas import tpu as pltpu
from jax.sharding import PartitionSpec as P

NB = 32


def shortened(x):

    def short(part):
        return part.astype(jnp.bfloat16) if part.dtype == jnp.float32 else part

    return jax.tree.map(short, x)


def layout(groups, per_group):
    half_group = per_group // 2
    slot_count = per_group * (per_group + 1) // 2
    row_table = np.full((groups * groups, slot_count), -1, np.int32)
    col_table = np.full((groups * groups, slot_count), -1, np.int32)
    for first_group in range(groups):
        for second_group in range(groups):
            cell_index = first_group * groups + second_group
            for inner_row in range(per_group):
                if first_group == second_group:
                    for inner_column in range(inner_row + 1):
                        slot_index = inner_row * (inner_row + 1) // 2 + inner_column
                        row_table[cell_index, slot_index] = first_group * per_group + inner_row
                        col_table[cell_index, slot_index] = first_group * per_group + inner_column
                else:
                    for inner_column in range(half_group):
                        slot_index = inner_row * half_group + inner_column
                        if first_group > second_group:
                            row_table[cell_index, slot_index] = first_group * per_group + inner_row
                            col_table[cell_index, slot_index] = (
                                second_group * per_group + inner_column
                            )
                        else:
                            row_table[cell_index, slot_index] = second_group * per_group + inner_row
                            col_table[cell_index, slot_index] = (
                                first_group * per_group + half_group + inner_column
                            )
    return (row_table, col_table)


def untiled(stored_tiles, cell_owner):
    tri_count = lax.axis_size("tri")
    groups = math.isqrt(tri_count)
    per_group = NB // groups
    half_group = per_group // 2
    strip_rows = stored_tiles.shape[2]
    block_order = stored_tiles.shape[3]
    row_table, col_table = layout(groups, per_group)
    position = lax.axis_index("tri")
    my_cell = jnp.sum(jnp.where(cell_owner == position, jnp.arange(tri_count, dtype=jnp.int32), 0))
    cell_down = my_cell // groups
    cell_across = my_cell % groups
    row_group = jnp.maximum(cell_down, cell_across)
    col_group = jnp.minimum(cell_down, cell_across)
    my_rows = jnp.asarray(row_table)[my_cell]
    my_cols = jnp.asarray(col_table)[my_cell]
    row_local = jnp.clip(my_rows - row_group * per_group, 0, per_group - 1)
    col_local = jnp.clip(my_cols - col_group * per_group, 0, per_group - 1)
    holders = cell_owner[jnp.arange(groups) * groups]
    highest = lax.Precision.HIGHEST
    current = stored_tiles[0]
    lower_slots = np.array([member * half_group for member in range(per_group)], np.int32)
    first_slots = np.array(
        [member * (member + 1) // 2 if member > 0 else 0 for member in range(per_group)], np.int32
    )
    keep_first = np.array([1.0 if member > 0 else 0.0 for member in range(per_group)], np.float32)
    from_lower = current[lower_slots]
    from_first = current[first_slots] * keep_first[:, None, None]
    holder_part = jnp.where(cell_down > 0, from_lower, from_first)
    holder_part = jnp.where(cell_across == 0, holder_part, 0.0).astype(jnp.bfloat16)
    pivot_slot = 0 // 2
    pivot_part = jnp.where(my_cell == 0, current[pivot_slot], 0.0)
    piece_size = holder_part.size // tri_count
    pivot_piece = pivot_part.size // tri_count
    spread_panel = lax.all_to_all(
        holder_part.reshape(tri_count, piece_size), "tri", split_axis=0, concat_axis=0, tiled=True
    )
    spread_pivot = lax.all_to_all(
        pivot_part.reshape(tri_count, pivot_piece).astype(jnp.bfloat16),
        "tri",
        split_axis=0,
        concat_axis=0,
        tiled=True,
    ).astype(jnp.float32)
    picked_panel = spread_panel[holders][:, None, :]
    picked_pivot = spread_pivot[holders[0]][None, :]
    whole_panel = lax.all_gather(picked_panel, "tri", axis=1, tiled=True)
    whole_pivot = lax.all_gather(
        picked_pivot.astype(jnp.bfloat16), "tri", axis=0, tiled=True
    ).astype(picked_pivot.dtype)
    panels = whole_panel.reshape(groups, per_group, strip_rows, block_order)
    pivot_strip = whole_pivot.reshape(strip_rows, block_order)
    own_strips = panels[row_group]
    other_strips = panels[col_group]
    pivot_block = lax.all_gather(
        pivot_strip.astype(jnp.bfloat16), "sub", axis=0, tiled=True
    ).astype(pivot_strip.dtype)
    partner = lax.all_gather(other_strips, "sub", axis=1, tiled=True)
    gram_matrix = jnp.dot(pivot_block.T, pivot_block, precision=highest)
    factor = jnp.linalg.cholesky(gram_matrix)
    column_count = block_order // lax.axis_size("sub")
    first_column = lax.axis_index("sub") * column_count
    columns = lax.dynamic_slice_in_dim(pivot_block.T, first_column, column_count, 1)
    column_part = jax.scipy.linalg.cho_solve((factor, True), columns)
    inverse = lax.all_gather(shortened(column_part), "sub", axis=1, tiled=True).astype(
        column_part.dtype
    )
    scaled = jnp.einsum(
        "irk,kc->irc", own_strips.astype(jnp.float32), inverse, precision=highest
    ).astype(jnp.bfloat16)
    left_slots = scaled[row_local]
    right_slots = partner[col_local]
    update = jnp.einsum("qrk,qck->qrc", left_slots, right_slots, preferred_element_type=jnp.float32)
    live_slots = (my_rows > 0) & (my_cols > 0)
    current = current + jnp.where(live_slots[:, None, None], update, 0.0)
    return current[None]


class Plan:
    def __init__(self, tri, subs, slots, strip, order, chunks):
        self.tri, self.subs, self.slots, self.strip, self.order = tri, subs, slots, strip, order
        self.chunks = chunks
        self.groups = math.isqrt(tri)
        self.per_group = NB // self.groups
        self.half_group = self.per_group // 2
        self.half_tri = tri // 2
        self.piece = strip // self.half_tri
        self.wide = self.half_group // chunks
        self.in_chunk = 2 * self.wide
        self.o_sub = 0
        self.o_diag = 1
        self.o_slot = 2
        self.o_src = self.o_slot + self.per_group
        self.o_here = self.o_src + self.groups
        self.o_rg = self.o_here + self.groups
        self.o_cg = self.o_rg + self.half_tri
        self.o_hf = self.o_cg + self.half_tri
        self.o_i = self.o_hf + self.half_tri
        self.o_j = self.o_i + slots
        self.o_live = self.o_j + slots
        self.o_new = self.o_live + slots
        self.size = self.o_new + slots

    def tiled(self):
        return (
            self.piece % 16 == 0
            and self.order % 128 == 0
            and self.half_group % self.chunks == 0
            and self.groups * self.groups == self.tri
            and self.subs * self.strip == self.order
        )

    def tile_of(self, chunk, place):
        half, inner = divmod(place, self.wide)
        return half * self.half_group + chunk * self.wide + inner


def table_call(p, cell_owner):
    def kernel(owner, out, cell_of):
        position = lax.axis_index("tri")
        for cell in range(p.tri):
            cell_of[owner[cell]] = cell

        def split(cell):
            down = cell // p.groups
            across = cell - down * p.groups
            return down, across

        down, across = split(cell_of[position])
        row_group = jnp.maximum(down, across)
        col_group = jnp.minimum(down, across)
        diag = down == across
        my_half = position // p.half_tri
        out[p.o_sub] = lax.axis_index("sub")
        out[p.o_diag] = jnp.where(diag, 1, 0)
        for chunk in range(p.chunks):
            for place in range(p.in_chunk):
                member = p.tile_of(chunk, place)
                out[p.o_slot + chunk * p.in_chunk + place] = jnp.where(
                    down > 0, member * p.half_group, member * (member + 1) // 2
                )
        for group in range(p.groups):
            holder = owner[group * p.groups]
            half = holder // p.half_tri
            out[p.o_src + group] = holder - half * p.half_tri
            out[p.o_here + group] = jnp.where(half == my_half, 1, 0)
        for end in range(p.half_tri):
            there_down, there_across = split(cell_of[my_half * p.half_tri + end])
            out[p.o_rg + end] = jnp.maximum(there_down, there_across)
            out[p.o_cg + end] = jnp.minimum(there_down, there_across)
            out[p.o_hf + end] = jnp.where(there_down < there_across, 1, 0)
        col_shift = jnp.where(down < across, p.half_group, 0)
        triangle = [(i, j) for i in range(p.per_group) for j in range(i + 1)]
        for slot in range(p.slots):
            tri_i, tri_j = triangle[slot] if slot < len(triangle) else (0, -1)
            box_i, box_j = divmod(slot, p.half_group)
            if box_i >= p.per_group:
                box_i, box_j = 0, -1
            inner_i = jnp.where(diag, tri_i, box_i)
            inner_j = jnp.where(diag, tri_j, box_j)
            row = row_group * p.per_group + inner_i
            col = col_group * p.per_group + jnp.where(diag, 0, col_shift) + inner_j
            live = (inner_j >= 0) & (row > 0) & (col > 0)
            out[p.o_i + slot] = inner_i
            out[p.o_j + slot] = jnp.maximum(inner_j, 0)
            out[p.o_live + slot] = jnp.where(live, 1, 0)
            new_tri = 1 if tri_j == 0 else 0
            new_box = 1 if box_j == 0 else 0
            out[p.o_new + slot] = jnp.where(diag, new_tri, new_box)

    return pl.pallas_call(
        kernel,
        out_shape=jax.ShapeDtypeStruct((p.size,), jnp.int32),
        in_specs=[pl.BlockSpec(memory_space=pltpu.SMEM)],
        out_specs=pl.BlockSpec(memory_space=pltpu.SMEM),
        scratch_shapes=[pltpu.SMEM((p.tri,), jnp.int32)],
        name="table",
    )(cell_owner)


def extract_call(p, table, current, chunk):
    def kernel(t, tile, out):
        out[...] = tile[...].reshape(p.half_tri, 1, p.piece, p.order).astype(jnp.bfloat16)

    return pl.pallas_call(
        kernel,
        out_shape=jax.ShapeDtypeStruct((p.half_tri, p.in_chunk, p.piece, p.order), jnp.bfloat16),
        grid_spec=pltpu.PrefetchScalarGridSpec(
            num_scalar_prefetch=1,
            grid=(p.in_chunk,),
            in_specs=[
                pl.BlockSpec(
                    (1, p.strip, p.order),
                    lambda i, t: (t[p.o_slot + chunk * p.in_chunk + i], 0, 0),
                )
            ],
            out_specs=pl.BlockSpec(
                (p.half_tri, 1, p.piece, p.order), lambda i, t: (0, i, 0, 0)
            ),
        ),
        name=f"extract{chunk}",
    )(table, current)


def pick_call(p, table, spread):
    def kernel(t, spread_ref, out, sems):
        copies = [
            pltpu.make_async_copy(spread_ref.at[t[p.o_src + g]], out.at[g], sems.at[g])
            for g in range(p.groups)
        ]
        for copy in copies:
            copy.start()
        for copy in copies:
            copy.wait()

    return pl.pallas_call(
        kernel,
        out_shape=jax.ShapeDtypeStruct((p.groups,) + spread.shape[1:], jnp.bfloat16),
        grid_spec=pltpu.PrefetchScalarGridSpec(
            num_scalar_prefetch=1,
            grid=(),
            in_specs=[pl.BlockSpec(memory_space=pltpu.VMEM)],
            out_specs=pl.BlockSpec(memory_space=pl.ANY),
            scratch_shapes=[pltpu.SemaphoreType.DMA((p.groups,))],
        ),
        name="pick",
    )(table, spread)


def build_call(p, table, near, far, with_pivot):
    rows = p.in_chunk + p.wide + (1 if with_pivot else 0)

    def kernel(t, near_ref, far_ref, out, sems):
        def part(group, first, count, end, place, sem):
            here = t[p.o_here + group] == 1
            target = out.at[end, pl.ds(place, count)]

            @pl.when(here)
            def _():
                pltpu.make_async_copy(near_ref.at[group, pl.ds(first, count)], target, sem).start()

            @pl.when(jnp.logical_not(here))
            def _():
                pltpu.make_async_copy(far_ref.at[group, pl.ds(first, count)], target, sem).start()

        for end in range(p.half_tri):
            part(t[p.o_rg + end], 0, p.in_chunk, end, 0, sems.at[end, 0])
            part(
                t[p.o_cg + end],
                t[p.o_hf + end] * p.wide,
                p.wide,
                end,
                p.in_chunk,
                sems.at[end, 1],
            )
            if with_pivot:
                part(0, 0, 1, end, p.in_chunk + p.wide, sems.at[end, 2])

        def await_part(end, place, count, sem):
            target = out.at[end, pl.ds(place, count)]
            pltpu.make_async_copy(near_ref.at[0, pl.ds(0, count)], target, sem).wait()

        for end in range(p.half_tri):
            await_part(end, 0, p.in_chunk, sems.at[end, 0])
            await_part(end, p.in_chunk, p.wide, sems.at[end, 1])
            if with_pivot:
                await_part(end, p.in_chunk + p.wide, 1, sems.at[end, 2])

    return pl.pallas_call(
        kernel,
        out_shape=jax.ShapeDtypeStruct((p.half_tri, rows, p.piece, p.order), jnp.bfloat16),
        grid_spec=pltpu.PrefetchScalarGridSpec(
            num_scalar_prefetch=1,
            grid=(),
            in_specs=[pl.BlockSpec(memory_space=pltpu.VMEM)] * 2,
            out_specs=pl.BlockSpec(memory_space=pl.ANY),
            scratch_shapes=[pltpu.SemaphoreType.DMA((p.half_tri, 3))],
        ),
        name="build",
    )(table, near, far)


def inverse_call(p, table, arrived):
    place = p.in_chunk + p.wide
    order = p.order

    def kernel(t, *refs):
        sources = refs[: p.subs]
        high, low, pivot, x_wide, x_half, e_ref, sem = refs[p.subs :]
        for shift in range(p.subs):
            strip = lax.rem(t[p.o_sub] + shift, p.subs) * p.strip
            for s in range(p.half_tri):
                at = pl.multiple_of(strip + s * p.piece, p.piece)
                pltpu.make_async_copy(
                    sources[shift].at[s, place], pivot.at[pl.ds(at, p.piece)], sem
                ).start()
        pltpu.make_async_copy(pivot, pivot, sem).wait()

        def dot(a, b):
            return lax.dot_general(
                a, b, (((1,), (0,)), ((), ())), preferred_element_type=jnp.float32
            )

        def eye():
            r = lax.broadcasted_iota(jnp.int32, (order, order), 0)
            c = lax.broadcasted_iota(jnp.int32, (order, order), 1)
            return jnp.where(r == c, 1.0, 0.0)

        square = dot(pivot[...], pivot[...])
        bound = jnp.max(jnp.sum(jnp.abs(square), axis=1))
        start = pivot[...].astype(jnp.float32) * (-1.0 / bound)
        x_wide[...] = start
        x_half[...] = start.astype(jnp.bfloat16)

        def coarse_on(carry):
            step, error, noise = carry
            return (step < 40) & (error > 0.01) & (noise < 0.1)

        def coarse(carry):
            step, _, _ = carry
            x = x_half[...]
            residual = eye() - dot(pivot[...], x)
            e_ref[...] = residual.astype(jnp.bfloat16)
            error = jnp.sum(residual * residual)
            new = x.astype(jnp.float32) + dot(x, e_ref[...])
            x_wide[...] = new
            x_half[...] = new.astype(jnp.bfloat16)
            noise = jnp.sum(new * new) * bound * 2.0**-18
            return step + 1, error, noise

        lax.while_loop(coarse_on, coarse, (jnp.int32(0), jnp.float32(1e30), jnp.float32(0.0)))

        def fine_on(carry):
            step, error, before = carry
            stuck = (before < 0.5) & (error > 0.5 * before)
            return (step < 100) & (error > 1e-4) & jnp.logical_not(stuck)

        def fine(carry):
            step, before, _ = carry
            x = x_wide[...]
            x_high = x.astype(jnp.bfloat16)
            x_low = (x - x_high.astype(jnp.float32)).astype(jnp.bfloat16)
            residual = eye() - (dot(pivot[...], x_high) + dot(pivot[...], x_low))
            error = jnp.sum(residual * residual)
            e_high = residual.astype(jnp.bfloat16)
            e_low = (residual - e_high.astype(jnp.float32)).astype(jnp.bfloat16)
            x_wide[...] = x + (dot(x_high, e_high) + (dot(x_high, e_low) + dot(x_low, e_high)))
            return step + 1, error, before

        lax.while_loop(fine_on, fine, (jnp.int32(0), jnp.float32(1e30), jnp.float32(1e30)))
        x = x_wide[...]
        rounded = x.astype(jnp.bfloat16)
        high[...] = rounded
        low[...] = (x - rounded.astype(jnp.float32)).astype(jnp.bfloat16)

    any_space = pl.BlockSpec(memory_space=pl.ANY)
    whole = pl.BlockSpec((order, order), lambda t: (0, 0))
    square_shape = jax.ShapeDtypeStruct((order, order), jnp.bfloat16)
    return pl.pallas_call(
        kernel,
        out_shape=(square_shape, square_shape),
        grid_spec=pltpu.PrefetchScalarGridSpec(
            num_scalar_prefetch=1,
            grid=(),
            in_specs=[any_space] * p.subs,
            out_specs=(pl.BlockSpec(memory_space=pltpu.VMEM),) * 2,
            scratch_shapes=[
                pltpu.VMEM((order, order), jnp.bfloat16),
                pltpu.VMEM((order, order), jnp.float32),
                pltpu.VMEM((order, order), jnp.bfloat16),
                pltpu.VMEM((order, order), jnp.bfloat16),
                pltpu.SemaphoreType.DMA,
            ],
        ),
        cost_estimate=pl.CostEstimate(
            flops=60 * 2 * order**3, bytes_accessed=4 * order**2, transcendentals=0
        ),
        name="inverse",
    )(table, *arrived)


def update_call(p, table, current, arrived, inverse):
    per_step = 2 if p.slots % 2 == 0 else 1

    def kernel(t, tiles, high, low, *refs):
        sources = [refs[k * p.subs : (k + 1) * p.subs] for k in range(p.chunks)]
        out, left, right, scaled, left_sem, right_sem = refs[p.chunks * p.subs :]
        step = pl.program_id(0)
        diag = t[p.o_diag] == 1

        @pl.when(step == 0)
        def _():
            for k in range(p.chunks):
                for shift in range(p.subs):
                    ref = sources[k][shift]
                    strip = lax.rem(t[p.o_sub] + shift, p.subs) * p.strip
                    for s in range(p.half_tri):
                        at = pl.multiple_of(strip + s * p.piece, p.piece)
                        for half in range(2):
                            tiles_at = pl.ds(half * p.half_group + k * p.wide, p.wide)
                            part = ref.at[s, pl.ds(half * p.wide, p.wide)]
                            if shift == 0:
                                pltpu.make_async_copy(
                                    part, left.at[tiles_at, pl.ds(s * p.piece, p.piece)], left_sem
                                ).start()

                            @pl.when(diag)
                            def _():
                                pltpu.make_async_copy(
                                    part, right.at[tiles_at, pl.ds(at, p.piece)], right_sem
                                ).start()

                        @pl.when(jnp.logical_not(diag))
                        def _():
                            pltpu.make_async_copy(
                                ref.at[s, pl.ds(p.in_chunk, p.wide)],
                                right.at[pl.ds(k * p.wide, p.wide), pl.ds(at, p.piece)],
                                right_sem,
                            ).start()

            pltpu.make_async_copy(left, left, left_sem).wait()

            @pl.when(diag)
            def _():
                pltpu.make_async_copy(right, right, right_sem).wait()

            @pl.when(jnp.logical_not(diag))
            def _():
                some = right.at[pl.ds(0, p.half_group)]
                pltpu.make_async_copy(some, some, right_sem).wait()

        for u in range(per_step):
            slot = step * per_step + u

            @pl.when(t[p.o_new + slot] == 1)
            def _():
                strip = left[t[p.o_i + slot]]
                dims = (((1,), (0,)), ((), ()))
                product = lax.dot_general(
                    strip, high[...], dims, preferred_element_type=jnp.float32
                ) + lax.dot_general(strip, low[...], dims, preferred_element_type=jnp.float32)
                scaled[...] = product.astype(jnp.bfloat16)

            live = t[p.o_live + slot] == 1

            @pl.when(live)
            def _():
                out[u] = tiles[u] + lax.dot_general(
                    scaled[...],
                    right[t[p.o_j + slot]],
                    (((1,), (1,)), ((), ())),
                    preferred_element_type=jnp.float32,
                )

            @pl.when(jnp.logical_not(live))
            def _():
                out[u] = tiles[u]

    any_space = pl.BlockSpec(memory_space=pl.ANY)
    block = pl.BlockSpec((per_step, p.strip, p.order), lambda i, t: (i, 0, 0))
    square = pl.BlockSpec((p.order, p.order), lambda i, t: (0, 0))
    return pl.pallas_call(
        kernel,
        out_shape=jax.ShapeDtypeStruct(current.shape, jnp.float32),
        grid_spec=pltpu.PrefetchScalarGridSpec(
            num_scalar_prefetch=1,
            grid=(p.slots // per_step,),
            in_specs=[block, square, square] + [any_space] * (p.chunks * p.subs),
            out_specs=block,
            scratch_shapes=[
                pltpu.VMEM((p.per_group, p.strip, p.order), jnp.bfloat16),
                pltpu.VMEM((p.per_group, p.order, p.order), jnp.bfloat16),
                pltpu.VMEM((p.strip, p.order), jnp.bfloat16),
                pltpu.SemaphoreType.DMA,
                pltpu.SemaphoreType.DMA,
            ],
        ),
        compiler_params=pltpu.CompilerParams(dimension_semantics=("arbitrary",)),
        name="update",
    )(table, current, *inverse, *[ref for chunk in arrived for ref in chunk])


def planned(p, stored_tiles, cell_owner):
    table = table_call(p, cell_owner)
    current = stored_tiles[0]
    halves = [list(range(h * p.half_tri, (h + 1) * p.half_tri)) for h in range(2)]
    swap = [(i, (i + p.half_tri) % p.tri) for i in range(p.tri)]

    def exchange(x):
        return lax.all_to_all(
            x, "tri", split_axis=0, concat_axis=0, tiled=True, axis_index_groups=halves
        )

    def arrivals(x):
        return [x] + [
            lax.ppermute(x, "sub", [((i + shift) % p.subs, i) for i in range(p.subs)])
            for shift in range(1, p.subs)
        ]

    near = []
    for chunk in range(p.chunks):
        spread = exchange(extract_call(p, table, current, chunk))
        near.append(pick_call(p, table, spread))
    far = [lax.ppermute(x, "tri", swap) for x in near]
    arrived = []
    for chunk in range(p.chunks):
        built = build_call(p, table, near[chunk], far[chunk], chunk == 0)
        arrived.append(arrivals(exchange(built)))
    inverse = inverse_call(p, table, arrived[0])
    return update_call(p, table, current, arrived, inverse)[None]


def shards(stored_tiles, cell_owner):
    p = Plan(
        lax.axis_size("tri"),
        lax.axis_size("sub"),
        stored_tiles.shape[1],
        stored_tiles.shape[2],
        stored_tiles.shape[3],
        2,
    )
    if p.tiled():
        return planned(p, stored_tiles, cell_owner)
    return untiled(stored_tiles, cell_owner)


def solution(mesh):
    placed = (P("tri", None, "sub", None), P())
    return jax.shard_map(
        shards, mesh=mesh, in_specs=placed, out_specs=P("tri", None, "sub", None), check_vma=False
    )
```

```python
import math

import jax
import jax.numpy as jnp
import numpy as np
from jax import lax
from jax.experimental import pallas as pl
from jax.experimental.pallas import tpu as pltpu
from jax.sharding import PartitionSpec as P


NB = 32


def shortened(x):

    def short(part):
        return part.astype(jnp.bfloat16) if part.dtype == jnp.float32 else part

    return jax.tree.map(short, x)


def layout(groups, per_group):
    half_group = per_group // 2
    slot_count = per_group * (per_group + 1) // 2
    row_table = np.full((groups * groups, slot_count), -1, np.int32)
    col_table = np.full((groups * groups, slot_count), -1, np.int32)
    for first_group in range(groups):
        for second_group in range(groups):
            cell_index = first_group * groups + second_group
            for inner_row in range(per_group):
                if first_group == second_group:
                    for inner_column in range(inner_row + 1):
                        slot_index = inner_row * (inner_row + 1) // 2 + inner_column
                        row_table[cell_index, slot_index] = first_group * per_group + inner_row
                        col_table[cell_index, slot_index] = first_group * per_group + inner_column
                else:
                    for inner_column in range(half_group):
                        slot_index = inner_row * half_group + inner_column
                        if first_group > second_group:
                            row_table[cell_index, slot_index] = first_group * per_group + inner_row
                            col_table[cell_index, slot_index] = (
                                second_group * per_group + inner_column
                            )
                        else:
                            row_table[cell_index, slot_index] = second_group * per_group + inner_row
                            col_table[cell_index, slot_index] = (
                                first_group * per_group + half_group + inner_column
                            )
    return (row_table, col_table)


def untiled(stored_tiles, cell_owner):
    tri_count = lax.axis_size("tri")
    groups = math.isqrt(tri_count)
    per_group = NB // groups
    half_group = per_group // 2
    strip_rows = stored_tiles.shape[2]
    block_order = stored_tiles.shape[3]
    row_table, col_table = layout(groups, per_group)
    position = lax.axis_index("tri")
    my_cell = jnp.sum(jnp.where(cell_owner == position, jnp.arange(tri_count, dtype=jnp.int32), 0))
    cell_down = my_cell // groups
    cell_across = my_cell % groups
    row_group = jnp.maximum(cell_down, cell_across)
    col_group = jnp.minimum(cell_down, cell_across)
    my_rows = jnp.asarray(row_table)[my_cell]
    my_cols = jnp.asarray(col_table)[my_cell]
    row_local = jnp.clip(my_rows - row_group * per_group, 0, per_group - 1)
    col_local = jnp.clip(my_cols - col_group * per_group, 0, per_group - 1)
    holders = cell_owner[jnp.arange(groups) * groups]
    highest = lax.Precision.HIGHEST
    current = stored_tiles[0]
    lower_slots = np.array([member * half_group for member in range(per_group)], np.int32)
    first_slots = np.array(
        [member * (member + 1) // 2 if member > 0 else 0 for member in range(per_group)], np.int32
    )
    keep_first = np.array([1.0 if member > 0 else 0.0 for member in range(per_group)], np.float32)
    from_lower = current[lower_slots]
    from_first = current[first_slots] * keep_first[:, None, None]
    holder_part = jnp.where(cell_down > 0, from_lower, from_first)
    holder_part = jnp.where(cell_across == 0, holder_part, 0.0).astype(jnp.bfloat16)
    pivot_slot = 0 // 2
    pivot_part = jnp.where(my_cell == 0, current[pivot_slot], 0.0)
    piece_size = holder_part.size // tri_count
    pivot_piece = pivot_part.size // tri_count
    spread_panel = lax.all_to_all(
        holder_part.reshape(tri_count, piece_size), "tri", split_axis=0, concat_axis=0, tiled=True
    )
    spread_pivot = lax.all_to_all(
        pivot_part.reshape(tri_count, pivot_piece).astype(jnp.bfloat16),
        "tri",
        split_axis=0,
        concat_axis=0,
        tiled=True,
    ).astype(jnp.float32)
    picked_panel = spread_panel[holders][:, None, :]
    picked_pivot = spread_pivot[holders[0]][None, :]
    whole_panel = lax.all_gather(picked_panel, "tri", axis=1, tiled=True)
    whole_pivot = lax.all_gather(
        picked_pivot.astype(jnp.bfloat16), "tri", axis=0, tiled=True
    ).astype(picked_pivot.dtype)
    panels = whole_panel.reshape(groups, per_group, strip_rows, block_order)
    pivot_strip = whole_pivot.reshape(strip_rows, block_order)
    own_strips = panels[row_group]
    other_strips = panels[col_group]
    pivot_block = lax.all_gather(
        pivot_strip.astype(jnp.bfloat16), "sub", axis=0, tiled=True
    ).astype(pivot_strip.dtype)
    partner = lax.all_gather(other_strips, "sub", axis=1, tiled=True)
    gram_matrix = jnp.dot(pivot_block.T, pivot_block, precision=highest)
    factor = jnp.linalg.cholesky(gram_matrix)
    column_count = block_order // lax.axis_size("sub")
    first_column = lax.axis_index("sub") * column_count
    columns = lax.dynamic_slice_in_dim(pivot_block.T, first_column, column_count, 1)
    column_part = jax.scipy.linalg.cho_solve((factor, True), columns)
    inverse = lax.all_gather(shortened(column_part), "sub", axis=1, tiled=True).astype(
        column_part.dtype
    )
    scaled = jnp.einsum(
        "irk,kc->irc", own_strips.astype(jnp.float32), inverse, precision=highest
    ).astype(jnp.bfloat16)
    left_slots = scaled[row_local]
    right_slots = partner[col_local]
    update = jnp.einsum("qrk,qck->qrc", left_slots, right_slots, preferred_element_type=jnp.float32)
    live_slots = (my_rows > 0) & (my_cols > 0)
    current = current + jnp.where(live_slots[:, None, None], update, 0.0)
    return current[None]


class Plan:
    def __init__(self, tri, subs, slots, strip, order, chunks):
        self.tri, self.subs, self.slots, self.strip, self.order = tri, subs, slots, strip, order
        self.chunks = chunks
        self.groups = math.isqrt(tri)
        self.per_group = NB // self.groups
        self.half_group = self.per_group // 2
        self.half_tri = tri // 2
        self.piece = strip // self.half_tri
        self.wide = self.half_group // chunks
        self.in_chunk = 2 * self.wide
        self.o_sub = 0
        self.o_diag = 1
        self.o_slot = 2
        self.o_src = self.o_slot + self.per_group
        self.o_here = self.o_src + self.groups
        self.o_rg = self.o_here + self.groups
        self.o_cg = self.o_rg + self.half_tri
        self.o_hf = self.o_cg + self.half_tri
        self.o_row_chunk = self.o_hf + self.half_tri
        self.o_row_place = self.o_row_chunk + slots
        self.o_col_chunk = self.o_row_place + slots
        self.o_col_place = self.o_col_chunk + slots
        self.o_live = self.o_col_place + slots
        self.o_new = self.o_live + slots
        self.size = self.o_new + slots

    def tiled(self):
        return (
            self.piece % 16 == 0
            and self.order % 128 == 0
            and self.half_group % self.chunks == 0
            and self.groups * self.groups == self.tri
            and self.subs * self.strip == self.order
        )

    def place_of(self, member):
        half, inner = divmod(member, self.half_group)
        chunk, rest = divmod(inner, self.wide)
        return chunk, half * self.wide + rest

    def tile_of(self, chunk, place):
        half, inner = divmod(place, self.wide)
        return half * self.half_group + chunk * self.wide + inner


def table_call(p, cell_owner):
    def kernel(owner, out, cell_of):
        position = lax.axis_index("tri")
        for cell in range(p.tri):
            cell_of[owner[cell]] = cell

        def split(cell):
            down = cell // p.groups
            across = cell - down * p.groups
            return down, across

        down, across = split(cell_of[position])
        row_group = jnp.maximum(down, across)
        col_group = jnp.minimum(down, across)
        diag = down == across
        my_half = position // p.half_tri
        out[p.o_sub] = lax.axis_index("sub")
        out[p.o_diag] = jnp.where(diag, 1, 0)
        for chunk in range(p.chunks):
            for place in range(p.in_chunk):
                member = p.tile_of(chunk, place)
                out[p.o_slot + chunk * p.in_chunk + place] = jnp.where(
                    down > 0, member * p.half_group, member * (member + 1) // 2
                )
        for group in range(p.groups):
            holder = owner[group * p.groups]
            half = holder // p.half_tri
            out[p.o_src + group] = holder - half * p.half_tri
            out[p.o_here + group] = jnp.where(half == my_half, 1, 0)
        for end in range(p.half_tri):
            there_down, there_across = split(cell_of[my_half * p.half_tri + end])
            out[p.o_rg + end] = jnp.maximum(there_down, there_across)
            out[p.o_cg + end] = jnp.minimum(there_down, there_across)
            out[p.o_hf + end] = jnp.where(there_down < there_across, 1, 0)
        col_shift = jnp.where(down < across, p.half_group, 0)
        triangle = [(i, j) for i in range(p.per_group) for j in range(i + 1)]
        for slot in range(p.slots):
            tri_i, tri_j = triangle[slot] if slot < len(triangle) else (0, -1)
            box_i, box_j = divmod(slot, p.half_group)
            if box_i >= p.per_group:
                box_i, box_j = 0, -1
            inner_i = jnp.where(diag, tri_i, box_i)
            inner_j = jnp.where(diag, tri_j, box_j)
            row = row_group * p.per_group + inner_i
            col = col_group * p.per_group + jnp.where(diag, 0, col_shift) + inner_j
            live = (inner_j >= 0) & (row > 0) & (col > 0)
            tri_row, tri_col = p.place_of(tri_i), p.place_of(max(tri_j, 0))
            box_row, box_col = p.place_of(box_i), p.place_of(max(box_j, 0))
            out[p.o_row_chunk + slot] = jnp.where(diag, tri_row[0], box_row[0])
            out[p.o_row_place + slot] = jnp.where(diag, tri_row[1], box_row[1])
            out[p.o_col_chunk + slot] = jnp.where(diag, tri_col[0], box_col[0])
            out[p.o_col_place + slot] = jnp.where(diag, tri_col[1], p.in_chunk + box_col[1])
            out[p.o_live + slot] = jnp.where(live, 1, 0)
            new_tri = 1 if tri_j == 0 else 0
            new_box = 1 if box_j == 0 else 0
            out[p.o_new + slot] = jnp.where(diag, new_tri, new_box)

    return pl.pallas_call(
        kernel,
        out_shape=jax.ShapeDtypeStruct((p.size,), jnp.int32),
        in_specs=[pl.BlockSpec(memory_space=pltpu.SMEM)],
        out_specs=pl.BlockSpec(memory_space=pltpu.SMEM),
        scratch_shapes=[pltpu.SMEM((p.tri,), jnp.int32)],
        name="table",
    )(cell_owner)


IN_VMEM = pl.BlockSpec(memory_space=pltpu.VMEM)


def in_vmem(x):
    return pltpu.with_memory_space_constraint(x, pltpu.VMEM)


def limit(mib):
    return pltpu.CompilerParams(vmem_limit_bytes=mib * 2**20)


def in_hbm(x):
    return pltpu.with_memory_space_constraint(x, pltpu.HBM)


def in_hbm(x):
    return pltpu.with_memory_space_constraint(x, pltpu.HBM)


def extract_call(p, table, current, chunk):
    def kernel(t, tile, out):
        out[...] = tile[...].reshape(p.half_tri, 1, p.piece, p.order).astype(jnp.bfloat16)

    return pl.pallas_call(
        kernel,
        out_shape=jax.ShapeDtypeStruct((p.half_tri, p.in_chunk, p.piece, p.order), jnp.bfloat16),
        grid_spec=pltpu.PrefetchScalarGridSpec(
            num_scalar_prefetch=1,
            grid=(p.in_chunk,),
            in_specs=[
                pl.BlockSpec(
                    (1, p.strip, p.order),
                    lambda i, t: (t[p.o_slot + chunk * p.in_chunk + i], 0, 0),
                )
            ],
            out_specs=pl.BlockSpec(
                (p.half_tri, 1, p.piece, p.order), lambda i, t: (0, i, 0, 0)
            ),
        ),
        compiler_params=limit(8),
        name="extract",
    )(table, in_hbm(current))


def pick_call(p, table, spread):
    def kernel(t, spread_ref, out):
        for g in range(p.groups):
            out[g] = spread_ref[t[p.o_src + g]]

    return pl.pallas_call(
        kernel,
        out_shape=pltpu.VMEM((p.groups,) + spread.shape[1:], jnp.bfloat16),
        grid_spec=pltpu.PrefetchScalarGridSpec(
            num_scalar_prefetch=1, grid=(), in_specs=[IN_VMEM], out_specs=IN_VMEM
        ),
        compiler_params=limit(8),
        name="pick",
    )(table, in_vmem(spread))


def build_call(p, table, near, far, with_pivot):
    rows = p.in_chunk + p.wide + (1 if with_pivot else 0)

    def kernel(t, near_ref, far_ref, out):
        def part(group, first, count, end, place):
            here = t[p.o_here + group] == 1

            @pl.when(here)
            def _():
                out[end, place : place + count] = near_ref[group, pl.ds(first, count)]

            @pl.when(jnp.logical_not(here))
            def _():
                out[end, place : place + count] = far_ref[group, pl.ds(first, count)]

        for end in range(p.half_tri):
            part(t[p.o_rg + end], 0, p.in_chunk, end, 0)
            part(t[p.o_cg + end], t[p.o_hf + end] * p.wide, p.wide, end, p.in_chunk)
            if with_pivot:
                part(0, 0, 1, end, p.in_chunk + p.wide)

    return pl.pallas_call(
        kernel,
        out_shape=pltpu.VMEM((p.half_tri, rows, p.piece, p.order), jnp.bfloat16),
        grid_spec=pltpu.PrefetchScalarGridSpec(
            num_scalar_prefetch=1, grid=(), in_specs=[IN_VMEM, IN_VMEM], out_specs=IN_VMEM
        ),
        compiler_params=limit(8),
        name="build",
    )(table, in_vmem(near), in_vmem(far))


def inverse_call(p, table, arrived):
    place = p.in_chunk + p.wide
    order = p.order

    def kernel(t, *refs):
        sources = refs[: p.subs]
        high, low, pivot, x_wide, x_half, e_ref = refs[p.subs :]
        for shift in range(p.subs):
            strip = lax.rem(t[p.o_sub] + shift, p.subs) * p.strip
            at = pl.multiple_of(strip, p.strip)
            pivot[pl.ds(at, p.strip)] = sources[shift][:, place].reshape(p.strip, order)

        def dot(a, b):
            return lax.dot_general(
                a, b, (((1,), (0,)), ((), ())), preferred_element_type=jnp.float32
            )

        def eye():
            r = lax.broadcasted_iota(jnp.int32, (order, order), 0)
            c = lax.broadcasted_iota(jnp.int32, (order, order), 1)
            return jnp.where(r == c, 1.0, 0.0)

        square = dot(pivot[...], pivot[...])
        bound = jnp.max(jnp.sum(jnp.abs(square), axis=1))
        start = pivot[...].astype(jnp.float32) * (-1.0 / bound)
        x_wide[...] = start
        x_half[...] = start.astype(jnp.bfloat16)

        def coarse_on(carry):
            step, error, noise = carry
            return (step < 40) & (error > 0.01) & (noise < 0.1)

        def coarse(carry):
            step, _, _ = carry
            x = x_half[...]
            residual = eye() - dot(pivot[...], x)
            e_ref[...] = residual.astype(jnp.bfloat16)
            error = jnp.sum(residual * residual)
            new = x.astype(jnp.float32) + dot(x, e_ref[...])
            x_wide[...] = new
            x_half[...] = new.astype(jnp.bfloat16)
            noise = jnp.sum(new * new) * bound * 2.0**-18
            return step + 1, error, noise

        lax.while_loop(coarse_on, coarse, (jnp.int32(0), jnp.float32(1e30), jnp.float32(0.0)))

        def fine_on(carry):
            step, error, before = carry
            stuck = (before < 0.5) & (error > 0.5 * before)
            return (step < 100) & (error > 1e-4) & jnp.logical_not(stuck)

        def fine(carry):
            step, before, _ = carry
            x = x_wide[...]
            x_high = x.astype(jnp.bfloat16)
            x_low = (x - x_high.astype(jnp.float32)).astype(jnp.bfloat16)
            residual = eye() - (dot(pivot[...], x_high) + dot(pivot[...], x_low))
            error = jnp.sum(residual * residual)
            e_high = residual.astype(jnp.bfloat16)
            e_low = (residual - e_high.astype(jnp.float32)).astype(jnp.bfloat16)
            x_wide[...] = x + (dot(x_high, e_high) + (dot(x_high, e_low) + dot(x_low, e_high)))
            return step + 1, error, before

        lax.while_loop(fine_on, fine, (jnp.int32(0), jnp.float32(1e30), jnp.float32(1e30)))
        x = x_wide[...]
        rounded = x.astype(jnp.bfloat16)
        high[...] = rounded
        low[...] = (x - rounded.astype(jnp.float32)).astype(jnp.bfloat16)

    square_shape = pltpu.VMEM((order, order), jnp.bfloat16)
    return pl.pallas_call(
        kernel,
        out_shape=(square_shape, square_shape),
        grid_spec=pltpu.PrefetchScalarGridSpec(
            num_scalar_prefetch=1,
            grid=(),
            in_specs=[IN_VMEM] * p.subs,
            out_specs=(IN_VMEM, IN_VMEM),
            scratch_shapes=[
                pltpu.VMEM((order, order), jnp.bfloat16),
                pltpu.VMEM((order, order), jnp.float32),
                pltpu.VMEM((order, order), jnp.bfloat16),
                pltpu.VMEM((order, order), jnp.bfloat16),
            ],
        ),
        compiler_params=limit(12),
        cost_estimate=pl.CostEstimate(
            flops=60 * 2 * order**3, bytes_accessed=4 * order**2, transcendentals=0
        ),
        name="inverse",
    )(table, *[in_vmem(x) for x in arrived])


def update_call(p, table, current, arrived, inverse):
    per_step = next(n for n in (4, 3, 2, 1) if p.slots % n == 0)

    def kernel(t, tiles, high, low, *refs):
        sources = [refs[k * p.subs : (k + 1) * p.subs] for k in range(p.chunks)]
        out, scaled = refs[p.chunks * p.subs :]
        step = pl.program_id(0)
        sub = t[p.o_sub]

        for u in range(per_step):
            slot = step * per_step + u
            for k in range(p.chunks):

                @pl.when((t[p.o_new + slot] == 1) & (t[p.o_row_chunk + slot] == k))
                def _():
                    strip = sources[k][0][:, t[p.o_row_place + slot]].reshape(p.strip, p.order)
                    dims = (((1,), (0,)), ((), ()))
                    product = lax.dot_general(
                        strip, high[...], dims, preferred_element_type=jnp.float32
                    ) + lax.dot_general(strip, low[...], dims, preferred_element_type=jnp.float32)
                    scaled[...] = product.astype(jnp.bfloat16)

            live = t[p.o_live + slot] == 1
            for k in range(p.chunks):

                @pl.when(live & (t[p.o_col_chunk + slot] == k))
                def _():
                    strips = [
                        sources[k][shift][:, t[p.o_col_place + slot]].reshape(p.strip, p.order)
                        for shift in range(p.subs)
                    ]
                    for place in range(p.subs):
                        strip = strips[0]
                        for shift in range(1, p.subs):
                            here = lax.rem(sub + shift, p.subs) == place
                            strip = jnp.where(here, strips[shift], strip)
                        at = slice(place * p.strip, (place + 1) * p.strip)
                        out[u, :, at] = tiles[u, :, at] + lax.dot_general(
                            scaled[...],
                            strip,
                            (((1,), (1,)), ((), ())),
                            preferred_element_type=jnp.float32,
                        )

            @pl.when(jnp.logical_not(live))
            def _():
                out[u] = tiles[u]

    block = pl.BlockSpec((per_step, p.strip, p.order), lambda i, t: (i, 0, 0))
    return pl.pallas_call(
        kernel,
        out_shape=jax.ShapeDtypeStruct(current.shape, jnp.float32),
        grid_spec=pltpu.PrefetchScalarGridSpec(
            num_scalar_prefetch=1,
            grid=(p.slots // per_step,),
            in_specs=[block] + [IN_VMEM] * (2 + p.chunks * p.subs),
            out_specs=block,
            scratch_shapes=[pltpu.VMEM((p.strip, p.order), jnp.bfloat16)],
        ),
        compiler_params=pltpu.CompilerParams(
            dimension_semantics=("arbitrary",), vmem_limit_bytes=24 * 2**20
        ),
        name="update",
    )(
        table,
        in_hbm(current),
        in_vmem(inverse[0]),
        in_vmem(inverse[1]),
        *[in_vmem(ref) for chunk in arrived for ref in chunk],
    )


def planned(p, stored_tiles, cell_owner):
    table = table_call(p, cell_owner)
    current = stored_tiles[0]
    halves = [list(range(h * p.half_tri, (h + 1) * p.half_tri)) for h in range(2)]
    swap = [(i, (i + p.half_tri) % p.tri) for i in range(p.tri)]

    def exchange(x):
        return lax.all_to_all(
            x, "tri", split_axis=0, concat_axis=0, tiled=True, axis_index_groups=halves
        )

    def arrivals(x):
        return [x] + [
            lax.ppermute(x, "sub", [((i + shift) % p.subs, i) for i in range(p.subs)])
            for shift in range(1, p.subs)
        ]

    near, far, arrived = [], [], []
    for chunk in range(p.chunks):
        pieces = extract_call(p, table, current, chunk)
        spread = exchange(pieces)
        near.append(pick_call(p, table, spread))
    for chunk in range(p.chunks):
        far.append(lax.ppermute(near[chunk], "tri", swap))
    for chunk in range(p.chunks):
        built = build_call(p, table, near[chunk], far[chunk], chunk == 0)
        whole = exchange(built)
        arrived.append(arrivals(whole))
    inverse = inverse_call(p, table, arrived[0])
    return update_call(p, table, current, arrived, inverse)[None]


def shards(stored_tiles, cell_owner):
    p = Plan(
        lax.axis_size("tri"),
        lax.axis_size("sub"),
        stored_tiles.shape[1],
        stored_tiles.shape[2],
        stored_tiles.shape[3],
        2,
    )
    if p.tiled():
        return planned(p, stored_tiles, cell_owner)
    return untiled(stored_tiles, cell_owner)


def solution(mesh):
    placed = (P("tri", None, "sub", None), P())
    return jax.shard_map(
        shards, mesh=mesh, in_specs=placed, out_specs=P("tri", None, "sub", None), check_vma=False
    )
```

```python
import math

import jax
import jax.numpy as jnp
import numpy as np
from jax import lax
from jax.experimental import pallas as pl
from jax.experimental.pallas import tpu as pltpu
from jax.sharding import PartitionSpec as P


NB = 32


def shortened(x):

    def short(part):
        return part.astype(jnp.bfloat16) if part.dtype == jnp.float32 else part

    return jax.tree.map(short, x)


def layout(groups, per_group):
    half_group = per_group // 2
    slot_count = per_group * (per_group + 1) // 2
    row_table = np.full((groups * groups, slot_count), -1, np.int32)
    col_table = np.full((groups * groups, slot_count), -1, np.int32)
    for first_group in range(groups):
        for second_group in range(groups):
            cell_index = first_group * groups + second_group
            for inner_row in range(per_group):
                if first_group == second_group:
                    for inner_column in range(inner_row + 1):
                        slot_index = inner_row * (inner_row + 1) // 2 + inner_column
                        row_table[cell_index, slot_index] = first_group * per_group + inner_row
                        col_table[cell_index, slot_index] = first_group * per_group + inner_column
                else:
                    for inner_column in range(half_group):
                        slot_index = inner_row * half_group + inner_column
                        if first_group > second_group:
                            row_table[cell_index, slot_index] = first_group * per_group + inner_row
                            col_table[cell_index, slot_index] = (
                                second_group * per_group + inner_column
                            )
                        else:
                            row_table[cell_index, slot_index] = second_group * per_group + inner_row
                            col_table[cell_index, slot_index] = (
                                first_group * per_group + half_group + inner_column
                            )
    return (row_table, col_table)


def untiled(stored_tiles, cell_owner):
    tri_count = lax.axis_size("tri")
    groups = math.isqrt(tri_count)
    per_group = NB // groups
    half_group = per_group // 2
    strip_rows = stored_tiles.shape[2]
    block_order = stored_tiles.shape[3]
    row_table, col_table = layout(groups, per_group)
    position = lax.axis_index("tri")
    my_cell = jnp.sum(jnp.where(cell_owner == position, jnp.arange(tri_count, dtype=jnp.int32), 0))
    cell_down = my_cell // groups
    cell_across = my_cell % groups
    row_group = jnp.maximum(cell_down, cell_across)
    col_group = jnp.minimum(cell_down, cell_across)
    my_rows = jnp.asarray(row_table)[my_cell]
    my_cols = jnp.asarray(col_table)[my_cell]
    row_local = jnp.clip(my_rows - row_group * per_group, 0, per_group - 1)
    col_local = jnp.clip(my_cols - col_group * per_group, 0, per_group - 1)
    holders = cell_owner[jnp.arange(groups) * groups]
    highest = lax.Precision.HIGHEST
    current = stored_tiles[0]
    lower_slots = np.array([member * half_group for member in range(per_group)], np.int32)
    first_slots = np.array(
        [member * (member + 1) // 2 if member > 0 else 0 for member in range(per_group)], np.int32
    )
    keep_first = np.array([1.0 if member > 0 else 0.0 for member in range(per_group)], np.float32)
    from_lower = current[lower_slots]
    from_first = current[first_slots] * keep_first[:, None, None]
    holder_part = jnp.where(cell_down > 0, from_lower, from_first)
    holder_part = jnp.where(cell_across == 0, holder_part, 0.0).astype(jnp.bfloat16)
    pivot_slot = 0 // 2
    pivot_part = jnp.where(my_cell == 0, current[pivot_slot], 0.0)
    piece_size = holder_part.size // tri_count
    pivot_piece = pivot_part.size // tri_count
    spread_panel = lax.all_to_all(
        holder_part.reshape(tri_count, piece_size), "tri", split_axis=0, concat_axis=0, tiled=True
    )
    spread_pivot = lax.all_to_all(
        pivot_part.reshape(tri_count, pivot_piece).astype(jnp.bfloat16),
        "tri",
        split_axis=0,
        concat_axis=0,
        tiled=True,
    ).astype(jnp.float32)
    picked_panel = spread_panel[holders][:, None, :]
    picked_pivot = spread_pivot[holders[0]][None, :]
    whole_panel = lax.all_gather(picked_panel, "tri", axis=1, tiled=True)
    whole_pivot = lax.all_gather(
        picked_pivot.astype(jnp.bfloat16), "tri", axis=0, tiled=True
    ).astype(picked_pivot.dtype)
    panels = whole_panel.reshape(groups, per_group, strip_rows, block_order)
    pivot_strip = whole_pivot.reshape(strip_rows, block_order)
    own_strips = panels[row_group]
    other_strips = panels[col_group]
    pivot_block = lax.all_gather(
        pivot_strip.astype(jnp.bfloat16), "sub", axis=0, tiled=True
    ).astype(pivot_strip.dtype)
    partner = lax.all_gather(other_strips, "sub", axis=1, tiled=True)
    gram_matrix = jnp.dot(pivot_block.T, pivot_block, precision=highest)
    factor = jnp.linalg.cholesky(gram_matrix)
    column_count = block_order // lax.axis_size("sub")
    first_column = lax.axis_index("sub") * column_count
    columns = lax.dynamic_slice_in_dim(pivot_block.T, first_column, column_count, 1)
    column_part = jax.scipy.linalg.cho_solve((factor, True), columns)
    inverse = lax.all_gather(shortened(column_part), "sub", axis=1, tiled=True).astype(
        column_part.dtype
    )
    scaled = jnp.einsum(
        "irk,kc->irc", own_strips.astype(jnp.float32), inverse, precision=highest
    ).astype(jnp.bfloat16)
    left_slots = scaled[row_local]
    right_slots = partner[col_local]
    update = jnp.einsum("qrk,qck->qrc", left_slots, right_slots, preferred_element_type=jnp.float32)
    live_slots = (my_rows > 0) & (my_cols > 0)
    current = current + jnp.where(live_slots[:, None, None], update, 0.0)
    return current[None]


class Plan:
    def __init__(self, tri, subs, slots, strip, order, chunks):
        self.tri, self.subs, self.slots, self.strip, self.order = tri, subs, slots, strip, order
        self.chunks = chunks
        self.groups = math.isqrt(tri)
        self.per_group = NB // self.groups
        self.half_group = self.per_group // 2
        self.half_tri = tri // 2
        self.piece = strip // self.half_tri
        self.wide = self.half_group // chunks
        self.in_chunk = 2 * self.wide
        self.o_sub = 0
        self.o_diag = 1
        self.o_me = 2
        self.o_slot = 3
        self.o_src = self.o_slot + self.per_group
        self.o_here = self.o_src + self.groups
        self.o_rg = self.o_here + self.groups
        self.o_cg = self.o_rg + self.half_tri
        self.o_hf = self.o_cg + self.half_tri
        self.o_row_chunk = self.o_hf + self.half_tri
        self.o_row_place = self.o_row_chunk + slots
        self.o_col_chunk = self.o_row_place + slots
        self.o_col_place = self.o_col_chunk + slots
        self.o_live = self.o_col_place + slots
        self.o_new = self.o_live + slots
        self.size = self.o_new + slots

    def tiled(self):
        return (
            self.piece % 16 == 0
            and self.order % 128 == 0
            and self.half_group % self.chunks == 0
            and self.groups * self.groups == self.tri
            and self.half_tri & (self.half_tri - 1) == 0
            and self.subs * self.strip == self.order
        )

    def place_of(self, member):
        half, inner = divmod(member, self.half_group)
        chunk, rest = divmod(inner, self.wide)
        return chunk, half * self.wide + rest

    def tile_of(self, chunk, place):
        half, inner = divmod(place, self.wide)
        return half * self.half_group + chunk * self.wide + inner


def table_call(p, cell_owner):
    def kernel(owner, out, cell_of):
        position = lax.axis_index("tri")
        for cell in range(p.tri):
            cell_of[owner[cell]] = cell

        def split(cell):
            down = cell // p.groups
            across = cell - down * p.groups
            return down, across

        down, across = split(cell_of[position])
        row_group = jnp.maximum(down, across)
        col_group = jnp.minimum(down, across)
        diag = down == across
        my_half = position // p.half_tri
        out[p.o_sub] = lax.axis_index("sub")
        out[p.o_me] = position - my_half * p.half_tri
        out[p.o_diag] = jnp.where(diag, 1, 0)
        for chunk in range(p.chunks):
            for place in range(p.in_chunk):
                member = p.tile_of(chunk, place)
                out[p.o_slot + chunk * p.in_chunk + place] = jnp.where(
                    down > 0, member * p.half_group, member * (member + 1) // 2
                )
        for group in range(p.groups):
            holder = owner[group * p.groups]
            half = holder // p.half_tri
            out[p.o_src + group] = holder - half * p.half_tri
            out[p.o_here + group] = jnp.where(half == my_half, 1, 0)
        for end in range(p.half_tri):
            there_down, there_across = split(cell_of[my_half * p.half_tri + end])
            out[p.o_rg + end] = jnp.maximum(there_down, there_across)
            out[p.o_cg + end] = jnp.minimum(there_down, there_across)
            out[p.o_hf + end] = jnp.where(there_down < there_across, 1, 0)
        col_shift = jnp.where(down < across, p.half_group, 0)
        triangle = [(i, j) for i in range(p.per_group) for j in range(i + 1)]
        for slot in range(p.slots):
            tri_i, tri_j = triangle[slot] if slot < len(triangle) else (0, -1)
            box_i, box_j = divmod(slot, p.half_group)
            if box_i >= p.per_group:
                box_i, box_j = 0, -1
            inner_i = jnp.where(diag, tri_i, box_i)
            inner_j = jnp.where(diag, tri_j, box_j)
            row = row_group * p.per_group + inner_i
            col = col_group * p.per_group + jnp.where(diag, 0, col_shift) + inner_j
            live = (inner_j >= 0) & (row > 0) & (col > 0)
            tri_row, tri_col = p.place_of(tri_i), p.place_of(max(tri_j, 0))
            box_row, box_col = p.place_of(box_i), p.place_of(max(box_j, 0))
            out[p.o_row_chunk + slot] = jnp.where(diag, tri_row[0], box_row[0])
            out[p.o_row_place + slot] = jnp.where(diag, tri_row[1], box_row[1])
            out[p.o_col_chunk + slot] = jnp.where(diag, tri_col[0], box_col[0])
            out[p.o_col_place + slot] = jnp.where(diag, tri_col[1], p.in_chunk + box_col[1])
            out[p.o_live + slot] = jnp.where(live, 1, 0)
            new_tri = 1 if tri_j == 0 else 0
            new_box = 1 if box_j == 0 else 0
            out[p.o_new + slot] = jnp.where(diag, new_tri, new_box)

    return pl.pallas_call(
        kernel,
        out_shape=jax.ShapeDtypeStruct((p.size,), jnp.int32),
        in_specs=[pl.BlockSpec(memory_space=pltpu.SMEM)],
        out_specs=pl.BlockSpec(memory_space=pltpu.SMEM),
        scratch_shapes=[pltpu.SMEM((p.tri,), jnp.int32)],
        name="table",
    )(cell_owner)


IN_VMEM = pl.BlockSpec(memory_space=pltpu.VMEM)


def in_vmem(x):
    return pltpu.with_memory_space_constraint(x, pltpu.VMEM)


def limit(mib):
    return pltpu.CompilerParams(vmem_limit_bytes=mib * 2**20)


def in_hbm(x):
    return pltpu.with_memory_space_constraint(x, pltpu.HBM)


def in_hbm(x):
    return pltpu.with_memory_space_constraint(x, pltpu.HBM)


def mark_call(p, table):
    def kernel(t, out):
        def copy(i, _):
            out[i] = t[i]
            return 0

        lax.fori_loop(0, p.size, copy, 0)

    smem = pl.BlockSpec(memory_space=pltpu.SMEM)
    return pl.pallas_call(
        kernel,
        out_shape=jax.ShapeDtypeStruct((p.size,), jnp.int32),
        in_specs=[smem],
        out_specs=smem,
        compiler_params=limit(1),
        name="mark",
    )(table)


def extract_call(p, table, current, chunk):
    def kernel(t, tile, out):
        out[...] = tile[...].reshape(p.half_tri, 1, p.piece, p.order).astype(jnp.bfloat16)

    return pl.pallas_call(
        kernel,
        out_shape=jax.ShapeDtypeStruct((p.half_tri, p.in_chunk, p.piece, p.order), jnp.bfloat16),
        grid_spec=pltpu.PrefetchScalarGridSpec(
            num_scalar_prefetch=1,
            grid=(p.in_chunk,),
            in_specs=[
                pl.BlockSpec(
                    (1, p.strip, p.order),
                    lambda i, t: (t[p.o_slot + chunk * p.in_chunk + i], 0, 0),
                )
            ],
            out_specs=pl.BlockSpec(
                (p.half_tri, 1, p.piece, p.order), lambda i, t: (0, i, 0, 0)
            ),
        ),
        compiler_params=limit(8),
        name="extract",
    )(table, in_hbm(current))


def pick_call(p, table, spread):
    def kernel(t, spread_ref, out):
        for g in range(p.groups):
            out[g] = spread_ref[t[p.o_src + g]]

    return pl.pallas_call(
        kernel,
        out_shape=pltpu.VMEM((p.groups,) + spread.shape[1:], jnp.bfloat16),
        grid_spec=pltpu.PrefetchScalarGridSpec(
            num_scalar_prefetch=1, grid=(), in_specs=[IN_VMEM], out_specs=IN_VMEM
        ),
        compiler_params=limit(8),
        name="pick",
    )(table, in_vmem(spread))


def build_call(p, table, near, far, with_pivot, apart):
    rows = p.in_chunk + p.wide + (1 if with_pivot else 0)

    def kernel(t, near_ref, far_ref, *outs):
        def part(group, first, count, n, place):
            here = t[p.o_here + group] == 1
            at = pl.ds(place, count)

            def store(value):
                if apart:
                    outs[n][at] = value
                else:
                    outs[0][n, at] = value

            @pl.when(here)
            def _():
                store(near_ref[group, pl.ds(first, count)])

            @pl.when(jnp.logical_not(here))
            def _():
                store(far_ref[group, pl.ds(first, count)])

        for n in range(p.half_tri):
            end = t[p.o_me] ^ n if apart else n
            part(t[p.o_rg + end], 0, p.in_chunk, n, 0)
            part(t[p.o_cg + end], t[p.o_hf + end] * p.wide, p.wide, n, p.in_chunk)
            if with_pivot:
                part(0, 0, 1, n, p.in_chunk + p.wide)

    one = (rows, p.piece, p.order)
    if apart:
        out_shape = [pltpu.VMEM(one, jnp.bfloat16)] * p.half_tri
    else:
        out_shape = [pltpu.VMEM((p.half_tri,) + one, jnp.bfloat16)]
    outs = pl.pallas_call(
        kernel,
        out_shape=out_shape,
        grid_spec=pltpu.PrefetchScalarGridSpec(
            num_scalar_prefetch=1,
            grid=(),
            in_specs=[IN_VMEM, IN_VMEM],
            out_specs=[IN_VMEM] * len(out_shape),
        ),
        compiler_params=limit(8),
        name="build",
    )(table, in_vmem(near), in_vmem(far))
    return outs if apart else outs[0]


def inverse_call(p, table, arrived, current):
    loads = next(n for n in (6, 5, 4, 3, 2, 1) if p.slots % n == 0)
    each = p.slots // loads
    place = p.in_chunk + p.wide
    order = p.order

    def kernel(t, *refs):
        sources = refs[: p.subs]
        tiles, high, low, held, pivot, x_wide, x_half, e_ref, sems = refs[p.subs :]
        copies = [
            pltpu.make_async_copy(
                tiles.at[pl.ds(n * each, each)], held.at[pl.ds(n * each, each)], sems.at[n]
            )
            for n in range(loads)
        ]
        for copy in copies:
            copy.start()
        for shift in range(p.subs):
            strip = lax.rem(t[p.o_sub] + shift, p.subs) * p.strip
            at = pl.multiple_of(strip, p.strip)
            pivot[pl.ds(at, p.strip)] = sources[shift][:, place].reshape(p.strip, order)

        def dot(a, b):
            return lax.dot_general(
                a, b, (((1,), (0,)), ((), ())), preferred_element_type=jnp.float32
            )

        def eye():
            r = lax.broadcasted_iota(jnp.int32, (order, order), 0)
            c = lax.broadcasted_iota(jnp.int32, (order, order), 1)
            return jnp.where(r == c, 1.0, 0.0)

        square = dot(pivot[...], pivot[...])
        bound = jnp.max(jnp.sum(jnp.abs(square), axis=1))
        start = pivot[...].astype(jnp.float32) * (-1.0 / bound)
        x_wide[...] = start
        x_half[...] = start.astype(jnp.bfloat16)

        def coarse_on(carry):
            step, error, noise = carry
            return (step < 40) & (error > 0.01) & (noise < 0.1)

        def coarse(carry):
            step, _, _ = carry
            x = x_half[...]
            residual = eye() - dot(pivot[...], x)
            e_ref[...] = residual.astype(jnp.bfloat16)
            error = jnp.sum(residual * residual)
            new = x.astype(jnp.float32) + dot(x, e_ref[...])
            x_wide[...] = new
            x_half[...] = new.astype(jnp.bfloat16)
            noise = jnp.sum(new * new) * bound * 2.0**-18
            return step + 1, error, noise

        lax.while_loop(coarse_on, coarse, (jnp.int32(0), jnp.float32(1e30), jnp.float32(0.0)))

        def fine_on(carry):
            step, error, before = carry
            stuck = (before < 0.5) & (error > 0.5 * before)
            return (step < 100) & (error > 1e-4) & jnp.logical_not(stuck)

        def fine(carry):
            step, before, _ = carry
            x = x_wide[...]
            x_high = x.astype(jnp.bfloat16)
            x_low = (x - x_high.astype(jnp.float32)).astype(jnp.bfloat16)
            residual = eye() - (dot(pivot[...], x_high) + dot(pivot[...], x_low))
            error = jnp.sum(residual * residual)
            e_high = residual.astype(jnp.bfloat16)
            e_low = (residual - e_high.astype(jnp.float32)).astype(jnp.bfloat16)
            x_wide[...] = x + (dot(x_high, e_high) + (dot(x_high, e_low) + dot(x_low, e_high)))
            return step + 1, error, before

        lax.while_loop(fine_on, fine, (jnp.int32(0), jnp.float32(1e30), jnp.float32(1e30)))
        x = x_wide[...]
        rounded = x.astype(jnp.bfloat16)
        high[...] = rounded
        low[...] = (x - rounded.astype(jnp.float32)).astype(jnp.bfloat16)
        for copy in copies:
            copy.wait()

    square_shape = pltpu.VMEM((order, order), jnp.bfloat16)
    return pl.pallas_call(
        kernel,
        out_shape=(square_shape, square_shape, pltpu.VMEM(current.shape, jnp.float32)),
        grid_spec=pltpu.PrefetchScalarGridSpec(
            num_scalar_prefetch=1,
            grid=(),
            in_specs=[IN_VMEM] * p.subs + [pl.BlockSpec(memory_space=pltpu.HBM)],
            out_specs=(IN_VMEM, IN_VMEM, IN_VMEM),
            scratch_shapes=[
                pltpu.VMEM((order, order), jnp.bfloat16),
                pltpu.VMEM((order, order), jnp.float32),
                pltpu.VMEM((order, order), jnp.bfloat16),
                pltpu.VMEM((order, order), jnp.bfloat16),
                pltpu.SemaphoreType.DMA((loads,)),
            ],
        ),
        compiler_params=limit(12),
        cost_estimate=pl.CostEstimate(
            flops=60 * 2 * order**3, bytes_accessed=4 * order**2, transcendentals=0
        ),
        name="inverse",
    )(table, *[in_vmem(x) for x in arrived], in_hbm(current))


def update_call(p, table, held, together, apart, inverse):
    per_step = next(n for n in (4, 3, 2, 1) if p.slots % n == 0)
    last = p.chunks - 1
    n_together = last * p.subs
    n_apart = p.subs * p.half_tri

    def kernel(t, tiles, high, low, *refs):
        sources = [refs[k * p.subs : (k + 1) * p.subs] for k in range(last)]
        loose = refs[n_together : n_together + n_apart]
        out, scaled, packed = refs[n_together + n_apart :]
        sources.append([packed.at[shift] for shift in range(p.subs)])
        step = pl.program_id(0)
        sub = t[p.o_sub]

        @pl.when(step == 0)
        def _():
            for shift in range(p.subs):
                for n in range(p.half_tri):
                    packed[shift, t[p.o_me] ^ n] = loose[shift * p.half_tri + n][...]

        for u in range(per_step):
            slot = step * per_step + u
            for k in range(p.chunks):

                @pl.when((t[p.o_new + slot] == 1) & (t[p.o_row_chunk + slot] == k))
                def _():
                    strip = sources[k][0][:, t[p.o_row_place + slot]].reshape(p.strip, p.order)
                    dims = (((1,), (0,)), ((), ()))
                    product = lax.dot_general(
                        strip, high[...], dims, preferred_element_type=jnp.float32
                    ) + lax.dot_general(strip, low[...], dims, preferred_element_type=jnp.float32)
                    scaled[...] = product.astype(jnp.bfloat16)

            live = t[p.o_live + slot] == 1
            for k in range(p.chunks):

                @pl.when(live & (t[p.o_col_chunk + slot] == k))
                def _():
                    strips = [
                        sources[k][shift][:, t[p.o_col_place + slot]].reshape(p.strip, p.order)
                        for shift in range(p.subs)
                    ]
                    for place in range(p.subs):
                        strip = strips[0]
                        for shift in range(1, p.subs):
                            here = lax.rem(sub + shift, p.subs) == place
                            strip = jnp.where(here, strips[shift], strip)
                        at = slice(place * p.strip, (place + 1) * p.strip)
                        out[u, :, at] = tiles[slot, :, at] + lax.dot_general(
                            scaled[...],
                            strip,
                            (((1,), (1,)), ((), ())),
                            preferred_element_type=jnp.float32,
                        )

            @pl.when(jnp.logical_not(live))
            def _():
                out[u] = tiles[slot]

    loose = [in_vmem(ref) for shift in apart for ref in shift]
    return pl.pallas_call(
        kernel,
        out_shape=jax.ShapeDtypeStruct(held.shape, jnp.float32),
        grid_spec=pltpu.PrefetchScalarGridSpec(
            num_scalar_prefetch=1,
            grid=(p.slots // per_step,),
            in_specs=[IN_VMEM] * (3 + n_together + n_apart),
            out_specs=pl.BlockSpec((per_step, p.strip, p.order), lambda i, t: (i, 0, 0)),
            scratch_shapes=[
                pltpu.VMEM((p.strip, p.order), jnp.bfloat16),
                pltpu.VMEM((p.subs, p.half_tri) + loose[0].shape, jnp.bfloat16),
            ],
        ),
        compiler_params=pltpu.CompilerParams(
            dimension_semantics=("arbitrary",), vmem_limit_bytes=16 * 2**20
        ),
        name="update",
    )(
        table,
        in_vmem(held),
        in_vmem(inverse[0]),
        in_vmem(inverse[1]),
        *[in_vmem(ref) for chunk in together for ref in chunk],
        *loose,
    )


def planned(p, stored_tiles, cell_owner):
    table = table_call(p, cell_owner)
    current = stored_tiles[0]
    halves = [list(range(h * p.half_tri, (h + 1) * p.half_tri)) for h in range(2)]
    swap = [(i, (i + p.half_tri) % p.tri) for i in range(p.tri)]

    def exchange(x):
        return lax.all_to_all(
            x, "tri", split_axis=0, concat_axis=0, tiled=True, axis_index_groups=halves
        )

    def arrivals(x):
        return [x] + [
            lax.ppermute(x, "sub", [((i + shift) % p.subs, i) for i in range(p.subs)])
            for shift in range(1, p.subs)
        ]

    near, far, arrived = [], [], []
    for chunk in range(p.chunks):
        pieces = extract_call(p, table, current, chunk)
        spread = exchange(pieces)
        near.append(pick_call(p, table, spread))
    for chunk in range(p.chunks):
        far.append(lax.ppermute(near[chunk], "tri", swap))
    last = p.chunks - 1
    for chunk in range(last):
        built = build_call(p, table, near[chunk], far[chunk], chunk == 0, False)
        whole = exchange(built)
        arrived.append(arrivals(whole))
    built = build_call(p, table, near[last], far[last], last == 0, True)
    loose = [built[0]]
    for n in range(1, p.half_tri):
        pairs = [(i, i ^ n) for i in range(p.tri)]
        loose.append(lax.ppermute(built[n], "tri", pairs))
    pieces = [arrivals(x) for x in loose]
    apart = [[piece[shift] for piece in pieces] for shift in range(p.subs)]
    marked = mark_call(p, table)
    high, low, held = inverse_call(p, marked, arrived[0], current)
    return update_call(p, table, held, arrived, apart, (high, low))[None]


def shards(stored_tiles, cell_owner):
    p = Plan(
        lax.axis_size("tri"),
        lax.axis_size("sub"),
        stored_tiles.shape[1],
        stored_tiles.shape[2],
        stored_tiles.shape[3],
        2,
    )
    if p.tiled():
        return planned(p, stored_tiles, cell_owner)
    return untiled(stored_tiles, cell_owner)


def solution(mesh):
    placed = (P("tri", None, "sub", None), P())
    return jax.shard_map(
        shards, mesh=mesh, in_specs=placed, out_specs=P("tri", None, "sub", None), check_vma=False
    )
```

```python
import math

import jax
import jax.numpy as jnp
import numpy as np
from jax import lax
from jax.experimental import pallas as pl
from jax.experimental.pallas import tpu as pltpu
from jax.sharding import PartitionSpec as P


NB = 32


def shortened(x):

    def short(part):
        return part.astype(jnp.bfloat16) if part.dtype == jnp.float32 else part

    return jax.tree.map(short, x)


def layout(groups, per_group):
    half_group = per_group // 2
    slot_count = per_group * (per_group + 1) // 2
    row_table = np.full((groups * groups, slot_count), -1, np.int32)
    col_table = np.full((groups * groups, slot_count), -1, np.int32)
    for first_group in range(groups):
        for second_group in range(groups):
            cell_index = first_group * groups + second_group
            for inner_row in range(per_group):
                if first_group == second_group:
                    for inner_column in range(inner_row + 1):
                        slot_index = inner_row * (inner_row + 1) // 2 + inner_column
                        row_table[cell_index, slot_index] = first_group * per_group + inner_row
                        col_table[cell_index, slot_index] = first_group * per_group + inner_column
                else:
                    for inner_column in range(half_group):
                        slot_index = inner_row * half_group + inner_column
                        if first_group > second_group:
                            row_table[cell_index, slot_index] = first_group * per_group + inner_row
                            col_table[cell_index, slot_index] = (
                                second_group * per_group + inner_column
                            )
                        else:
                            row_table[cell_index, slot_index] = second_group * per_group + inner_row
                            col_table[cell_index, slot_index] = (
                                first_group * per_group + half_group + inner_column
                            )
    return (row_table, col_table)


def untiled(stored_tiles, cell_owner):
    tri_count = lax.axis_size("tri")
    groups = math.isqrt(tri_count)
    per_group = NB // groups
    half_group = per_group // 2
    strip_rows = stored_tiles.shape[2]
    block_order = stored_tiles.shape[3]
    row_table, col_table = layout(groups, per_group)
    position = lax.axis_index("tri")
    my_cell = jnp.sum(jnp.where(cell_owner == position, jnp.arange(tri_count, dtype=jnp.int32), 0))
    cell_down = my_cell // groups
    cell_across = my_cell % groups
    row_group = jnp.maximum(cell_down, cell_across)
    col_group = jnp.minimum(cell_down, cell_across)
    my_rows = jnp.asarray(row_table)[my_cell]
    my_cols = jnp.asarray(col_table)[my_cell]
    row_local = jnp.clip(my_rows - row_group * per_group, 0, per_group - 1)
    col_local = jnp.clip(my_cols - col_group * per_group, 0, per_group - 1)
    holders = cell_owner[jnp.arange(groups) * groups]
    highest = lax.Precision.HIGHEST
    current = stored_tiles[0]
    lower_slots = np.array([member * half_group for member in range(per_group)], np.int32)
    first_slots = np.array(
        [member * (member + 1) // 2 if member > 0 else 0 for member in range(per_group)], np.int32
    )
    keep_first = np.array([1.0 if member > 0 else 0.0 for member in range(per_group)], np.float32)
    from_lower = current[lower_slots]
    from_first = current[first_slots] * keep_first[:, None, None]
    holder_part = jnp.where(cell_down > 0, from_lower, from_first)
    holder_part = jnp.where(cell_across == 0, holder_part, 0.0).astype(jnp.bfloat16)
    pivot_slot = 0 // 2
    pivot_part = jnp.where(my_cell == 0, current[pivot_slot], 0.0)
    piece_size = holder_part.size // tri_count
    pivot_piece = pivot_part.size // tri_count
    spread_panel = lax.all_to_all(
        holder_part.reshape(tri_count, piece_size), "tri", split_axis=0, concat_axis=0, tiled=True
    )
    spread_pivot = lax.all_to_all(
        pivot_part.reshape(tri_count, pivot_piece).astype(jnp.bfloat16),
        "tri",
        split_axis=0,
        concat_axis=0,
        tiled=True,
    ).astype(jnp.float32)
    picked_panel = spread_panel[holders][:, None, :]
    picked_pivot = spread_pivot[holders[0]][None, :]
    whole_panel = lax.all_gather(picked_panel, "tri", axis=1, tiled=True)
    whole_pivot = lax.all_gather(
        picked_pivot.astype(jnp.bfloat16), "tri", axis=0, tiled=True
    ).astype(picked_pivot.dtype)
    panels = whole_panel.reshape(groups, per_group, strip_rows, block_order)
    pivot_strip = whole_pivot.reshape(strip_rows, block_order)
    own_strips = panels[row_group]
    other_strips = panels[col_group]
    pivot_block = lax.all_gather(
        pivot_strip.astype(jnp.bfloat16), "sub", axis=0, tiled=True
    ).astype(pivot_strip.dtype)
    partner = lax.all_gather(other_strips, "sub", axis=1, tiled=True)
    gram_matrix = jnp.dot(pivot_block.T, pivot_block, precision=highest)
    factor = jnp.linalg.cholesky(gram_matrix)
    column_count = block_order // lax.axis_size("sub")
    first_column = lax.axis_index("sub") * column_count
    columns = lax.dynamic_slice_in_dim(pivot_block.T, first_column, column_count, 1)
    column_part = jax.scipy.linalg.cho_solve((factor, True), columns)
    inverse = lax.all_gather(shortened(column_part), "sub", axis=1, tiled=True).astype(
        column_part.dtype
    )
    scaled = jnp.einsum(
        "irk,kc->irc", own_strips.astype(jnp.float32), inverse, precision=highest
    ).astype(jnp.bfloat16)
    left_slots = scaled[row_local]
    right_slots = partner[col_local]
    update = jnp.einsum("qrk,qck->qrc", left_slots, right_slots, preferred_element_type=jnp.float32)
    live_slots = (my_rows > 0) & (my_cols > 0)
    current = current + jnp.where(live_slots[:, None, None], update, 0.0)
    return current[None]


class Plan:
    def __init__(self, tri, subs, slots, strip, order, chunks):
        self.tri, self.subs, self.slots, self.strip, self.order = tri, subs, slots, strip, order
        self.chunks = chunks
        self.groups = math.isqrt(tri)
        self.per_group = NB // self.groups
        self.half_group = self.per_group // 2
        self.half_tri = tri // 2
        self.piece = strip // self.half_tri
        self.wide = self.half_group // chunks
        self.in_chunk = 2 * self.wide
        self.o_sub = 0
        self.o_diag = 1
        self.o_me = 2
        self.o_src = 8
        self.o_here = self.o_src + self.groups
        self.o_rg = self.o_here + self.groups
        self.o_cg = self.o_rg + self.half_tri
        self.o_hf = self.o_cg + self.half_tri
        self.o_row_chunk = self.o_hf + self.half_tri
        self.o_row_place = self.o_row_chunk + slots
        self.o_col_chunk = self.o_row_place + slots
        self.o_col_place = self.o_col_chunk + slots
        self.o_live = self.o_col_place + slots
        self.o_new = self.o_live + slots
        self.size = self.o_new + slots

    def tiled(self):
        return (
            self.piece % 16 == 0
            and self.order % 128 == 0
            and self.half_group % self.chunks == 0
            and self.groups * self.groups == self.tri
            and self.half_tri & (self.half_tri - 1) == 0
            and self.subs * self.strip == self.order
        )

    def place_of(self, member):
        half, inner = divmod(member, self.half_group)
        chunk, rest = divmod(inner, self.wide)
        return chunk, half * self.wide + rest

    def tile_of(self, chunk, place):
        half, inner = divmod(place, self.wide)
        return half * self.half_group + chunk * self.wide + inner


def table_call(p, cell_owner):
    def kernel(owner, out, cell_of):
        position = lax.axis_index("tri")
        for cell in range(p.tri):
            cell_of[owner[cell]] = cell

        def split(cell):
            down = cell // p.groups
            across = cell - down * p.groups
            return down, across

        down, across = split(cell_of[position])
        row_group = jnp.maximum(down, across)
        col_group = jnp.minimum(down, across)
        diag = down == across
        my_half = position // p.half_tri
        out[p.o_sub] = lax.axis_index("sub")
        out[p.o_me] = position - my_half * p.half_tri
        out[p.o_diag] = jnp.where(diag, 1, 0)
        for group in range(p.groups):
            holder = owner[group * p.groups]
            half = holder // p.half_tri
            out[p.o_src + group] = holder - half * p.half_tri
            out[p.o_here + group] = jnp.where(half == my_half, 1, 0)
        for end in range(p.half_tri):
            there_down, there_across = split(cell_of[my_half * p.half_tri + end])
            out[p.o_rg + end] = jnp.maximum(there_down, there_across)
            out[p.o_cg + end] = jnp.minimum(there_down, there_across)
            out[p.o_hf + end] = jnp.where(there_down < there_across, 1, 0)
        col_shift = jnp.where(down < across, p.half_group, 0)
        triangle = [(i, j) for i in range(p.per_group) for j in range(i + 1)]
        for slot in range(p.slots):
            tri_i, tri_j = triangle[slot] if slot < len(triangle) else (0, -1)
            box_i, box_j = divmod(slot, p.half_group)
            if box_i >= p.per_group:
                box_i, box_j = 0, -1
            inner_i = jnp.where(diag, tri_i, box_i)
            inner_j = jnp.where(diag, tri_j, box_j)
            row = row_group * p.per_group + inner_i
            col = col_group * p.per_group + jnp.where(diag, 0, col_shift) + inner_j
            live = (inner_j >= 0) & (row > 0) & (col > 0)
            tri_row, tri_col = p.place_of(tri_i), p.place_of(max(tri_j, 0))
            box_row, box_col = p.place_of(box_i), p.place_of(max(box_j, 0))
            out[p.o_row_chunk + slot] = jnp.where(diag, tri_row[0], box_row[0])
            out[p.o_row_place + slot] = jnp.where(diag, tri_row[1], box_row[1])
            out[p.o_col_chunk + slot] = jnp.where(diag, tri_col[0], box_col[0])
            out[p.o_col_place + slot] = jnp.where(diag, tri_col[1], p.in_chunk + box_col[1])
            out[p.o_live + slot] = jnp.where(live, 1, 0)
            new_tri = 1 if tri_j == 0 else 0
            new_box = 1 if box_j == 0 else 0
            out[p.o_new + slot] = jnp.where(diag, new_tri, new_box)

    return pl.pallas_call(
        kernel,
        out_shape=jax.ShapeDtypeStruct((p.size,), jnp.int32),
        in_specs=[pl.BlockSpec(memory_space=pltpu.SMEM)],
        out_specs=pl.BlockSpec(memory_space=pltpu.SMEM),
        scratch_shapes=[pltpu.SMEM((p.tri,), jnp.int32)],
        name="table",
    )(cell_owner)


IN_VMEM = pl.BlockSpec(memory_space=pltpu.VMEM)


def in_vmem(x):
    return pltpu.with_memory_space_constraint(x, pltpu.VMEM)


def limit(mib):
    return pltpu.CompilerParams(vmem_limit_bytes=mib * 2**20)


def in_hbm(x):
    return pltpu.with_memory_space_constraint(x, pltpu.HBM)


def in_hbm(x):
    return pltpu.with_memory_space_constraint(x, pltpu.HBM)


def mark_call(p, table):
    def kernel(t, out):
        for i in (p.o_sub, p.o_diag, p.o_me):
            out[i] = t[i]

    smem = pl.BlockSpec(memory_space=pltpu.SMEM)
    return pl.pallas_call(
        kernel,
        out_shape=jax.ShapeDtypeStruct((p.o_src,), jnp.int32),
        in_specs=[smem],
        out_specs=smem,
        compiler_params=limit(1),
        name="mark",
    )(table)


def extract_call(p, cell_owner, current, chunk):
    def kernel(owner, tiles, out, wide, sems):
        position = lax.axis_index("tri")
        cell = jnp.int32(0)
        for n in range(1, p.tri):
            cell = jnp.where(owner[n] == position, n, cell)
        down = cell // p.groups
        copies = []
        for place in range(p.in_chunk):
            member = p.tile_of(chunk, place)
            slot = jnp.where(down > 0, member * p.half_group, member * (member + 1) // 2)
            copies.append(
                pltpu.make_async_copy(tiles.at[slot], wide.at[place], sems.at[place])
            )
        for copy in copies:
            copy.start()
        for place, copy in enumerate(copies):
            copy.wait()
            rounded = wide[place].astype(jnp.bfloat16)
            out[:, place] = rounded.reshape(p.half_tri, p.piece, p.order)

    return pl.pallas_call(
        kernel,
        out_shape=pltpu.VMEM((p.half_tri, p.in_chunk, p.piece, p.order), jnp.bfloat16),
        in_specs=[
            pl.BlockSpec(memory_space=pltpu.SMEM),
            pl.BlockSpec(memory_space=pltpu.HBM),
        ],
        out_specs=IN_VMEM,
        scratch_shapes=[
            pltpu.VMEM((p.in_chunk, p.strip, p.order), jnp.float32),
            pltpu.SemaphoreType.DMA((p.in_chunk,)),
        ],
        compiler_params=limit(8),
        name="extract",
    )(cell_owner, in_hbm(current))


def pick_call(p, table, spread):
    def kernel(t, spread_ref, out):
        for g in range(p.groups):
            out[g] = spread_ref[t[p.o_src + g]]

    return pl.pallas_call(
        kernel,
        out_shape=pltpu.VMEM((p.groups,) + spread.shape[1:], jnp.bfloat16),
        grid_spec=pltpu.PrefetchScalarGridSpec(
            num_scalar_prefetch=1, grid=(), in_specs=[IN_VMEM], out_specs=IN_VMEM
        ),
        compiler_params=limit(8),
        name="pick",
    )(table, in_vmem(spread))


def build_call(p, table, near, far, with_pivot, apart):
    rows = p.in_chunk + p.wide + (1 if with_pivot else 0)

    def kernel(t, near_ref, far_ref, *outs):
        def part(group, first, count, n, place):
            here = t[p.o_here + group] == 1
            at = pl.ds(place, count)

            def store(value):
                if apart:
                    outs[n][at] = value
                else:
                    outs[0][n, at] = value

            @pl.when(here)
            def _():
                store(near_ref[group, pl.ds(first, count)])

            @pl.when(jnp.logical_not(here))
            def _():
                store(far_ref[group, pl.ds(first, count)])

        for n in range(p.half_tri):
            end = t[p.o_me] ^ n if apart else n
            part(t[p.o_rg + end], 0, p.in_chunk, n, 0)
            part(t[p.o_cg + end], t[p.o_hf + end] * p.wide, p.wide, n, p.in_chunk)
            if with_pivot:
                part(0, 0, 1, n, p.in_chunk + p.wide)

    one = (rows, p.piece, p.order)
    if apart:
        out_shape = [pltpu.VMEM(one, jnp.bfloat16)] * p.half_tri
    else:
        out_shape = [pltpu.VMEM((p.half_tri,) + one, jnp.bfloat16)]
    outs = pl.pallas_call(
        kernel,
        out_shape=out_shape,
        grid_spec=pltpu.PrefetchScalarGridSpec(
            num_scalar_prefetch=1,
            grid=(),
            in_specs=[IN_VMEM, IN_VMEM],
            out_specs=[IN_VMEM] * len(out_shape),
        ),
        compiler_params=limit(8),
        name="build",
    )(table, in_vmem(near), in_vmem(far))
    return outs if apart else outs[0]


def inverse_call(p, table, arrived, current):
    loads = next(n for n in (6, 5, 4, 3, 2, 1) if p.slots % n == 0)
    each = p.slots // loads
    place = p.in_chunk + p.wide
    order = p.order

    def kernel(t, *refs):
        sources = refs[: p.subs]
        tiles, high, held, pivot, x_wide, x_half, e_ref, sems = refs[p.subs :]
        copies = [
            pltpu.make_async_copy(
                tiles.at[pl.ds(n * each, each)], held.at[pl.ds(n * each, each)], sems.at[n]
            )
            for n in range(loads)
        ]
        for copy in copies:
            copy.start()
        for shift in range(p.subs):
            strip = lax.rem(t[p.o_sub] + shift, p.subs) * p.strip
            at = pl.multiple_of(strip, p.strip)
            pivot[pl.ds(at, p.strip)] = sources[shift][:, place].reshape(p.strip, order)

        def dot(a, b):
            return lax.dot_general(
                a, b, (((1,), (0,)), ((), ())), preferred_element_type=jnp.float32
            )

        def eye():
            r = lax.broadcasted_iota(jnp.int32, (order, order), 0)
            c = lax.broadcasted_iota(jnp.int32, (order, order), 1)
            return jnp.where(r == c, 1.0, 0.0)

        square = -dot(pivot[...], pivot[...])
        factor = 1.9 / jnp.max(jnp.sum(jnp.abs(square), axis=1))
        residual = eye() - factor * square
        e_ref[...] = residual.astype(jnp.bfloat16)
        wide = -factor * (pivot[...].astype(jnp.float32) + dot(pivot[...], e_ref[...]))
        x_wide[...] = wide
        x_half[...] = wide.astype(jnp.bfloat16)

        def coarse_on(carry):
            step, error, before, noise = carry
            stuck = (before < 1.0) & (error > 0.5 * before)
            return (step < 60) & (error > 3e-3) & (noise < 0.1) & jnp.logical_not(stuck)

        def coarse(carry):
            step, before, _, _ = carry
            x = x_half[...]
            residual = eye() - dot(pivot[...], x)
            e_ref[...] = residual.astype(jnp.bfloat16)
            error = jnp.sum(residual * residual)
            new = x.astype(jnp.float32) + dot(x, e_ref[...])
            x_wide[...] = new
            x_half[...] = new.astype(jnp.bfloat16)
            noise = jnp.sum(new * new) / factor * 2.0**-18
            return step + 1, error, before, noise

        big = jnp.float32(1e30)
        _, reached, _, _ = lax.while_loop(
            coarse_on, coarse, (jnp.int32(0), big, big, jnp.float32(0.0))
        )

        def fine_on(carry):
            step, error, before = carry
            stuck = (before < 0.5) & (error > 0.5 * before)
            return (step < 100) & (error > 1e-4) & jnp.logical_not(stuck)

        def fine(carry):
            step, before, _ = carry
            x = x_wide[...]
            x_high = x.astype(jnp.bfloat16)
            x_low = (x - x_high.astype(jnp.float32)).astype(jnp.bfloat16)
            residual = eye() - (dot(pivot[...], x_high) + dot(pivot[...], x_low))
            error = jnp.sum(residual * residual)
            e_high = residual.astype(jnp.bfloat16)
            e_low = (residual - e_high.astype(jnp.float32)).astype(jnp.bfloat16)
            x_wide[...] = x + (dot(x_high, e_high) + (dot(x_high, e_low) + dot(x_low, e_high)))
            return step + 1, error, before

        @pl.when(jnp.logical_not(reached <= 3e-3))
        def _():
            lax.while_loop(fine_on, fine, (jnp.int32(0), big, big))

        high[...] = x_wide[...].astype(jnp.bfloat16)
        for copy in copies:
            copy.wait()

    square_shape = pltpu.VMEM((order, order), jnp.bfloat16)
    return pl.pallas_call(
        kernel,
        out_shape=(square_shape, pltpu.VMEM(current.shape, jnp.float32)),
        grid_spec=pltpu.PrefetchScalarGridSpec(
            num_scalar_prefetch=1,
            grid=(),
            in_specs=[IN_VMEM] * p.subs + [pl.BlockSpec(memory_space=pltpu.HBM)],
            out_specs=(IN_VMEM, IN_VMEM),
            scratch_shapes=[
                pltpu.VMEM((order, order), jnp.bfloat16),
                pltpu.VMEM((order, order), jnp.float32),
                pltpu.VMEM((order, order), jnp.bfloat16),
                pltpu.VMEM((order, order), jnp.bfloat16),
                pltpu.SemaphoreType.DMA((loads,)),
            ],
        ),
        compiler_params=limit(12),
        cost_estimate=pl.CostEstimate(
            flops=60 * 2 * order**3, bytes_accessed=4 * order**2, transcendentals=0
        ),
        name="inverse",
    )(table, *[in_vmem(x) for x in arrived], in_hbm(current))


def update_call(p, table, held, together, apart, inverse):
    per_step = next(n for n in (4, 3, 2, 1) if p.slots % n == 0)
    last = p.chunks - 1
    n_together = last * p.subs
    n_apart = p.subs * p.half_tri

    def kernel(t, tiles, high, *refs):
        sources = [refs[k * p.subs : (k + 1) * p.subs] for k in range(last)]
        loose = refs[n_together : n_together + n_apart]
        out, scaled, packed = refs[n_together + n_apart :]
        sources.append([packed.at[shift] for shift in range(p.subs)])
        step = pl.program_id(0)
        sub = t[p.o_sub]

        @pl.when(step == 0)
        def _():
            for shift in range(p.subs):
                for n in range(p.half_tri):
                    packed[shift, t[p.o_me] ^ n] = loose[shift * p.half_tri + n][...]

        for u in range(per_step):
            slot = step * per_step + u
            for k in range(p.chunks):

                @pl.when((t[p.o_new + slot] == 1) & (t[p.o_row_chunk + slot] == k))
                def _():
                    strip = sources[k][0][:, t[p.o_row_place + slot]].reshape(p.strip, p.order)
                    dims = (((1,), (0,)), ((), ()))
                    product = lax.dot_general(
                        strip, high[...], dims, preferred_element_type=jnp.float32
                    )
                    scaled[...] = product.astype(jnp.bfloat16)

            live = t[p.o_live + slot] == 1
            for k in range(p.chunks):

                @pl.when(live & (t[p.o_col_chunk + slot] == k))
                def _():
                    strips = [
                        sources[k][shift][:, t[p.o_col_place + slot]].reshape(p.strip, p.order)
                        for shift in range(p.subs)
                    ]
                    for place in range(p.subs):
                        strip = strips[0]
                        for shift in range(1, p.subs):
                            here = lax.rem(sub + shift, p.subs) == place
                            strip = jnp.where(here, strips[shift], strip)
                        at = slice(place * p.strip, (place + 1) * p.strip)
                        out[u, :, at] = tiles[slot, :, at] + lax.dot_general(
                            scaled[...],
                            strip,
                            (((1,), (1,)), ((), ())),
                            preferred_element_type=jnp.float32,
                        )

            @pl.when(jnp.logical_not(live))
            def _():
                out[u] = tiles[slot]

    loose = [in_vmem(ref) for shift in apart for ref in shift]
    return pl.pallas_call(
        kernel,
        out_shape=jax.ShapeDtypeStruct(held.shape, jnp.float32),
        grid_spec=pltpu.PrefetchScalarGridSpec(
            num_scalar_prefetch=1,
            grid=(p.slots // per_step,),
            in_specs=[IN_VMEM] * (2 + n_together + n_apart),
            out_specs=pl.BlockSpec((per_step, p.strip, p.order), lambda i, t: (i, 0, 0)),
            scratch_shapes=[
                pltpu.VMEM((p.strip, p.order), jnp.bfloat16),
                pltpu.VMEM((p.subs, p.half_tri) + loose[0].shape, jnp.bfloat16),
            ],
        ),
        compiler_params=pltpu.CompilerParams(
            dimension_semantics=("arbitrary",), vmem_limit_bytes=16 * 2**20
        ),
        name="update",
    )(
        table,
        in_vmem(held),
        in_vmem(inverse),
        *[in_vmem(ref) for chunk in together for ref in chunk],
        *loose,
    )


def planned(p, stored_tiles, cell_owner):
    table = table_call(p, cell_owner)
    current = stored_tiles[0]
    halves = [list(range(h * p.half_tri, (h + 1) * p.half_tri)) for h in range(2)]
    swap = [(i, (i + p.half_tri) % p.tri) for i in range(p.tri)]

    def exchange(x):
        return lax.all_to_all(
            x, "tri", split_axis=0, concat_axis=0, tiled=True, axis_index_groups=halves
        )

    def arrivals(x):
        return [x] + [
            lax.ppermute(x, "sub", [((i + shift) % p.subs, i) for i in range(p.subs)])
            for shift in range(1, p.subs)
        ]

    near, far, arrived = [], [], []
    for chunk in range(p.chunks):
        pieces = extract_call(p, cell_owner, current, chunk)
        spread = exchange(pieces)
        near.append(pick_call(p, table, spread))
    for chunk in range(p.chunks):
        far.append(lax.ppermute(near[chunk], "tri", swap))
    last = p.chunks - 1
    for chunk in range(last):
        built = build_call(p, table, near[chunk], far[chunk], chunk == 0, False)
        whole = exchange(built)
        arrived.append(arrivals(whole))
    built = build_call(p, table, near[last], far[last], last == 0, True)
    loose = [built[0]]
    for n in range(1, p.half_tri):
        pairs = [(i, i ^ n) for i in range(p.tri)]
        loose.append(lax.ppermute(built[n], "tri", pairs))
    pieces = [arrivals(x) for x in loose]
    apart = [[piece[shift] for piece in pieces] for shift in range(p.subs)]
    marked = mark_call(p, table)
    inverse, held = inverse_call(p, marked, arrived[0], current)
    return update_call(p, table, held, arrived, apart, inverse)[None]


def shards(stored_tiles, cell_owner):
    p = Plan(
        lax.axis_size("tri"),
        lax.axis_size("sub"),
        stored_tiles.shape[1],
        stored_tiles.shape[2],
        stored_tiles.shape[3],
        2,
    )
    if p.tiled():
        return planned(p, stored_tiles, cell_owner)
    return untiled(stored_tiles, cell_owner)


def solution(mesh):
    placed = (P("tri", None, "sub", None), P())
    return jax.shard_map(
        shards, mesh=mesh, in_specs=placed, out_specs=P("tri", None, "sub", None), check_vma=False
    )
```

```python
import math

import jax
import jax.numpy as jnp
import numpy as np
from jax import lax
from jax.experimental import pallas as pl
from jax.experimental.pallas import tpu as pltpu
from jax.sharding import PartitionSpec as P


NB = 32


def shortened(x):

    def short(part):
        return part.astype(jnp.bfloat16) if part.dtype == jnp.float32 else part

    return jax.tree.map(short, x)


def layout(groups, per_group):
    half_group = per_group // 2
    slot_count = per_group * (per_group + 1) // 2
    row_table = np.full((groups * groups, slot_count), -1, np.int32)
    col_table = np.full((groups * groups, slot_count), -1, np.int32)
    for first_group in range(groups):
        for second_group in range(groups):
            cell_index = first_group * groups + second_group
            for inner_row in range(per_group):
                if first_group == second_group:
                    for inner_column in range(inner_row + 1):
                        slot_index = inner_row * (inner_row + 1) // 2 + inner_column
                        row_table[cell_index, slot_index] = first_group * per_group + inner_row
                        col_table[cell_index, slot_index] = first_group * per_group + inner_column
                else:
                    for inner_column in range(half_group):
                        slot_index = inner_row * half_group + inner_column
                        if first_group > second_group:
                            row_table[cell_index, slot_index] = first_group * per_group + inner_row
                            col_table[cell_index, slot_index] = (
                                second_group * per_group + inner_column
                            )
                        else:
                            row_table[cell_index, slot_index] = second_group * per_group + inner_row
                            col_table[cell_index, slot_index] = (
                                first_group * per_group + half_group + inner_column
                            )
    return (row_table, col_table)


def untiled(stored_tiles, cell_owner):
    tri_count = lax.axis_size("tri")
    groups = math.isqrt(tri_count)
    per_group = NB // groups
    half_group = per_group // 2
    strip_rows = stored_tiles.shape[2]
    block_order = stored_tiles.shape[3]
    row_table, col_table = layout(groups, per_group)
    position = lax.axis_index("tri")
    my_cell = jnp.sum(jnp.where(cell_owner == position, jnp.arange(tri_count, dtype=jnp.int32), 0))
    cell_down = my_cell // groups
    cell_across = my_cell % groups
    row_group = jnp.maximum(cell_down, cell_across)
    col_group = jnp.minimum(cell_down, cell_across)
    my_rows = jnp.asarray(row_table)[my_cell]
    my_cols = jnp.asarray(col_table)[my_cell]
    row_local = jnp.clip(my_rows - row_group * per_group, 0, per_group - 1)
    col_local = jnp.clip(my_cols - col_group * per_group, 0, per_group - 1)
    holders = cell_owner[jnp.arange(groups) * groups]
    highest = lax.Precision.HIGHEST
    current = stored_tiles[0]
    lower_slots = np.array([member * half_group for member in range(per_group)], np.int32)
    first_slots = np.array(
        [member * (member + 1) // 2 if member > 0 else 0 for member in range(per_group)], np.int32
    )
    keep_first = np.array([1.0 if member > 0 else 0.0 for member in range(per_group)], np.float32)
    from_lower = current[lower_slots]
    from_first = current[first_slots] * keep_first[:, None, None]
    holder_part = jnp.where(cell_down > 0, from_lower, from_first)
    holder_part = jnp.where(cell_across == 0, holder_part, 0.0).astype(jnp.bfloat16)
    pivot_slot = 0 // 2
    pivot_part = jnp.where(my_cell == 0, current[pivot_slot], 0.0)
    piece_size = holder_part.size // tri_count
    pivot_piece = pivot_part.size // tri_count
    spread_panel = lax.all_to_all(
        holder_part.reshape(tri_count, piece_size), "tri", split_axis=0, concat_axis=0, tiled=True
    )
    spread_pivot = lax.all_to_all(
        pivot_part.reshape(tri_count, pivot_piece).astype(jnp.bfloat16),
        "tri",
        split_axis=0,
        concat_axis=0,
        tiled=True,
    ).astype(jnp.float32)
    picked_panel = spread_panel[holders][:, None, :]
    picked_pivot = spread_pivot[holders[0]][None, :]
    whole_panel = lax.all_gather(picked_panel, "tri", axis=1, tiled=True)
    whole_pivot = lax.all_gather(
        picked_pivot.astype(jnp.bfloat16), "tri", axis=0, tiled=True
    ).astype(picked_pivot.dtype)
    panels = whole_panel.reshape(groups, per_group, strip_rows, block_order)
    pivot_strip = whole_pivot.reshape(strip_rows, block_order)
    own_strips = panels[row_group]
    other_strips = panels[col_group]
    pivot_block = lax.all_gather(
        pivot_strip.astype(jnp.bfloat16), "sub", axis=0, tiled=True
    ).astype(pivot_strip.dtype)
    partner = lax.all_gather(other_strips, "sub", axis=1, tiled=True)
    gram_matrix = jnp.dot(pivot_block.T, pivot_block, precision=highest)
    factor = jnp.linalg.cholesky(gram_matrix)
    column_count = block_order // lax.axis_size("sub")
    first_column = lax.axis_index("sub") * column_count
    columns = lax.dynamic_slice_in_dim(pivot_block.T, first_column, column_count, 1)
    column_part = jax.scipy.linalg.cho_solve((factor, True), columns)
    inverse = lax.all_gather(shortened(column_part), "sub", axis=1, tiled=True).astype(
        column_part.dtype
    )
    scaled = jnp.einsum(
        "irk,kc->irc", own_strips.astype(jnp.float32), inverse, precision=highest
    ).astype(jnp.bfloat16)
    left_slots = scaled[row_local]
    right_slots = partner[col_local]
    update = jnp.einsum("qrk,qck->qrc", left_slots, right_slots, preferred_element_type=jnp.float32)
    live_slots = (my_rows > 0) & (my_cols > 0)
    current = current + jnp.where(live_slots[:, None, None], update, 0.0)
    return current[None]


class Plan:
    def __init__(self, tri, subs, slots, strip, order):
        self.tri, self.subs, self.slots, self.strip, self.order = tri, subs, slots, strip, order
        self.groups = math.isqrt(tri)
        self.per_group = NB // self.groups
        self.half_group = self.per_group // 2
        self.half_tri = tri // 2
        self.piece = strip // self.half_tri
        quarter = self.half_group // 4
        self.wides = [2 * quarter, quarter, quarter]
        self.firsts = [0, 2 * quarter, 3 * quarter]
        self.spreads = [[0], [1, 2]]
        self.o_sub = 0
        self.o_diag = 1
        self.o_me = 2
        self.o_dead = 3
        self.o_src = 8
        self.o_here = self.o_src + self.groups
        self.o_rg = self.o_here + self.groups
        self.o_cg = self.o_rg + self.half_tri
        self.o_hf = self.o_cg + self.half_tri
        self.size = self.o_hf + self.half_tri

    def tiled(self):
        return (
            self.piece % 16 == 0
            and self.order % 128 == 0
            and self.half_group % 4 == 0
            and self.groups * self.groups == self.tri
            and self.half_tri & (self.half_tri - 1) == 0
            and self.subs * self.strip == self.order
            and self.slots == self.per_group * (self.per_group + 1) // 2
        )

    def tiles_of(self, chunk):
        inner = range(self.firsts[chunk], self.firsts[chunk] + self.wides[chunk])
        return [half * self.half_group + n for half in range(2) for n in inner]

    def place_of(self, member):
        for chunk in range(len(self.wides)):
            if member in self.tiles_of(chunk):
                return chunk, self.tiles_of(chunk).index(member)
        raise ValueError(member)

    def column_of(self, inner):
        chunk, place = self.place_of(inner)
        return chunk, 2 * self.wides[chunk] + place


def table_call(p, cell_owner):
    def kernel(owner, out, cell_of):
        position = lax.axis_index("tri")
        for cell in range(p.tri):
            cell_of[owner[cell]] = cell

        def split(cell):
            down = cell // p.groups
            across = cell - down * p.groups
            return down, across

        down, across = split(cell_of[position])
        col_group = jnp.minimum(down, across)
        diag = down == across
        my_half = position // p.half_tri
        out[p.o_sub] = lax.axis_index("sub")
        out[p.o_me] = position - my_half * p.half_tri
        out[p.o_diag] = jnp.where(diag, 1, 0)
        for group in range(p.groups):
            holder = owner[group * p.groups]
            half = holder // p.half_tri
            out[p.o_src + group] = holder - half * p.half_tri
            out[p.o_here + group] = jnp.where(half == my_half, 1, 0)
        for end in range(p.half_tri):
            there_down, there_across = split(cell_of[my_half * p.half_tri + end])
            out[p.o_rg + end] = jnp.maximum(there_down, there_across)
            out[p.o_cg + end] = jnp.minimum(there_down, there_across)
            out[p.o_hf + end] = jnp.where(there_down < there_across, 1, 0)
        out[p.o_dead] = jnp.where((col_group == 0) & (down >= across), 1, 0)

    return pl.pallas_call(
        kernel,
        out_shape=jax.ShapeDtypeStruct((p.size,), jnp.int32),
        in_specs=[pl.BlockSpec(memory_space=pltpu.SMEM)],
        out_specs=pl.BlockSpec(memory_space=pltpu.SMEM),
        scratch_shapes=[pltpu.SMEM((p.tri,), jnp.int32)],
        name="table",
    )(cell_owner)


IN_VMEM = pl.BlockSpec(memory_space=pltpu.VMEM)


def in_vmem(x):
    return pltpu.with_memory_space_constraint(x, pltpu.VMEM)


def limit(mib):
    return pltpu.CompilerParams(vmem_limit_bytes=mib * 2**20)


def in_hbm(x):
    return pltpu.with_memory_space_constraint(x, pltpu.HBM)


def in_hbm(x):
    return pltpu.with_memory_space_constraint(x, pltpu.HBM)


def mark_call(p, table):
    def kernel(t, out):
        for i in (p.o_sub, p.o_diag, p.o_me):
            out[i] = t[i]

    smem = pl.BlockSpec(memory_space=pltpu.SMEM)
    return pl.pallas_call(
        kernel,
        out_shape=jax.ShapeDtypeStruct((p.o_src,), jnp.int32),
        in_specs=[smem],
        out_specs=smem,
        compiler_params=limit(1),
        name="mark",
    )(table)


def extract_call(p, cell_owner, current, members):
    def kernel(owner, tiles, out, wide, sems):
        position = lax.axis_index("tri")
        cell = jnp.int32(0)
        for n in range(1, p.tri):
            cell = jnp.where(owner[n] == position, n, cell)
        down = cell // p.groups
        copies = []
        for place, member in enumerate(members):
            slot = jnp.where(down > 0, member * p.half_group, member * (member + 1) // 2)
            copies.append(
                pltpu.make_async_copy(tiles.at[slot], wide.at[place], sems.at[place])
            )
        for copy in copies:
            copy.start()
        for place, copy in enumerate(copies):
            copy.wait()
            rounded = wide[place].astype(jnp.bfloat16)
            out[:, place] = rounded.reshape(p.half_tri, p.piece, p.order)

    return pl.pallas_call(
        kernel,
        out_shape=pltpu.VMEM((p.half_tri, len(members), p.piece, p.order), jnp.bfloat16),
        in_specs=[
            pl.BlockSpec(memory_space=pltpu.SMEM),
            pl.BlockSpec(memory_space=pltpu.HBM),
        ],
        out_specs=IN_VMEM,
        scratch_shapes=[
            pltpu.VMEM((len(members), p.strip, p.order), jnp.float32),
            pltpu.SemaphoreType.DMA((len(members),)),
        ],
        compiler_params=limit(8),
        name="extract",
    )(cell_owner, in_hbm(current))


def pick_call(p, table, spread, chunks):
    def kernel(t, spread_ref, *outs):
        for g in range(p.groups):
            first = 0
            for out in outs:
                count = out.shape[1]
                out[g] = spread_ref[t[p.o_src + g], first : first + count]
                first += count

    return pl.pallas_call(
        kernel,
        out_shape=[
            pltpu.VMEM((p.groups, 2 * p.wides[k], p.piece, p.order), jnp.bfloat16) for k in chunks
        ],
        grid_spec=pltpu.PrefetchScalarGridSpec(
            num_scalar_prefetch=1,
            grid=(),
            in_specs=[IN_VMEM],
            out_specs=[IN_VMEM] * len(chunks),
        ),
        compiler_params=limit(8),
        name="pick",
    )(table, in_vmem(spread))


def build_call(p, table, near, far, wide, with_pivot, apart):
    rows = 3 * wide + (1 if with_pivot else 0)

    def kernel(t, near_ref, far_ref, *outs):
        def part(group, first, count, n, place):
            here = t[p.o_here + group] == 1
            at = pl.ds(place, count)

            def store(value):
                if apart:
                    outs[n][at] = value
                else:
                    outs[0][n, at] = value

            @pl.when(here)
            def _():
                store(near_ref[group, pl.ds(first, count)])

            @pl.when(jnp.logical_not(here))
            def _():
                store(far_ref[group, pl.ds(first, count)])

        for n in range(p.half_tri):
            end = t[p.o_me] ^ n if apart else n
            part(t[p.o_rg + end], 0, 2 * wide, n, 0)
            part(t[p.o_cg + end], t[p.o_hf + end] * wide, wide, n, 2 * wide)
            if with_pivot:
                part(0, 0, 1, n, 3 * wide)

    one = (rows, p.piece, p.order)
    if apart:
        out_shape = [pltpu.VMEM(one, jnp.bfloat16)] * p.half_tri
    else:
        out_shape = [pltpu.VMEM((p.half_tri,) + one, jnp.bfloat16)]
    outs = pl.pallas_call(
        kernel,
        out_shape=out_shape,
        grid_spec=pltpu.PrefetchScalarGridSpec(
            num_scalar_prefetch=1,
            grid=(),
            in_specs=[IN_VMEM, IN_VMEM],
            out_specs=[IN_VMEM] * len(out_shape),
        ),
        compiler_params=limit(8),
        name="build",
    )(table, in_vmem(near), in_vmem(far))
    return outs if apart else outs[0]


def inverse_call(p, table, arrived, current):
    loads = next(n for n in (6, 5, 4, 3, 2, 1) if p.slots % n == 0)
    each = p.slots // loads
    place = 3 * p.wides[0]
    order = p.order

    def kernel(t, *refs):
        sources = refs[: p.subs]
        tiles, high, held, pivot, x_wide, x_half, e_ref, sems = refs[p.subs :]
        copies = [
            pltpu.make_async_copy(
                tiles.at[pl.ds(n * each, each)], held.at[pl.ds(n * each, each)], sems.at[n]
            )
            for n in range(loads)
        ]
        for copy in copies:
            copy.start()
        for shift in range(p.subs):
            strip = lax.rem(t[p.o_sub] + shift, p.subs) * p.strip
            at = pl.multiple_of(strip, p.strip)
            pivot[pl.ds(at, p.strip)] = sources[shift][:, place].reshape(p.strip, order)

        def dot(a, b):
            return lax.dot_general(
                a, b, (((1,), (0,)), ((), ())), preferred_element_type=jnp.float32
            )

        def eye():
            r = lax.broadcasted_iota(jnp.int32, (order, order), 0)
            c = lax.broadcasted_iota(jnp.int32, (order, order), 1)
            return jnp.where(r == c, 1.0, 0.0)

        square = -dot(pivot[...], pivot[...])
        factor = 1.9 / jnp.max(jnp.sum(jnp.abs(square), axis=1))
        residual = eye() - factor * square
        e_ref[...] = residual.astype(jnp.bfloat16)
        wide = -factor * (pivot[...].astype(jnp.float32) + dot(pivot[...], e_ref[...]))
        x_wide[...] = wide
        x_half[...] = wide.astype(jnp.bfloat16)

        def coarse_on(carry):
            step, error, before, noise = carry
            stuck = (before < 1.0) & (error > 0.5 * before)
            return (step < 60) & (error > 3e-3) & (noise < 0.1) & jnp.logical_not(stuck)

        def coarse(carry):
            step, before, _, _ = carry
            x = x_half[...]
            residual = eye() - dot(pivot[...], x)
            e_ref[...] = residual.astype(jnp.bfloat16)
            error = jnp.sum(residual * residual)
            new = x.astype(jnp.float32) + dot(x, e_ref[...])
            x_wide[...] = new
            x_half[...] = new.astype(jnp.bfloat16)
            noise = jnp.sum(new * new) / factor * 2.0**-18
            return step + 1, error, before, noise

        big = jnp.float32(1e30)
        _, reached, _, _ = lax.while_loop(
            coarse_on, coarse, (jnp.int32(0), big, big, jnp.float32(0.0))
        )

        def fine_on(carry):
            step, error, before = carry
            stuck = (before < 0.5) & (error > 0.5 * before)
            return (step < 100) & (error > 1e-4) & jnp.logical_not(stuck)

        def fine(carry):
            step, before, _ = carry
            x = x_wide[...]
            x_high = x.astype(jnp.bfloat16)
            x_low = (x - x_high.astype(jnp.float32)).astype(jnp.bfloat16)
            residual = eye() - (dot(pivot[...], x_high) + dot(pivot[...], x_low))
            error = jnp.sum(residual * residual)
            e_high = residual.astype(jnp.bfloat16)
            e_low = (residual - e_high.astype(jnp.float32)).astype(jnp.bfloat16)
            x_wide[...] = x + (dot(x_high, e_high) + (dot(x_high, e_low) + dot(x_low, e_high)))
            return step + 1, error, before

        @pl.when(jnp.logical_not(reached <= 3e-3))
        def _():
            lax.while_loop(fine_on, fine, (jnp.int32(0), big, big))

        high[...] = x_wide[...].astype(jnp.bfloat16)
        for copy in copies:
            copy.wait()

    square_shape = pltpu.VMEM((order, order), jnp.bfloat16)
    return pl.pallas_call(
        kernel,
        out_shape=(square_shape, pltpu.VMEM(current.shape, jnp.float32)),
        grid_spec=pltpu.PrefetchScalarGridSpec(
            num_scalar_prefetch=1,
            grid=(),
            in_specs=[IN_VMEM] * p.subs + [pl.BlockSpec(memory_space=pltpu.HBM)],
            out_specs=(IN_VMEM, IN_VMEM),
            scratch_shapes=[
                pltpu.VMEM((order, order), jnp.bfloat16),
                pltpu.VMEM((order, order), jnp.float32),
                pltpu.VMEM((order, order), jnp.bfloat16),
                pltpu.VMEM((order, order), jnp.bfloat16),
                pltpu.SemaphoreType.DMA((loads,)),
            ],
        ),
        compiler_params=limit(12),
        cost_estimate=pl.CostEstimate(
            flops=60 * 2 * order**3, bytes_accessed=4 * order**2, transcendentals=0
        ),
        name="inverse",
    )(table, *[in_vmem(x) for x in arrived], in_hbm(current))


def update_call(p, table, held, together, apart, inverse):
    ring_size = 8
    chunks = len(p.wides)
    rows_in_box = p.per_group * p.half_group

    def kernel(t, tiles, inv, *refs):
        sources = [list(refs[: p.subs])]
        at = p.subs
        loose = []
        for _ in range(1, chunks):
            loose.append(refs[at : at + p.subs * p.half_tri])
            at += p.subs * p.half_tri
        out, column, ring, ring_sems, rest_sem, *packed = refs[at:]
        sub = t[p.o_sub]
        diag = t[p.o_diag] == 1
        dead = t[p.o_dead] == 1

        for k in range(chunks - 1):
            for shift in range(p.subs):
                for n in range(p.half_tri):
                    packed[k][shift, t[p.o_me] ^ n] = loose[k][shift * p.half_tri + n][...]
            sources.append([packed[k].at[shift] for shift in range(p.subs)])

        def strip_of(shift, chunk, place):
            return sources[chunk][shift][:, place].reshape(p.strip, p.order)

        def gather_column(j, chunk, place):
            strips = [strip_of(shift, chunk, place) for shift in range(p.subs)]
            for at in range(p.subs):
                strip = strips[0]
                for shift in range(1, p.subs):
                    here = lax.rem(sub + shift, p.subs) == at
                    strip = jnp.where(here, strips[shift], strip)
                if j == 0:
                    strip = jnp.where(dead, jnp.zeros_like(strip), strip)
                column[j, at * p.strip : (at + 1) * p.strip] = strip

        def scale(members):
            strips = [strip_of(0, *p.place_of(member)) for member in members]
            product = lax.dot_general(
                jnp.concatenate(strips, axis=0),
                inv[...],
                (((1,), (0,)), ((), ())),
                preferred_element_type=jnp.float32,
            )
            return product.astype(jnp.bfloat16)

        def times(left, j):
            return lax.dot_general(
                left, column[j], (((1,), (1,)), ((), ())), preferred_element_type=jnp.float32
            )

        class Writer:
            def __init__(self):
                self.copies = []

            def put(self, slot, product):
                n = len(self.copies)
                if n >= ring_size:
                    self.copies[n - ring_size].wait()
                ring[n % ring_size] = tiles[slot] + product
                copy = pltpu.make_async_copy(
                    ring.at[n % ring_size], out.at[slot], ring_sems.at[n % ring_size]
                )
                copy.start()
                self.copies.append(copy)

            def finish(self):
                for copy in self.copies[-ring_size:]:
                    copy.wait()

        @pl.when(diag)
        def _():
            writer = Writer()
            for i in range(0, p.per_group, 2):
                left = scale([i, i + 1])
                for j in range(i + 1):
                    if j == i:
                        gather_column(j, *p.place_of(j))
                    product = times(left, j)
                    for r in range(2):
                        slot = (i + r) * (i + r + 1) // 2 + j
                        writer.put(slot, product[r * p.strip : (r + 1) * p.strip])
                gather_column(i + 1, *p.place_of(i + 1))
                slot = (i + 1) * (i + 2) // 2 + i + 1
                writer.put(slot, times(left[p.strip :], i + 1))
            writer.finish()

        @pl.when(jnp.logical_not(diag))
        def _():
            if p.slots > rows_in_box:
                empty = pl.ds(rows_in_box, p.slots - rows_in_box)
                rest = pltpu.make_async_copy(tiles.at[empty], out.at[empty], rest_sem)
                rest.start()
            writer = Writer()
            for i in range(0, p.per_group, 2):
                left = scale([i, i + 1])
                for j in range(p.half_group):
                    if i == 0:
                        gather_column(j, *p.column_of(j))
                    product = times(left, j)
                    for r in range(2):
                        slot = (i + r) * p.half_group + j
                        writer.put(slot, product[r * p.strip : (r + 1) * p.strip])
            writer.finish()
            if p.slots > rows_in_box:
                rest.wait()

    loose = [in_vmem(ref) for chunk in apart for shift in chunk for ref in shift]
    return pl.pallas_call(
        kernel,
        out_shape=jax.ShapeDtypeStruct(held.shape, jnp.float32),
        grid_spec=pltpu.PrefetchScalarGridSpec(
            num_scalar_prefetch=1,
            grid=(),
            in_specs=[IN_VMEM] * (2 + p.subs + len(loose)),
            out_specs=pl.BlockSpec(memory_space=pltpu.HBM),
            scratch_shapes=[
                pltpu.VMEM((p.per_group, p.order, p.order), jnp.bfloat16),
                pltpu.VMEM((ring_size, p.strip, p.order), jnp.float32),
                pltpu.SemaphoreType.DMA((ring_size,)),
                pltpu.SemaphoreType.DMA,
            ]
            + [
                pltpu.VMEM((p.subs, p.half_tri) + chunk[0][0].shape, jnp.bfloat16)
                for chunk in apart
            ],
        ),
        compiler_params=limit(24),
        name="update",
    )(table, in_vmem(held), in_vmem(inverse), *[in_vmem(ref) for ref in together], *loose)


def planned(p, stored_tiles, cell_owner):
    table = table_call(p, cell_owner)
    current = stored_tiles[0]
    halves = [list(range(h * p.half_tri, (h + 1) * p.half_tri)) for h in range(2)]
    swap = [(i, (i + p.half_tri) % p.tri) for i in range(p.tri)]

    def exchange(x):
        return lax.all_to_all(
            x, "tri", split_axis=0, concat_axis=0, tiled=True, axis_index_groups=halves
        )

    def arrivals(x):
        return [x] + [
            lax.ppermute(x, "sub", [((i + shift) % p.subs, i) for i in range(p.subs)])
            for shift in range(1, p.subs)
        ]

    chunks = len(p.wides)
    near, far = [], []
    for members in p.spreads:
        tiles = [tile for chunk in members for tile in p.tiles_of(chunk)]
        pieces = extract_call(p, cell_owner, current, tiles)
        spread = exchange(pieces)
        near.extend(pick_call(p, table, spread, members))
    for chunk in range(chunks):
        far.append(lax.ppermute(near[chunk], "tri", swap))
    built = build_call(p, table, near[0], far[0], p.wides[0], True, False)
    whole = exchange(built)
    together = arrivals(whole)
    apart = []
    for chunk in range(1, chunks):
        built = build_call(p, table, near[chunk], far[chunk], p.wides[chunk], False, True)
        loose = [built[0]]
        for n in range(1, p.half_tri):
            pairs = [(i, i ^ n) for i in range(p.tri)]
            loose.append(lax.ppermute(built[n], "tri", pairs))
        sides = [arrivals(x) for x in loose]
        apart.append([[piece[shift] for piece in sides] for shift in range(p.subs)])
    marked = mark_call(p, table)
    inverse, held = inverse_call(p, marked, together, current)
    return update_call(p, table, held, together, apart, inverse)[None]


def shards(stored_tiles, cell_owner):
    p = Plan(
        lax.axis_size("tri"),
        lax.axis_size("sub"),
        stored_tiles.shape[1],
        stored_tiles.shape[2],
        stored_tiles.shape[3],
    )
    if p.tiled():
        return planned(p, stored_tiles, cell_owner)
    return untiled(stored_tiles, cell_owner)


def solution(mesh):
    placed = (P("tri", None, "sub", None), P())
    return jax.shard_map(
        shards, mesh=mesh, in_specs=placed, out_specs=P("tri", None, "sub", None), check_vma=False
    )
```

```python
import math

import jax
import jax.numpy as jnp
import numpy as np
from jax import lax
from jax.experimental import pallas as pl
from jax.experimental.pallas import tpu as pltpu
from jax.sharding import PartitionSpec as P


NB = 32


def shortened(x):

    def short(part):
        return part.astype(jnp.bfloat16) if part.dtype == jnp.float32 else part

    return jax.tree.map(short, x)


def layout(groups, per_group):
    half_group = per_group // 2
    slot_count = per_group * (per_group + 1) // 2
    row_table = np.full((groups * groups, slot_count), -1, np.int32)
    col_table = np.full((groups * groups, slot_count), -1, np.int32)
    for first_group in range(groups):
        for second_group in range(groups):
            cell_index = first_group * groups + second_group
            for inner_row in range(per_group):
                if first_group == second_group:
                    for inner_column in range(inner_row + 1):
                        slot_index = inner_row * (inner_row + 1) // 2 + inner_column
                        row_table[cell_index, slot_index] = first_group * per_group + inner_row
                        col_table[cell_index, slot_index] = first_group * per_group + inner_column
                else:
                    for inner_column in range(half_group):
                        slot_index = inner_row * half_group + inner_column
                        if first_group > second_group:
                            row_table[cell_index, slot_index] = first_group * per_group + inner_row
                            col_table[cell_index, slot_index] = (
                                second_group * per_group + inner_column
                            )
                        else:
                            row_table[cell_index, slot_index] = second_group * per_group + inner_row
                            col_table[cell_index, slot_index] = (
                                first_group * per_group + half_group + inner_column
                            )
    return (row_table, col_table)


def untiled(stored_tiles, cell_owner):
    tri_count = lax.axis_size("tri")
    groups = math.isqrt(tri_count)
    per_group = NB // groups
    half_group = per_group // 2
    strip_rows = stored_tiles.shape[2]
    block_order = stored_tiles.shape[3]
    row_table, col_table = layout(groups, per_group)
    position = lax.axis_index("tri")
    my_cell = jnp.sum(jnp.where(cell_owner == position, jnp.arange(tri_count, dtype=jnp.int32), 0))
    cell_down = my_cell // groups
    cell_across = my_cell % groups
    row_group = jnp.maximum(cell_down, cell_across)
    col_group = jnp.minimum(cell_down, cell_across)
    my_rows = jnp.asarray(row_table)[my_cell]
    my_cols = jnp.asarray(col_table)[my_cell]
    row_local = jnp.clip(my_rows - row_group * per_group, 0, per_group - 1)
    col_local = jnp.clip(my_cols - col_group * per_group, 0, per_group - 1)
    holders = cell_owner[jnp.arange(groups) * groups]
    highest = lax.Precision.HIGHEST
    current = stored_tiles[0]
    lower_slots = np.array([member * half_group for member in range(per_group)], np.int32)
    first_slots = np.array(
        [member * (member + 1) // 2 if member > 0 else 0 for member in range(per_group)], np.int32
    )
    keep_first = np.array([1.0 if member > 0 else 0.0 for member in range(per_group)], np.float32)
    from_lower = current[lower_slots]
    from_first = current[first_slots] * keep_first[:, None, None]
    holder_part = jnp.where(cell_down > 0, from_lower, from_first)
    holder_part = jnp.where(cell_across == 0, holder_part, 0.0).astype(jnp.bfloat16)
    pivot_slot = 0 // 2
    pivot_part = jnp.where(my_cell == 0, current[pivot_slot], 0.0)
    piece_size = holder_part.size // tri_count
    pivot_piece = pivot_part.size // tri_count
    spread_panel = lax.all_to_all(
        holder_part.reshape(tri_count, piece_size), "tri", split_axis=0, concat_axis=0, tiled=True
    )
    spread_pivot = lax.all_to_all(
        pivot_part.reshape(tri_count, pivot_piece).astype(jnp.bfloat16),
        "tri",
        split_axis=0,
        concat_axis=0,
        tiled=True,
    ).astype(jnp.float32)
    picked_panel = spread_panel[holders][:, None, :]
    picked_pivot = spread_pivot[holders[0]][None, :]
    whole_panel = lax.all_gather(picked_panel, "tri", axis=1, tiled=True)
    whole_pivot = lax.all_gather(
        picked_pivot.astype(jnp.bfloat16), "tri", axis=0, tiled=True
    ).astype(picked_pivot.dtype)
    panels = whole_panel.reshape(groups, per_group, strip_rows, block_order)
    pivot_strip = whole_pivot.reshape(strip_rows, block_order)
    own_strips = panels[row_group]
    other_strips = panels[col_group]
    pivot_block = lax.all_gather(
        pivot_strip.astype(jnp.bfloat16), "sub", axis=0, tiled=True
    ).astype(pivot_strip.dtype)
    partner = lax.all_gather(other_strips, "sub", axis=1, tiled=True)
    gram_matrix = jnp.dot(pivot_block.T, pivot_block, precision=highest)
    factor = jnp.linalg.cholesky(gram_matrix)
    column_count = block_order // lax.axis_size("sub")
    first_column = lax.axis_index("sub") * column_count
    columns = lax.dynamic_slice_in_dim(pivot_block.T, first_column, column_count, 1)
    column_part = jax.scipy.linalg.cho_solve((factor, True), columns)
    inverse = lax.all_gather(shortened(column_part), "sub", axis=1, tiled=True).astype(
        column_part.dtype
    )
    scaled = jnp.einsum(
        "irk,kc->irc", own_strips.astype(jnp.float32), inverse, precision=highest
    ).astype(jnp.bfloat16)
    left_slots = scaled[row_local]
    right_slots = partner[col_local]
    update = jnp.einsum("qrk,qck->qrc", left_slots, right_slots, preferred_element_type=jnp.float32)
    live_slots = (my_rows > 0) & (my_cols > 0)
    current = current + jnp.where(live_slots[:, None, None], update, 0.0)
    return current[None]


class Plan:
    def __init__(self, tri, subs, slots, strip, order):
        self.tri, self.subs, self.slots, self.strip, self.order = tri, subs, slots, strip, order
        self.groups = math.isqrt(tri)
        self.per_group = NB // self.groups
        self.half_group = self.per_group // 2
        self.half_tri = tri // 2
        self.piece = strip // self.half_tri
        quarter = self.half_group // 4
        self.wides = [quarter, quarter, 2 * quarter]
        self.firsts = [0, quarter, 2 * quarter]
        self.spreads = [[0, 1], [2]]
        self.o_sub = 0
        self.o_diag = 1
        self.o_me = 2
        self.o_dead = 3
        self.o_src = 8
        self.o_here = self.o_src + self.groups
        self.o_rg = self.o_here + self.groups
        self.o_cg = self.o_rg + self.half_tri
        self.o_hf = self.o_cg + self.half_tri
        self.size = self.o_hf + self.half_tri

    def tiled(self):
        return (
            self.piece % 16 == 0
            and self.order % 128 == 0
            and self.half_group % 4 == 0
            and self.groups * self.groups == self.tri
            and self.half_tri & (self.half_tri - 1) == 0
            and self.subs * self.strip == self.order
            and self.slots == self.per_group * (self.per_group + 1) // 2
        )

    def tiles_of(self, chunk):
        inner = range(self.firsts[chunk], self.firsts[chunk] + self.wides[chunk])
        return [half * self.half_group + n for half in range(2) for n in inner]

    def place_of(self, member):
        for chunk in range(len(self.wides)):
            if member in self.tiles_of(chunk):
                return chunk, self.tiles_of(chunk).index(member)
        raise ValueError(member)

    def column_of(self, inner):
        chunk, place = self.place_of(inner)
        return chunk, 2 * self.wides[chunk] + place


def table_call(p, cell_owner):
    def kernel(owner, out, cell_of):
        position = lax.axis_index("tri")
        for cell in range(p.tri):
            cell_of[owner[cell]] = cell

        def split(cell):
            down = cell // p.groups
            across = cell - down * p.groups
            return down, across

        down, across = split(cell_of[position])
        col_group = jnp.minimum(down, across)
        diag = down == across
        my_half = position // p.half_tri
        out[p.o_sub] = lax.axis_index("sub")
        out[p.o_me] = position - my_half * p.half_tri
        out[p.o_diag] = jnp.where(diag, 1, 0)
        for group in range(p.groups):
            holder = owner[group * p.groups]
            half = holder // p.half_tri
            out[p.o_src + group] = holder - half * p.half_tri
            out[p.o_here + group] = jnp.where(half == my_half, 1, 0)
        for end in range(p.half_tri):
            there_down, there_across = split(cell_of[my_half * p.half_tri + end])
            out[p.o_rg + end] = jnp.maximum(there_down, there_across)
            out[p.o_cg + end] = jnp.minimum(there_down, there_across)
            out[p.o_hf + end] = jnp.where(there_down < there_across, 1, 0)
        out[p.o_dead] = jnp.where((col_group == 0) & (down >= across), 1, 0)

    return pl.pallas_call(
        kernel,
        out_shape=jax.ShapeDtypeStruct((p.size,), jnp.int32),
        in_specs=[pl.BlockSpec(memory_space=pltpu.SMEM)],
        out_specs=pl.BlockSpec(memory_space=pltpu.SMEM),
        scratch_shapes=[pltpu.SMEM((p.tri,), jnp.int32)],
        name="table",
    )(cell_owner)


IN_VMEM = pl.BlockSpec(memory_space=pltpu.VMEM)


def in_vmem(x):
    return pltpu.with_memory_space_constraint(x, pltpu.VMEM)


def limit(mib):
    return pltpu.CompilerParams(vmem_limit_bytes=mib * 2**20)


def in_hbm(x):
    return pltpu.with_memory_space_constraint(x, pltpu.HBM)


def in_hbm(x):
    return pltpu.with_memory_space_constraint(x, pltpu.HBM)


def mark_call(p, table):
    def kernel(t, out):
        for i in (p.o_sub, p.o_diag, p.o_me):
            out[i] = t[i]

    smem = pl.BlockSpec(memory_space=pltpu.SMEM)
    return pl.pallas_call(
        kernel,
        out_shape=jax.ShapeDtypeStruct((p.o_src,), jnp.int32),
        in_specs=[smem],
        out_specs=smem,
        compiler_params=limit(1),
        name="mark",
    )(table)


def extract_call(p, cell_owner, current, members):
    def kernel(owner, tiles, out, wide, sems):
        position = lax.axis_index("tri")
        cell = jnp.int32(0)
        for n in range(1, p.tri):
            cell = jnp.where(owner[n] == position, n, cell)
        down = cell // p.groups
        copies = []
        for place, member in enumerate(members):
            slot = jnp.where(down > 0, member * p.half_group, member * (member + 1) // 2)
            copies.append(
                pltpu.make_async_copy(tiles.at[slot], wide.at[place], sems.at[place])
            )
        for copy in copies:
            copy.start()
        for place, copy in enumerate(copies):
            copy.wait()
            rounded = wide[place].astype(jnp.bfloat16)
            out[:, place] = rounded.reshape(p.half_tri, p.piece, p.order)

    return pl.pallas_call(
        kernel,
        out_shape=pltpu.VMEM((p.half_tri, len(members), p.piece, p.order), jnp.bfloat16),
        in_specs=[
            pl.BlockSpec(memory_space=pltpu.SMEM),
            pl.BlockSpec(memory_space=pltpu.HBM),
        ],
        out_specs=IN_VMEM,
        scratch_shapes=[
            pltpu.VMEM((len(members), p.strip, p.order), jnp.float32),
            pltpu.SemaphoreType.DMA((len(members),)),
        ],
        compiler_params=limit(8),
        name="extract",
    )(cell_owner, in_hbm(current))


def pick_call(p, table, spread, chunks):
    def kernel(t, spread_ref, *outs):
        for g in range(p.groups):
            first = 0
            for out in outs:
                count = out.shape[1]
                out[g] = spread_ref[t[p.o_src + g], first : first + count]
                first += count

    return pl.pallas_call(
        kernel,
        out_shape=[
            pltpu.VMEM((p.groups, 2 * p.wides[k], p.piece, p.order), jnp.bfloat16) for k in chunks
        ],
        grid_spec=pltpu.PrefetchScalarGridSpec(
            num_scalar_prefetch=1,
            grid=(),
            in_specs=[IN_VMEM],
            out_specs=[IN_VMEM] * len(chunks),
        ),
        compiler_params=limit(8),
        name="pick",
    )(table, in_vmem(spread))


def build_call(p, table, near, far, wide, with_pivot):
    rows = 3 * wide + (1 if with_pivot else 0)

    def kernel(t, near_ref, far_ref, *outs):
        def part(group, first, count, out, place):
            here = t[p.o_here + group] == 1

            @pl.when(here)
            def _():
                out[place : place + count] = near_ref[group, pl.ds(first, count)]

            @pl.when(jnp.logical_not(here))
            def _():
                out[place : place + count] = far_ref[group, pl.ds(first, count)]

        for n, out in enumerate(outs):
            end = t[p.o_me] ^ n
            part(t[p.o_rg + end], 0, 2 * wide, out, 0)
            part(t[p.o_cg + end], t[p.o_hf + end] * wide, wide, out, 2 * wide)
            if with_pivot:
                part(0, 0, 1, out, 3 * wide)

    return pl.pallas_call(
        kernel,
        out_shape=[pltpu.VMEM((rows, p.piece, p.order), jnp.bfloat16)] * p.half_tri,
        grid_spec=pltpu.PrefetchScalarGridSpec(
            num_scalar_prefetch=1,
            grid=(),
            in_specs=[IN_VMEM, IN_VMEM],
            out_specs=[IN_VMEM] * p.half_tri,
        ),
        compiler_params=limit(8),
        name="build",
    )(table, in_vmem(near), in_vmem(far))


def pack_call(p, table, pieces):
    def kernel(t, *refs):
        out = refs[-1]
        for n in range(p.half_tri):
            out[t[p.o_me] ^ n] = refs[n][...]

    return pl.pallas_call(
        kernel,
        out_shape=pltpu.VMEM((p.half_tri,) + pieces[0].shape, jnp.bfloat16),
        grid_spec=pltpu.PrefetchScalarGridSpec(
            num_scalar_prefetch=1,
            grid=(),
            in_specs=[IN_VMEM] * p.half_tri,
            out_specs=IN_VMEM,
        ),
        compiler_params=limit(8),
        name="pack",
    )(table, *[in_vmem(x) for x in pieces])


def inverse_call(p, table, arrived, current):
    loads = next(n for n in (6, 5, 4, 3, 2, 1) if p.slots % n == 0)
    each = p.slots // loads
    place = 3 * p.wides[0]
    order = p.order

    def kernel(t, *refs):
        sources = refs[: p.subs]
        tiles, high, held, pivot, x_wide, x_half, e_ref, sems = refs[p.subs :]
        copies = [
            pltpu.make_async_copy(
                tiles.at[pl.ds(n * each, each)], held.at[pl.ds(n * each, each)], sems.at[n]
            )
            for n in range(loads)
        ]
        for copy in copies:
            copy.start()
        for shift in range(p.subs):
            strip = lax.rem(t[p.o_sub] + shift, p.subs) * p.strip
            at = pl.multiple_of(strip, p.strip)
            pivot[pl.ds(at, p.strip)] = sources[shift][:, place].reshape(p.strip, order)

        def dot(a, b):
            return lax.dot_general(
                a, b, (((1,), (0,)), ((), ())), preferred_element_type=jnp.float32
            )

        def eye():
            r = lax.broadcasted_iota(jnp.int32, (order, order), 0)
            c = lax.broadcasted_iota(jnp.int32, (order, order), 1)
            return jnp.where(r == c, 1.0, 0.0)

        square = -dot(pivot[...], pivot[...])
        factor = 1.9 / jnp.max(jnp.sum(jnp.abs(square), axis=1))
        residual = eye() - factor * square
        e_ref[...] = residual.astype(jnp.bfloat16)
        wide = -factor * (pivot[...].astype(jnp.float32) + dot(pivot[...], e_ref[...]))
        x_wide[...] = wide
        x_half[...] = wide.astype(jnp.bfloat16)

        def coarse_on(carry):
            step, error, before, noise = carry
            stuck = (before < 1.0) & (error > 0.5 * before)
            return (step < 60) & (error > 3e-3) & (noise < 0.1) & jnp.logical_not(stuck)

        def coarse(carry):
            step, before, _, _ = carry
            x = x_half[...]
            residual = eye() - dot(pivot[...], x)
            e_ref[...] = residual.astype(jnp.bfloat16)
            error = jnp.sum(residual * residual)
            new = x.astype(jnp.float32) + dot(x, e_ref[...])
            x_wide[...] = new
            x_half[...] = new.astype(jnp.bfloat16)
            noise = jnp.sum(new * new) / factor * 2.0**-18
            return step + 1, error, before, noise

        big = jnp.float32(1e30)
        _, reached, _, _ = lax.while_loop(
            coarse_on, coarse, (jnp.int32(0), big, big, jnp.float32(0.0))
        )

        def fine_on(carry):
            step, error, before = carry
            stuck = (before < 0.5) & (error > 0.5 * before)
            return (step < 100) & (error > 1e-4) & jnp.logical_not(stuck)

        def fine(carry):
            step, before, _ = carry
            x = x_wide[...]
            x_high = x.astype(jnp.bfloat16)
            x_low = (x - x_high.astype(jnp.float32)).astype(jnp.bfloat16)
            residual = eye() - (dot(pivot[...], x_high) + dot(pivot[...], x_low))
            error = jnp.sum(residual * residual)
            e_high = residual.astype(jnp.bfloat16)
            e_low = (residual - e_high.astype(jnp.float32)).astype(jnp.bfloat16)
            x_wide[...] = x + (dot(x_high, e_high) + (dot(x_high, e_low) + dot(x_low, e_high)))
            return step + 1, error, before

        @pl.when(jnp.logical_not(reached <= 3e-3))
        def _():
            lax.while_loop(fine_on, fine, (jnp.int32(0), big, big))

        high[...] = x_wide[...].astype(jnp.bfloat16)
        for copy in copies:
            copy.wait()

    square_shape = pltpu.VMEM((order, order), jnp.bfloat16)
    return pl.pallas_call(
        kernel,
        out_shape=(square_shape, pltpu.VMEM(current.shape, jnp.float32)),
        grid_spec=pltpu.PrefetchScalarGridSpec(
            num_scalar_prefetch=1,
            grid=(),
            in_specs=[IN_VMEM] * p.subs + [pl.BlockSpec(memory_space=pltpu.HBM)],
            out_specs=(IN_VMEM, IN_VMEM),
            scratch_shapes=[
                pltpu.VMEM((order, order), jnp.bfloat16),
                pltpu.VMEM((order, order), jnp.float32),
                pltpu.VMEM((order, order), jnp.bfloat16),
                pltpu.VMEM((order, order), jnp.bfloat16),
                pltpu.SemaphoreType.DMA((loads,)),
            ],
        ),
        compiler_params=limit(12),
        cost_estimate=pl.CostEstimate(
            flops=60 * 2 * order**3, bytes_accessed=4 * order**2, transcendentals=0
        ),
        name="inverse",
    )(table, *[in_vmem(x) for x in arrived], in_hbm(current))


def update_call(p, table, held, arrived, inverse):
    ring_size = 8
    chunks = len(p.wides)
    rows_in_box = p.per_group * p.half_group

    def kernel(t, tiles, inv, *refs):
        sources = [refs[k * p.subs : (k + 1) * p.subs] for k in range(chunks)]
        out, column, ring, ring_sems, rest_sem = refs[chunks * p.subs :]
        sub = t[p.o_sub]
        diag = t[p.o_diag] == 1
        dead = t[p.o_dead] == 1

        def strip_of(shift, chunk, place):
            return sources[chunk][shift][:, place].reshape(p.strip, p.order)

        def gather_column(j, chunk, place):
            strips = [strip_of(shift, chunk, place) for shift in range(p.subs)]
            for at in range(p.subs):
                strip = strips[0]
                for shift in range(1, p.subs):
                    here = lax.rem(sub + shift, p.subs) == at
                    strip = jnp.where(here, strips[shift], strip)
                if j == 0:
                    strip = jnp.where(dead, jnp.zeros_like(strip), strip)
                column[j, at * p.strip : (at + 1) * p.strip] = strip

        def scale(members):
            strips = [strip_of(0, *p.place_of(member)) for member in members]
            product = lax.dot_general(
                jnp.concatenate(strips, axis=0),
                inv[...],
                (((1,), (0,)), ((), ())),
                preferred_element_type=jnp.float32,
            )
            return product.astype(jnp.bfloat16)

        def times(left, j):
            return lax.dot_general(
                left, column[j], (((1,), (1,)), ((), ())), preferred_element_type=jnp.float32
            )

        class Writer:
            def __init__(self):
                self.copies = []

            def put(self, slot, product):
                n = len(self.copies)
                if n >= ring_size:
                    self.copies[n - ring_size].wait()
                ring[n % ring_size] = tiles[slot] + product
                copy = pltpu.make_async_copy(
                    ring.at[n % ring_size], out.at[slot], ring_sems.at[n % ring_size]
                )
                copy.start()
                self.copies.append(copy)

            def finish(self):
                for copy in self.copies[-ring_size:]:
                    copy.wait()

        @pl.when(diag)
        def _():
            writer = Writer()
            for i in range(0, p.per_group, 2):
                left = scale([i, i + 1])
                for j in range(i + 1):
                    if j == i:
                        gather_column(j, *p.place_of(j))
                    product = times(left, j)
                    for r in range(2):
                        slot = (i + r) * (i + r + 1) // 2 + j
                        writer.put(slot, product[r * p.strip : (r + 1) * p.strip])
                gather_column(i + 1, *p.place_of(i + 1))
                slot = (i + 1) * (i + 2) // 2 + i + 1
                writer.put(slot, times(left[p.strip :], i + 1))
            writer.finish()

        @pl.when(jnp.logical_not(diag))
        def _():
            if p.slots > rows_in_box:
                empty = pl.ds(rows_in_box, p.slots - rows_in_box)
                rest = pltpu.make_async_copy(tiles.at[empty], out.at[empty], rest_sem)
                rest.start()
            writer = Writer()
            for i in range(0, p.per_group, 2):
                left = scale([i, i + 1])
                for j in range(p.half_group):
                    if i == 0:
                        gather_column(j, *p.column_of(j))
                    product = times(left, j)
                    for r in range(2):
                        slot = (i + r) * p.half_group + j
                        writer.put(slot, product[r * p.strip : (r + 1) * p.strip])
            writer.finish()
            if p.slots > rows_in_box:
                rest.wait()

    return pl.pallas_call(
        kernel,
        out_shape=jax.ShapeDtypeStruct(held.shape, jnp.float32),
        grid_spec=pltpu.PrefetchScalarGridSpec(
            num_scalar_prefetch=1,
            grid=(),
            in_specs=[IN_VMEM] * (2 + chunks * p.subs),
            out_specs=pl.BlockSpec(memory_space=pltpu.HBM),
            scratch_shapes=[
                pltpu.VMEM((p.per_group, p.order, p.order), jnp.bfloat16),
                pltpu.VMEM((ring_size, p.strip, p.order), jnp.float32),
                pltpu.SemaphoreType.DMA((ring_size,)),
                pltpu.SemaphoreType.DMA,
            ],
        ),
        compiler_params=limit(20),
        name="update",
    )(
        table,
        in_vmem(held),
        in_vmem(inverse),
        *[in_vmem(ref) for chunk in arrived for ref in chunk],
    )


def planned(p, stored_tiles, cell_owner):
    table = table_call(p, cell_owner)
    current = stored_tiles[0]
    halves = [list(range(h * p.half_tri, (h + 1) * p.half_tri)) for h in range(2)]
    swap = [(i, (i + p.half_tri) % p.tri) for i in range(p.tri)]

    def exchange(x):
        return lax.all_to_all(
            x, "tri", split_axis=0, concat_axis=0, tiled=True, axis_index_groups=halves
        )

    def arrivals(x):
        return [x] + [
            lax.ppermute(x, "sub", [((i + shift) % p.subs, i) for i in range(p.subs)])
            for shift in range(1, p.subs)
        ]

    chunks = len(p.wides)
    near, far = [], []
    for members in p.spreads:
        tiles = [tile for chunk in members for tile in p.tiles_of(chunk)]
        pieces = extract_call(p, cell_owner, current, tiles)
        spread = exchange(pieces)
        near.extend(pick_call(p, table, spread, members))
    for chunk in range(chunks):
        far.append(lax.ppermute(near[chunk], "tri", swap))
    arrived = []
    for chunk in range(chunks):
        built = build_call(p, table, near[chunk], far[chunk], p.wides[chunk], chunk == 0)
        pieces = [built[0]]
        for n in range(1, p.half_tri):
            pairs = [(i, i ^ n) for i in range(p.tri)]
            pieces.append(lax.ppermute(built[n], "tri", pairs))
        if chunk == 0:
            table_after = mark_call(p, table)
        packed = pack_call(p, table_after, pieces)
        arrived.append(arrivals(packed))
    inverse, held = inverse_call(p, table_after, arrived[0], current)
    return update_call(p, table, held, arrived, inverse)[None]


def shards(stored_tiles, cell_owner):
    p = Plan(
        lax.axis_size("tri"),
        lax.axis_size("sub"),
        stored_tiles.shape[1],
        stored_tiles.shape[2],
        stored_tiles.shape[3],
    )
    if p.tiled():
        return planned(p, stored_tiles, cell_owner)
    return untiled(stored_tiles, cell_owner)


def solution(mesh):
    placed = (P("tri", None, "sub", None), P())
    return jax.shard_map(
        shards, mesh=mesh, in_specs=placed, out_specs=P("tri", None, "sub", None), check_vma=False
    )
```

```python
import math

import jax
import jax.numpy as jnp
import numpy as np
from jax import lax
from jax.experimental import pallas as pl
from jax.experimental.pallas import tpu as pltpu
from jax.sharding import PartitionSpec as P


NB = 32


def shortened(x):

    def short(part):
        return part.astype(jnp.bfloat16) if part.dtype == jnp.float32 else part

    return jax.tree.map(short, x)


def layout(groups, per_group):
    half_group = per_group // 2
    slot_count = per_group * (per_group + 1) // 2
    row_table = np.full((groups * groups, slot_count), -1, np.int32)
    col_table = np.full((groups * groups, slot_count), -1, np.int32)
    for first_group in range(groups):
        for second_group in range(groups):
            cell_index = first_group * groups + second_group
            for inner_row in range(per_group):
                if first_group == second_group:
                    for inner_column in range(inner_row + 1):
                        slot_index = inner_row * (inner_row + 1) // 2 + inner_column
                        row_table[cell_index, slot_index] = first_group * per_group + inner_row
                        col_table[cell_index, slot_index] = first_group * per_group + inner_column
                else:
                    for inner_column in range(half_group):
                        slot_index = inner_row * half_group + inner_column
                        if first_group > second_group:
                            row_table[cell_index, slot_index] = first_group * per_group + inner_row
                            col_table[cell_index, slot_index] = (
                                second_group * per_group + inner_column
                            )
                        else:
                            row_table[cell_index, slot_index] = second_group * per_group + inner_row
                            col_table[cell_index, slot_index] = (
                                first_group * per_group + half_group + inner_column
                            )
    return (row_table, col_table)


def untiled(stored_tiles, cell_owner):
    tri_count = lax.axis_size("tri")
    groups = math.isqrt(tri_count)
    per_group = NB // groups
    half_group = per_group // 2
    strip_rows = stored_tiles.shape[2]
    block_order = stored_tiles.shape[3]
    row_table, col_table = layout(groups, per_group)
    position = lax.axis_index("tri")
    my_cell = jnp.sum(jnp.where(cell_owner == position, jnp.arange(tri_count, dtype=jnp.int32), 0))
    cell_down = my_cell // groups
    cell_across = my_cell % groups
    row_group = jnp.maximum(cell_down, cell_across)
    col_group = jnp.minimum(cell_down, cell_across)
    my_rows = jnp.asarray(row_table)[my_cell]
    my_cols = jnp.asarray(col_table)[my_cell]
    row_local = jnp.clip(my_rows - row_group * per_group, 0, per_group - 1)
    col_local = jnp.clip(my_cols - col_group * per_group, 0, per_group - 1)
    holders = cell_owner[jnp.arange(groups) * groups]
    highest = lax.Precision.HIGHEST
    current = stored_tiles[0]
    lower_slots = np.array([member * half_group for member in range(per_group)], np.int32)
    first_slots = np.array(
        [member * (member + 1) // 2 if member > 0 else 0 for member in range(per_group)], np.int32
    )
    keep_first = np.array([1.0 if member > 0 else 0.0 for member in range(per_group)], np.float32)
    from_lower = current[lower_slots]
    from_first = current[first_slots] * keep_first[:, None, None]
    holder_part = jnp.where(cell_down > 0, from_lower, from_first)
    holder_part = jnp.where(cell_across == 0, holder_part, 0.0).astype(jnp.bfloat16)
    pivot_slot = 0 // 2
    pivot_part = jnp.where(my_cell == 0, current[pivot_slot], 0.0)
    piece_size = holder_part.size // tri_count
    pivot_piece = pivot_part.size // tri_count
    spread_panel = lax.all_to_all(
        holder_part.reshape(tri_count, piece_size), "tri", split_axis=0, concat_axis=0, tiled=True
    )
    spread_pivot = lax.all_to_all(
        pivot_part.reshape(tri_count, pivot_piece).astype(jnp.bfloat16),
        "tri",
        split_axis=0,
        concat_axis=0,
        tiled=True,
    ).astype(jnp.float32)
    picked_panel = spread_panel[holders][:, None, :]
    picked_pivot = spread_pivot[holders[0]][None, :]
    whole_panel = lax.all_gather(picked_panel, "tri", axis=1, tiled=True)
    whole_pivot = lax.all_gather(
        picked_pivot.astype(jnp.bfloat16), "tri", axis=0, tiled=True
    ).astype(picked_pivot.dtype)
    panels = whole_panel.reshape(groups, per_group, strip_rows, block_order)
    pivot_strip = whole_pivot.reshape(strip_rows, block_order)
    own_strips = panels[row_group]
    other_strips = panels[col_group]
    pivot_block = lax.all_gather(
        pivot_strip.astype(jnp.bfloat16), "sub", axis=0, tiled=True
    ).astype(pivot_strip.dtype)
    partner = lax.all_gather(other_strips, "sub", axis=1, tiled=True)
    gram_matrix = jnp.dot(pivot_block.T, pivot_block, precision=highest)
    factor = jnp.linalg.cholesky(gram_matrix)
    column_count = block_order // lax.axis_size("sub")
    first_column = lax.axis_index("sub") * column_count
    columns = lax.dynamic_slice_in_dim(pivot_block.T, first_column, column_count, 1)
    column_part = jax.scipy.linalg.cho_solve((factor, True), columns)
    inverse = lax.all_gather(shortened(column_part), "sub", axis=1, tiled=True).astype(
        column_part.dtype
    )
    scaled = jnp.einsum(
        "irk,kc->irc", own_strips.astype(jnp.float32), inverse, precision=highest
    ).astype(jnp.bfloat16)
    left_slots = scaled[row_local]
    right_slots = partner[col_local]
    update = jnp.einsum("qrk,qck->qrc", left_slots, right_slots, preferred_element_type=jnp.float32)
    live_slots = (my_rows > 0) & (my_cols > 0)
    current = current + jnp.where(live_slots[:, None, None], update, 0.0)
    return current[None]


class Plan:
    def __init__(self, tri, subs, slots, strip, order):
        self.tri, self.subs, self.slots, self.strip, self.order = tri, subs, slots, strip, order
        self.groups = math.isqrt(tri)
        self.per_group = NB // self.groups
        self.half_group = self.per_group // 2
        self.half_tri = tri // 2
        self.piece = strip // self.half_tri
        quarter = self.half_group // 4
        self.wides = [quarter, quarter, 2 * quarter]
        self.firsts = [0, quarter, 2 * quarter]
        self.spreads = [[0, 1], [2]]
        self.o_sub = 0
        self.o_diag = 1
        self.o_me = 2
        self.o_dead = 3
        self.o_src = 8
        self.o_here = self.o_src + self.groups
        self.o_rg = self.o_here + self.groups
        self.o_cg = self.o_rg + self.half_tri
        self.o_hf = self.o_cg + self.half_tri
        self.size = self.o_hf + self.half_tri

    def tiled(self):
        return (
            self.piece % 16 == 0
            and self.order % 128 == 0
            and self.half_group % 4 == 0
            and self.groups * self.groups == self.tri
            and self.half_tri & (self.half_tri - 1) == 0
            and self.subs * self.strip == self.order
            and self.slots == self.per_group * (self.per_group + 1) // 2
        )

    def tiles_of(self, chunk):
        inner = range(self.firsts[chunk], self.firsts[chunk] + self.wides[chunk])
        return [half * self.half_group + n for half in range(2) for n in inner]

    def place_of(self, member):
        for chunk in range(len(self.wides)):
            if member in self.tiles_of(chunk):
                return chunk, self.tiles_of(chunk).index(member)
        raise ValueError(member)

    def column_of(self, inner):
        chunk, place = self.place_of(inner)
        return chunk, 2 * self.wides[chunk] + place


def table_call(p, cell_owner):
    def kernel(owner, out, cell_of):
        position = lax.axis_index("tri")
        for cell in range(p.tri):
            cell_of[owner[cell]] = cell

        def split(cell):
            down = cell // p.groups
            across = cell - down * p.groups
            return down, across

        down, across = split(cell_of[position])
        col_group = jnp.minimum(down, across)
        diag = down == across
        my_half = position // p.half_tri
        out[p.o_sub] = lax.axis_index("sub")
        out[p.o_me] = position - my_half * p.half_tri
        out[p.o_diag] = jnp.where(diag, 1, 0)
        for group in range(p.groups):
            holder = owner[group * p.groups]
            half = holder // p.half_tri
            out[p.o_src + group] = holder - half * p.half_tri
            out[p.o_here + group] = jnp.where(half == my_half, 1, 0)
        for end in range(p.half_tri):
            there_down, there_across = split(cell_of[my_half * p.half_tri + end])
            out[p.o_rg + end] = jnp.maximum(there_down, there_across)
            out[p.o_cg + end] = jnp.minimum(there_down, there_across)
            out[p.o_hf + end] = jnp.where(there_down < there_across, 1, 0)
        out[p.o_dead] = jnp.where((col_group == 0) & (down >= across), 1, 0)

    return pl.pallas_call(
        kernel,
        out_shape=jax.ShapeDtypeStruct((p.size,), jnp.int32),
        in_specs=[pl.BlockSpec(memory_space=pltpu.SMEM)],
        out_specs=pl.BlockSpec(memory_space=pltpu.SMEM),
        scratch_shapes=[pltpu.SMEM((p.tri,), jnp.int32)],
        name="table",
    )(cell_owner)


IN_VMEM = pl.BlockSpec(memory_space=pltpu.VMEM)


def in_vmem(x):
    return pltpu.with_memory_space_constraint(x, pltpu.VMEM)


def limit(mib):
    return pltpu.CompilerParams(vmem_limit_bytes=mib * 2**20)


def in_hbm(x):
    return pltpu.with_memory_space_constraint(x, pltpu.HBM)


def in_hbm(x):
    return pltpu.with_memory_space_constraint(x, pltpu.HBM)


def extract_call(p, cell_owner, current, members, apart):
    one = (len(members), p.piece, p.order)

    def kernel(owner, tiles, *refs):
        outs, (wide, sems) = refs[:-2], refs[-2:]
        position = lax.axis_index("tri")
        me = lax.rem(position, p.half_tri)
        cell = jnp.int32(0)
        for n in range(1, p.tri):
            cell = jnp.where(owner[n] == position, n, cell)
        down = cell // p.groups
        copies = []
        for place, member in enumerate(members):
            slot = jnp.where(down > 0, member * p.half_group, member * (member + 1) // 2)
            copies.append(
                pltpu.make_async_copy(tiles.at[slot], wide.at[place], sems.at[place])
            )
        for copy in copies:
            copy.start()
        for place, copy in enumerate(copies):
            copy.wait()
            if apart:
                for n, out in enumerate(outs):
                    at = pl.multiple_of((me ^ n) * p.piece, p.piece)
                    out[place] = wide[place, pl.ds(at, p.piece)].astype(jnp.bfloat16)
            else:
                rounded = wide[place].astype(jnp.bfloat16)
                outs[0][:, place] = rounded.reshape(p.half_tri, p.piece, p.order)

    if apart:
        out_shape = [pltpu.VMEM(one, jnp.bfloat16)] * p.half_tri
    else:
        out_shape = [pltpu.VMEM((p.half_tri,) + one, jnp.bfloat16)]
    return pl.pallas_call(
        kernel,
        out_shape=out_shape,
        in_specs=[
            pl.BlockSpec(memory_space=pltpu.SMEM),
            pl.BlockSpec(memory_space=pltpu.HBM),
        ],
        out_specs=[IN_VMEM] * len(out_shape),
        scratch_shapes=[
            pltpu.VMEM((len(members), p.strip, p.order), jnp.float32),
            pltpu.SemaphoreType.DMA((len(members),)),
        ],
        compiler_params=limit(8),
        name="extract",
    )(cell_owner, in_hbm(current))


def pick_call(p, table, spread, chunks):
    def kernel(t, *refs):
        sources, outs = refs[: len(spread)], refs[len(spread) :]
        for g in range(p.groups):
            first = 0
            for out in outs:
                count = out.shape[1]
                part = slice(first, first + count)
                first += count
                if len(sources) == 1:
                    out[g] = sources[0][t[p.o_src + g], part]
                    continue
                for n, source in enumerate(sources):

                    @pl.when(t[p.o_src + g] == t[p.o_me] ^ n)
                    def _():
                        out[g] = source[part]

    return pl.pallas_call(
        kernel,
        out_shape=[
            pltpu.VMEM((p.groups, 2 * p.wides[k], p.piece, p.order), jnp.bfloat16) for k in chunks
        ],
        grid_spec=pltpu.PrefetchScalarGridSpec(
            num_scalar_prefetch=1,
            grid=(),
            in_specs=[IN_VMEM] * len(spread),
            out_specs=[IN_VMEM] * len(chunks),
        ),
        compiler_params=limit(8),
        name="pick",
    )(table, *[in_vmem(x) for x in spread])


def build_call(p, table, near, far, wide, with_pivot):
    rows = 3 * wide + (1 if with_pivot else 0)

    def kernel(t, near_ref, far_ref, *outs):
        def part(group, first, count, out, place):
            here = t[p.o_here + group] == 1

            @pl.when(here)
            def _():
                out[place : place + count] = near_ref[group, pl.ds(first, count)]

            @pl.when(jnp.logical_not(here))
            def _():
                out[place : place + count] = far_ref[group, pl.ds(first, count)]

        for n, out in enumerate(outs):
            end = t[p.o_me] ^ n
            part(t[p.o_rg + end], 0, 2 * wide, out, 0)
            part(t[p.o_cg + end], t[p.o_hf + end] * wide, wide, out, 2 * wide)
            if with_pivot:
                part(0, 0, 1, out, 3 * wide)

    return pl.pallas_call(
        kernel,
        out_shape=[pltpu.VMEM((rows, p.piece, p.order), jnp.bfloat16)] * p.half_tri,
        grid_spec=pltpu.PrefetchScalarGridSpec(
            num_scalar_prefetch=1,
            grid=(),
            in_specs=[IN_VMEM, IN_VMEM],
            out_specs=[IN_VMEM] * p.half_tri,
        ),
        compiler_params=limit(8),
        name="build",
    )(table, in_vmem(near), in_vmem(far))


def pack_call(p, table, pieces):
    def kernel(t, *refs):
        out = refs[-1]
        for n in range(p.half_tri):
            out[t[p.o_me] ^ n] = refs[n][...]

    return pl.pallas_call(
        kernel,
        out_shape=pltpu.VMEM((p.half_tri,) + pieces[0].shape, jnp.bfloat16),
        grid_spec=pltpu.PrefetchScalarGridSpec(
            num_scalar_prefetch=1,
            grid=(),
            in_specs=[IN_VMEM] * p.half_tri,
            out_specs=IN_VMEM,
        ),
        compiler_params=limit(8),
        name="pack",
    )(table, *[in_vmem(x) for x in pieces])


def inverse_call(p, table, arrived, current):
    loads = next(n for n in (6, 5, 4, 3, 2, 1) if p.slots % n == 0)
    each = p.slots // loads
    place = 3 * p.wides[0]
    order = p.order

    def kernel(t, *refs):
        sources = refs[: p.subs]
        tiles, high, held, pivot, x_wide, x_half, e_ref, sems = refs[p.subs :]
        copies = [
            pltpu.make_async_copy(
                tiles.at[pl.ds(n * each, each)], held.at[pl.ds(n * each, each)], sems.at[n]
            )
            for n in range(loads)
        ]
        for copy in copies:
            copy.start()
        for shift in range(p.subs):
            strip = lax.rem(t[p.o_sub] + shift, p.subs) * p.strip
            at = pl.multiple_of(strip, p.strip)
            pivot[pl.ds(at, p.strip)] = sources[shift][:, place].reshape(p.strip, order)

        def dot(a, b):
            return lax.dot_general(
                a, b, (((1,), (0,)), ((), ())), preferred_element_type=jnp.float32
            )

        def eye():
            r = lax.broadcasted_iota(jnp.int32, (order, order), 0)
            c = lax.broadcasted_iota(jnp.int32, (order, order), 1)
            return jnp.where(r == c, 1.0, 0.0)

        square = -dot(pivot[...], pivot[...])
        factor = 1.9 / jnp.max(jnp.sum(jnp.abs(square), axis=1))
        residual = eye() - factor * square
        e_ref[...] = residual.astype(jnp.bfloat16)
        wide = -factor * (pivot[...].astype(jnp.float32) + dot(pivot[...], e_ref[...]))
        x_wide[...] = wide
        x_half[...] = wide.astype(jnp.bfloat16)

        def coarse_on(carry):
            step, error, before, noise = carry
            stuck = (before < 1.0) & (error > 0.5 * before)
            return (step < 60) & (error > 3e-3) & (noise < 0.1) & jnp.logical_not(stuck)

        def coarse(carry):
            step, before, _, _ = carry
            x = x_half[...]
            residual = eye() - dot(pivot[...], x)
            e_ref[...] = residual.astype(jnp.bfloat16)
            error = jnp.sum(residual * residual)
            new = x.astype(jnp.float32) + dot(x, e_ref[...])
            x_wide[...] = new
            x_half[...] = new.astype(jnp.bfloat16)
            noise = jnp.sum(new * new) / factor * 2.0**-18
            return step + 1, error, before, noise

        big = jnp.float32(1e30)
        _, reached, _, _ = lax.while_loop(
            coarse_on, coarse, (jnp.int32(0), big, big, jnp.float32(0.0))
        )

        def fine_on(carry):
            step, error, before = carry
            stuck = (before < 0.5) & (error > 0.5 * before)
            return (step < 100) & (error > 1e-4) & jnp.logical_not(stuck)

        def fine(carry):
            step, before, _ = carry
            x = x_wide[...]
            x_high = x.astype(jnp.bfloat16)
            x_low = (x - x_high.astype(jnp.float32)).astype(jnp.bfloat16)
            residual = eye() - (dot(pivot[...], x_high) + dot(pivot[...], x_low))
            error = jnp.sum(residual * residual)
            e_high = residual.astype(jnp.bfloat16)
            e_low = (residual - e_high.astype(jnp.float32)).astype(jnp.bfloat16)
            x_wide[...] = x + (dot(x_high, e_high) + (dot(x_high, e_low) + dot(x_low, e_high)))
            return step + 1, error, before

        @pl.when(jnp.logical_not(reached <= 3e-3))
        def _():
            lax.while_loop(fine_on, fine, (jnp.int32(0), big, big))

        high[...] = x_wide[...].astype(jnp.bfloat16)
        for copy in copies:
            copy.wait()

    square_shape = pltpu.VMEM((order, order), jnp.bfloat16)
    return pl.pallas_call(
        kernel,
        out_shape=(square_shape, pltpu.VMEM(current.shape, jnp.float32)),
        grid_spec=pltpu.PrefetchScalarGridSpec(
            num_scalar_prefetch=1,
            grid=(),
            in_specs=[IN_VMEM] * p.subs + [pl.BlockSpec(memory_space=pltpu.HBM)],
            out_specs=(IN_VMEM, IN_VMEM),
            scratch_shapes=[
                pltpu.VMEM((order, order), jnp.bfloat16),
                pltpu.VMEM((order, order), jnp.float32),
                pltpu.VMEM((order, order), jnp.bfloat16),
                pltpu.VMEM((order, order), jnp.bfloat16),
                pltpu.SemaphoreType.DMA((loads,)),
            ],
        ),
        compiler_params=limit(12),
        cost_estimate=pl.CostEstimate(
            flops=60 * 2 * order**3, bytes_accessed=4 * order**2, transcendentals=0
        ),
        name="inverse",
    )(table, *[in_vmem(x) for x in arrived], in_hbm(current))


def update_call(p, table, held, arrived, inverse):
    ring_size = 8
    chunks = len(p.wides)
    rows_in_box = p.per_group * p.half_group

    def kernel(t, tiles, inv, *refs):
        sources = [refs[k * p.subs : (k + 1) * p.subs] for k in range(chunks)]
        out, column, ring, ring_sems, rest_sem = refs[chunks * p.subs :]
        sub = t[p.o_sub]
        diag = t[p.o_diag] == 1
        dead = t[p.o_dead] == 1

        def strip_of(shift, chunk, place):
            return sources[chunk][shift][:, place].reshape(p.strip, p.order)

        def gather_column(j, chunk, place):
            strips = [strip_of(shift, chunk, place) for shift in range(p.subs)]
            for at in range(p.subs):
                strip = strips[0]
                for shift in range(1, p.subs):
                    here = lax.rem(sub + shift, p.subs) == at
                    strip = jnp.where(here, strips[shift], strip)
                if j == 0:
                    strip = jnp.where(dead, jnp.zeros_like(strip), strip)
                column[j, at * p.strip : (at + 1) * p.strip] = strip

        def scale(members):
            strips = [strip_of(0, *p.place_of(member)) for member in members]
            product = lax.dot_general(
                jnp.concatenate(strips, axis=0),
                inv[...],
                (((1,), (0,)), ((), ())),
                preferred_element_type=jnp.float32,
            )
            return product.astype(jnp.bfloat16)

        def times(left, j):
            return lax.dot_general(
                left, column[j], (((1,), (1,)), ((), ())), preferred_element_type=jnp.float32
            )

        class Writer:
            def __init__(self):
                self.copies = []

            def put(self, slot, product):
                n = len(self.copies)
                if n >= ring_size:
                    self.copies[n - ring_size].wait()
                ring[n % ring_size] = tiles[slot] + product
                copy = pltpu.make_async_copy(
                    ring.at[n % ring_size], out.at[slot], ring_sems.at[n % ring_size]
                )
                copy.start()
                self.copies.append(copy)

            def finish(self):
                for copy in self.copies[-ring_size:]:
                    copy.wait()

        @pl.when(diag)
        def _():
            writer = Writer()
            for i in range(0, p.per_group, 2):
                left = scale([i, i + 1])
                for j in range(i + 1):
                    if j == i:
                        gather_column(j, *p.place_of(j))
                    product = times(left, j)
                    for r in range(2):
                        slot = (i + r) * (i + r + 1) // 2 + j
                        writer.put(slot, product[r * p.strip : (r + 1) * p.strip])
                gather_column(i + 1, *p.place_of(i + 1))
                slot = (i + 1) * (i + 2) // 2 + i + 1
                writer.put(slot, times(left[p.strip :], i + 1))
            writer.finish()

        @pl.when(jnp.logical_not(diag))
        def _():
            if p.slots > rows_in_box:
                empty = pl.ds(rows_in_box, p.slots - rows_in_box)
                rest = pltpu.make_async_copy(tiles.at[empty], out.at[empty], rest_sem)
                rest.start()
            writer = Writer()
            for i in range(0, p.per_group, 2):
                left = scale([i, i + 1])
                for j in range(p.half_group):
                    if i == 0:
                        gather_column(j, *p.column_of(j))
                    product = times(left, j)
                    for r in range(2):
                        slot = (i + r) * p.half_group + j
                        writer.put(slot, product[r * p.strip : (r + 1) * p.strip])
            writer.finish()
            if p.slots > rows_in_box:
                rest.wait()

    return pl.pallas_call(
        kernel,
        out_shape=jax.ShapeDtypeStruct(held.shape, jnp.float32),
        grid_spec=pltpu.PrefetchScalarGridSpec(
            num_scalar_prefetch=1,
            grid=(),
            in_specs=[IN_VMEM] * (2 + chunks * p.subs),
            out_specs=pl.BlockSpec(memory_space=pltpu.HBM),
            scratch_shapes=[
                pltpu.VMEM((p.per_group, p.order, p.order), jnp.bfloat16),
                pltpu.VMEM((ring_size, p.strip, p.order), jnp.float32),
                pltpu.SemaphoreType.DMA((ring_size,)),
                pltpu.SemaphoreType.DMA,
            ],
        ),
        compiler_params=limit(20),
        name="update",
    )(
        table,
        in_vmem(held),
        in_vmem(inverse),
        *[in_vmem(ref) for chunk in arrived for ref in chunk],
    )


def planned(p, stored_tiles, cell_owner):
    current = stored_tiles[0]
    halves = [list(range(h * p.half_tri, (h + 1) * p.half_tri)) for h in range(2)]
    swap = [(i, (i + p.half_tri) % p.tri) for i in range(p.tri)]
    chunks = len(p.wides)

    def send(pieces):
        arrived = {0: pieces[0]}
        for n in reversed(range(1, p.half_tri)):
            pairs = [(i, i ^ n) for i in range(p.tri)]
            arrived[n] = lax.ppermute(pieces[n], "tri", pairs)
        return [arrived[n] for n in range(p.half_tri)]

    def arrivals(x):
        return [x] + [
            lax.ppermute(x, "sub", [((i + shift) % p.subs, i) for i in range(p.subs)])
            for shift in range(1, p.subs)
        ]

    table = table_call(p, cell_owner)
    near, far, arrived = [], [], []
    for number, members in enumerate(p.spreads):
        tiles = [tile for chunk in members for tile in p.tiles_of(chunk)]
        pieces = extract_call(p, cell_owner, current, tiles, number > 0)
        if number == 0:
            spread = [
                lax.all_to_all(
                    pieces[0],
                    "tri",
                    split_axis=0,
                    concat_axis=0,
                    tiled=True,
                    axis_index_groups=halves,
                )
            ]
        else:
            spread = send(pieces)
        near.extend(pick_call(p, table, spread, members))
    for chunk in range(chunks):
        far.append(lax.ppermute(near[chunk], "tri", swap))
    for chunk in range(chunks):
        built = build_call(p, table, near[chunk], far[chunk], p.wides[chunk], chunk == 0)
        pieces = send(built)
        packed = pack_call(p, table, pieces)
        arrived.append(arrivals(packed))
    inverse, held = inverse_call(p, table, arrived[0], current)
    return update_call(p, table, held, arrived, inverse)[None]


def shards(stored_tiles, cell_owner):
    p = Plan(
        lax.axis_size("tri"),
        lax.axis_size("sub"),
        stored_tiles.shape[1],
        stored_tiles.shape[2],
        stored_tiles.shape[3],
    )
    if p.tiled():
        return planned(p, stored_tiles, cell_owner)
    return untiled(stored_tiles, cell_owner)


def solution(mesh):
    placed = (P("tri", None, "sub", None), P())
    return jax.shard_map(
        shards, mesh=mesh, in_specs=placed, out_specs=P("tri", None, "sub", None), check_vma=False
    )
```

```python
import math

import jax
import jax.numpy as jnp
import numpy as np
from jax import lax
from jax.experimental import pallas as pl
from jax.experimental.pallas import tpu as pltpu
from jax.sharding import PartitionSpec as P


NB = 32


def shortened(x):

    def short(part):
        return part.astype(jnp.bfloat16) if part.dtype == jnp.float32 else part

    return jax.tree.map(short, x)


def layout(groups, per_group):
    half_group = per_group // 2
    slot_count = per_group * (per_group + 1) // 2
    row_table = np.full((groups * groups, slot_count), -1, np.int32)
    col_table = np.full((groups * groups, slot_count), -1, np.int32)
    for first_group in range(groups):
        for second_group in range(groups):
            cell_index = first_group * groups + second_group
            for inner_row in range(per_group):
                if first_group == second_group:
                    for inner_column in range(inner_row + 1):
                        slot_index = inner_row * (inner_row + 1) // 2 + inner_column
                        row_table[cell_index, slot_index] = first_group * per_group + inner_row
                        col_table[cell_index, slot_index] = first_group * per_group + inner_column
                else:
                    for inner_column in range(half_group):
                        slot_index = inner_row * half_group + inner_column
                        if first_group > second_group:
                            row_table[cell_index, slot_index] = first_group * per_group + inner_row
                            col_table[cell_index, slot_index] = (
                                second_group * per_group + inner_column
                            )
                        else:
                            row_table[cell_index, slot_index] = second_group * per_group + inner_row
                            col_table[cell_index, slot_index] = (
                                first_group * per_group + half_group + inner_column
                            )
    return (row_table, col_table)


def untiled(stored_tiles, cell_owner):
    tri_count = lax.axis_size("tri")
    groups = math.isqrt(tri_count)
    per_group = NB // groups
    half_group = per_group // 2
    strip_rows = stored_tiles.shape[2]
    block_order = stored_tiles.shape[3]
    row_table, col_table = layout(groups, per_group)
    position = lax.axis_index("tri")
    my_cell = jnp.sum(jnp.where(cell_owner == position, jnp.arange(tri_count, dtype=jnp.int32), 0))
    cell_down = my_cell // groups
    cell_across = my_cell % groups
    row_group = jnp.maximum(cell_down, cell_across)
    col_group = jnp.minimum(cell_down, cell_across)
    my_rows = jnp.asarray(row_table)[my_cell]
    my_cols = jnp.asarray(col_table)[my_cell]
    row_local = jnp.clip(my_rows - row_group * per_group, 0, per_group - 1)
    col_local = jnp.clip(my_cols - col_group * per_group, 0, per_group - 1)
    holders = cell_owner[jnp.arange(groups) * groups]
    highest = lax.Precision.HIGHEST
    current = stored_tiles[0]
    lower_slots = np.array([member * half_group for member in range(per_group)], np.int32)
    first_slots = np.array(
        [member * (member + 1) // 2 if member > 0 else 0 for member in range(per_group)], np.int32
    )
    keep_first = np.array([1.0 if member > 0 else 0.0 for member in range(per_group)], np.float32)
    from_lower = current[lower_slots]
    from_first = current[first_slots] * keep_first[:, None, None]
    holder_part = jnp.where(cell_down > 0, from_lower, from_first)
    holder_part = jnp.where(cell_across == 0, holder_part, 0.0).astype(jnp.bfloat16)
    pivot_slot = 0 // 2
    pivot_part = jnp.where(my_cell == 0, current[pivot_slot], 0.0)
    piece_size = holder_part.size // tri_count
    pivot_piece = pivot_part.size // tri_count
    spread_panel = lax.all_to_all(
        holder_part.reshape(tri_count, piece_size), "tri", split_axis=0, concat_axis=0, tiled=True
    )
    spread_pivot = lax.all_to_all(
        pivot_part.reshape(tri_count, pivot_piece).astype(jnp.bfloat16),
        "tri",
        split_axis=0,
        concat_axis=0,
        tiled=True,
    ).astype(jnp.float32)
    picked_panel = spread_panel[holders][:, None, :]
    picked_pivot = spread_pivot[holders[0]][None, :]
    whole_panel = lax.all_gather(picked_panel, "tri", axis=1, tiled=True)
    whole_pivot = lax.all_gather(
        picked_pivot.astype(jnp.bfloat16), "tri", axis=0, tiled=True
    ).astype(picked_pivot.dtype)
    panels = whole_panel.reshape(groups, per_group, strip_rows, block_order)
    pivot_strip = whole_pivot.reshape(strip_rows, block_order)
    own_strips = panels[row_group]
    other_strips = panels[col_group]
    pivot_block = lax.all_gather(
        pivot_strip.astype(jnp.bfloat16), "sub", axis=0, tiled=True
    ).astype(pivot_strip.dtype)
    partner = lax.all_gather(other_strips, "sub", axis=1, tiled=True)
    gram_matrix = jnp.dot(pivot_block.T, pivot_block, precision=highest)
    factor = jnp.linalg.cholesky(gram_matrix)
    column_count = block_order // lax.axis_size("sub")
    first_column = lax.axis_index("sub") * column_count
    columns = lax.dynamic_slice_in_dim(pivot_block.T, first_column, column_count, 1)
    column_part = jax.scipy.linalg.cho_solve((factor, True), columns)
    inverse = lax.all_gather(shortened(column_part), "sub", axis=1, tiled=True).astype(
        column_part.dtype
    )
    scaled = jnp.einsum(
        "irk,kc->irc", own_strips.astype(jnp.float32), inverse, precision=highest
    ).astype(jnp.bfloat16)
    left_slots = scaled[row_local]
    right_slots = partner[col_local]
    update = jnp.einsum("qrk,qck->qrc", left_slots, right_slots, preferred_element_type=jnp.float32)
    live_slots = (my_rows > 0) & (my_cols > 0)
    current = current + jnp.where(live_slots[:, None, None], update, 0.0)
    return current[None]


class Plan:
    def __init__(self, tri, subs, slots, strip, order):
        self.tri, self.subs, self.slots, self.strip, self.order = tri, subs, slots, strip, order
        self.groups = math.isqrt(tri)
        self.per_group = NB // self.groups
        self.half_group = self.per_group // 2
        self.half_tri = tri // 2
        self.piece = strip // self.half_tri
        quarter = self.half_group // 4
        self.wides = [quarter, quarter, 2 * quarter]
        self.firsts = [0, quarter, 2 * quarter]
        self.spreads = [[0, 1], [2]]
        self.o_sub = 0
        self.o_diag = 1
        self.o_me = 2
        self.o_dead = 3
        self.o_src = 8
        self.o_here = self.o_src + self.groups
        self.o_rg = self.o_here + self.groups
        self.o_cg = self.o_rg + self.half_tri
        self.o_hf = self.o_cg + self.half_tri
        self.size = self.o_hf + self.half_tri

    def tiled(self):
        return (
            self.piece % 16 == 0
            and self.order % 128 == 0
            and self.half_group % 4 == 0
            and self.groups * self.groups == self.tri
            and self.half_tri & (self.half_tri - 1) == 0
            and self.subs * self.strip == self.order
            and self.slots == self.per_group * (self.per_group + 1) // 2
        )

    def tiles_of(self, chunk):
        inner = range(self.firsts[chunk], self.firsts[chunk] + self.wides[chunk])
        return [half * self.half_group + n for half in range(2) for n in inner]

    def place_of(self, member):
        for chunk in range(len(self.wides)):
            if member in self.tiles_of(chunk):
                return chunk, self.tiles_of(chunk).index(member)
        raise ValueError(member)

    def column_of(self, inner):
        chunk, place = self.place_of(inner)
        return chunk, 2 * self.wides[chunk] + place


def table_call(p, cell_owner):
    def kernel(owner, out, cell_of):
        position = lax.axis_index("tri")
        for cell in range(p.tri):
            cell_of[owner[cell]] = cell

        def split(cell):
            down = cell // p.groups
            across = cell - down * p.groups
            return down, across

        down, across = split(cell_of[position])
        col_group = jnp.minimum(down, across)
        diag = down == across
        my_half = position // p.half_tri
        out[p.o_sub] = lax.axis_index("sub")
        out[p.o_me] = position - my_half * p.half_tri
        out[p.o_diag] = jnp.where(diag, 1, 0)
        for group in range(p.groups):
            holder = owner[group * p.groups]
            half = holder // p.half_tri
            out[p.o_src + group] = holder - half * p.half_tri
            out[p.o_here + group] = jnp.where(half == my_half, 1, 0)
        for end in range(p.half_tri):
            there_down, there_across = split(cell_of[my_half * p.half_tri + end])
            out[p.o_rg + end] = jnp.maximum(there_down, there_across)
            out[p.o_cg + end] = jnp.minimum(there_down, there_across)
            out[p.o_hf + end] = jnp.where(there_down < there_across, 1, 0)
        out[p.o_dead] = jnp.where((col_group == 0) & (down >= across), 1, 0)

    return pl.pallas_call(
        kernel,
        out_shape=jax.ShapeDtypeStruct((p.size,), jnp.int32),
        in_specs=[pl.BlockSpec(memory_space=pltpu.SMEM)],
        out_specs=pl.BlockSpec(memory_space=pltpu.SMEM),
        scratch_shapes=[pltpu.SMEM((p.tri,), jnp.int32)],
        name="table",
    )(cell_owner)


IN_VMEM = pl.BlockSpec(memory_space=pltpu.VMEM)


def in_vmem(x):
    return pltpu.with_memory_space_constraint(x, pltpu.VMEM)


def limit(mib):
    return pltpu.CompilerParams(vmem_limit_bytes=mib * 2**20)


def in_hbm(x):
    return pltpu.with_memory_space_constraint(x, pltpu.HBM)


def in_hbm(x):
    return pltpu.with_memory_space_constraint(x, pltpu.HBM)


def extract_call(p, cell_owner, current, members, apart):
    one = (len(members), p.piece, p.order)

    def kernel(owner, tiles, *refs):
        outs, (wide, sems) = refs[:-2], refs[-2:]
        position = lax.axis_index("tri")
        me = lax.rem(position, p.half_tri)
        cell = jnp.int32(0)
        for n in range(1, p.tri):
            cell = jnp.where(owner[n] == position, n, cell)
        down = cell // p.groups
        copies = []
        for place, member in enumerate(members):
            slot = jnp.where(down > 0, member * p.half_group, member * (member + 1) // 2)
            copies.append(
                pltpu.make_async_copy(tiles.at[slot], wide.at[place], sems.at[place])
            )
        for copy in copies:
            copy.start()
        for place, copy in enumerate(copies):
            copy.wait()
            if apart:
                for n, out in enumerate(outs):
                    at = pl.multiple_of((me ^ n) * p.piece, p.piece)
                    out[place] = wide[place, pl.ds(at, p.piece)].astype(jnp.bfloat16)
            else:
                rounded = wide[place].astype(jnp.bfloat16)
                outs[0][:, place] = rounded.reshape(p.half_tri, p.piece, p.order)

    if apart:
        out_shape = [pltpu.VMEM(one, jnp.bfloat16)] * p.half_tri
    else:
        out_shape = [pltpu.VMEM((p.half_tri,) + one, jnp.bfloat16)]
    return pl.pallas_call(
        kernel,
        out_shape=out_shape,
        in_specs=[
            pl.BlockSpec(memory_space=pltpu.SMEM),
            pl.BlockSpec(memory_space=pltpu.HBM),
        ],
        out_specs=[IN_VMEM] * len(out_shape),
        scratch_shapes=[
            pltpu.VMEM((len(members), p.strip, p.order), jnp.float32),
            pltpu.SemaphoreType.DMA((len(members),)),
        ],
        compiler_params=limit(8),
        name="extract",
    )(cell_owner, in_hbm(current))


def pick_call(p, table, spread, chunks):
    def kernel(t, *refs):
        sources, outs = refs[: len(spread)], refs[len(spread) :]
        for g in range(p.groups):
            first = 0
            for out in outs:
                count = out.shape[1]
                part = slice(first, first + count)
                first += count
                if len(sources) == 1:
                    out[g] = sources[0][t[p.o_src + g], part]
                    continue
                for n, source in enumerate(sources):

                    @pl.when(t[p.o_src + g] == t[p.o_me] ^ n)
                    def _():
                        out[g] = source[part]

    return pl.pallas_call(
        kernel,
        out_shape=[
            pltpu.VMEM((p.groups, 2 * p.wides[k], p.piece, p.order), jnp.bfloat16) for k in chunks
        ],
        grid_spec=pltpu.PrefetchScalarGridSpec(
            num_scalar_prefetch=1,
            grid=(),
            in_specs=[IN_VMEM] * len(spread),
            out_specs=[IN_VMEM] * len(chunks),
        ),
        compiler_params=limit(8),
        name="pick",
    )(table, *[in_vmem(x) for x in spread])


def build_call(p, table, near, far, wide, with_pivot):
    rows = 3 * wide + (1 if with_pivot else 0)

    def kernel(t, near_ref, far_ref, *outs):
        def part(group, first, count, out, place):
            here = t[p.o_here + group] == 1

            @pl.when(here)
            def _():
                out[place : place + count] = near_ref[group, pl.ds(first, count)]

            @pl.when(jnp.logical_not(here))
            def _():
                out[place : place + count] = far_ref[group, pl.ds(first, count)]

        for n, out in enumerate(outs):
            end = t[p.o_me] ^ n
            part(t[p.o_rg + end], 0, 2 * wide, out, 0)
            part(t[p.o_cg + end], t[p.o_hf + end] * wide, wide, out, 2 * wide)
            if with_pivot:
                part(0, 0, 1, out, 3 * wide)

    return pl.pallas_call(
        kernel,
        out_shape=[pltpu.VMEM((rows, p.piece, p.order), jnp.bfloat16)] * p.half_tri,
        grid_spec=pltpu.PrefetchScalarGridSpec(
            num_scalar_prefetch=1,
            grid=(),
            in_specs=[IN_VMEM, IN_VMEM],
            out_specs=[IN_VMEM] * p.half_tri,
        ),
        compiler_params=limit(8),
        name="build",
    )(table, in_vmem(near), in_vmem(far))


def pack_call(p, table, pieces):
    def kernel(t, *refs):
        out = refs[-1]
        for n in range(p.half_tri):
            out[t[p.o_me] ^ n] = refs[n][...]

    return pl.pallas_call(
        kernel,
        out_shape=pltpu.VMEM((p.half_tri,) + pieces[0].shape, jnp.bfloat16),
        grid_spec=pltpu.PrefetchScalarGridSpec(
            num_scalar_prefetch=1,
            grid=(),
            in_specs=[IN_VMEM] * p.half_tri,
            out_specs=IN_VMEM,
        ),
        compiler_params=limit(8),
        name="pack",
    )(table, *[in_vmem(x) for x in pieces])


def inverse_call(p, table, arrived, current):
    loads = next(n for n in (6, 5, 4, 3, 2, 1) if p.slots % n == 0)
    each = p.slots // loads
    place = 3 * p.wides[0]
    order = p.order

    def kernel(t, *refs):
        sources = refs[: p.subs]
        tiles, high, held, pivot, x_wide, x_half, e_ref, sems = refs[p.subs :]
        copies = [
            pltpu.make_async_copy(
                tiles.at[pl.ds(n * each, each)], held.at[pl.ds(n * each, each)], sems.at[n]
            )
            for n in range(loads)
        ]
        for copy in copies:
            copy.start()
        for shift in range(p.subs):
            strip = lax.rem(t[p.o_sub] + shift, p.subs) * p.strip
            at = pl.multiple_of(strip, p.strip)
            pivot[pl.ds(at, p.strip)] = sources[shift][:, place].reshape(p.strip, order)

        def dot(a, b):
            return lax.dot_general(
                a, b, (((1,), (0,)), ((), ())), preferred_element_type=jnp.float32
            )

        def eye():
            r = lax.broadcasted_iota(jnp.int32, (order, order), 0)
            c = lax.broadcasted_iota(jnp.int32, (order, order), 1)
            return jnp.where(r == c, 1.0, 0.0)

        square = -dot(pivot[...], pivot[...])
        factor = 1.9 / jnp.max(jnp.sum(jnp.abs(square), axis=1))
        residual = eye() - factor * square
        e_ref[...] = residual.astype(jnp.bfloat16)
        wide = -factor * (pivot[...].astype(jnp.float32) + dot(pivot[...], e_ref[...]))
        x_wide[...] = wide
        x_half[...] = wide.astype(jnp.bfloat16)

        def coarse_on(carry):
            step, error, before, noise = carry
            stuck = (before < 1.0) & (error > 0.5 * before)
            return (step < 60) & (error > 3e-3) & (noise < 0.1) & jnp.logical_not(stuck)

        def coarse(carry):
            step, before, _, _ = carry
            x = x_half[...]
            residual = eye() - dot(pivot[...], x)
            e_ref[...] = residual.astype(jnp.bfloat16)
            error = jnp.sum(residual * residual)
            new = x.astype(jnp.float32) + dot(x, e_ref[...])
            x_wide[...] = new
            x_half[...] = new.astype(jnp.bfloat16)
            noise = jnp.sum(new * new) / factor * 2.0**-18
            return step + 1, error, before, noise

        big = jnp.float32(1e30)
        _, reached, _, _ = lax.while_loop(
            coarse_on, coarse, (jnp.int32(0), big, big, jnp.float32(0.0))
        )

        def fine_on(carry):
            step, error, before = carry
            stuck = (before < 0.5) & (error > 0.5 * before)
            return (step < 100) & (error > 1e-4) & jnp.logical_not(stuck)

        def fine(carry):
            step, before, _ = carry
            x = x_wide[...]
            x_high = x.astype(jnp.bfloat16)
            x_low = (x - x_high.astype(jnp.float32)).astype(jnp.bfloat16)
            residual = eye() - (dot(pivot[...], x_high) + dot(pivot[...], x_low))
            error = jnp.sum(residual * residual)
            e_high = residual.astype(jnp.bfloat16)
            e_low = (residual - e_high.astype(jnp.float32)).astype(jnp.bfloat16)
            x_wide[...] = x + (dot(x_high, e_high) + (dot(x_high, e_low) + dot(x_low, e_high)))
            return step + 1, error, before

        @pl.when(jnp.logical_not(reached <= 3e-3))
        def _():
            lax.while_loop(fine_on, fine, (jnp.int32(0), big, big))

        high[...] = x_wide[...].astype(jnp.bfloat16)
        for copy in copies:
            copy.wait()

    square_shape = pltpu.VMEM((order, order), jnp.bfloat16)
    return pl.pallas_call(
        kernel,
        out_shape=(square_shape, pltpu.VMEM(current.shape, jnp.float32)),
        grid_spec=pltpu.PrefetchScalarGridSpec(
            num_scalar_prefetch=1,
            grid=(),
            in_specs=[IN_VMEM] * p.subs + [pl.BlockSpec(memory_space=pltpu.HBM)],
            out_specs=(IN_VMEM, IN_VMEM),
            scratch_shapes=[
                pltpu.VMEM((order, order), jnp.bfloat16),
                pltpu.VMEM((order, order), jnp.float32),
                pltpu.VMEM((order, order), jnp.bfloat16),
                pltpu.VMEM((order, order), jnp.bfloat16),
                pltpu.SemaphoreType.DMA((loads,)),
            ],
        ),
        compiler_params=limit(12),
        cost_estimate=pl.CostEstimate(
            flops=60 * 2 * order**3, bytes_accessed=4 * order**2, transcendentals=0
        ),
        name="inverse",
    )(table, *[in_vmem(x) for x in arrived], in_hbm(current))


def update_call(p, table, held, arrived, inverse, before):
    ring_size = 8
    chunks = len(p.wides)
    early = before is None
    rows_in_box = p.per_group * p.half_group

    def mine(i, j):
        first = max(p.place_of(i)[0], p.place_of(j)[0]) < chunks - 1
        return first == early

    def kernel(t, tiles, inv, *refs):
        at_hand = len(arrived)
        sources = [refs[k * p.subs : (k + 1) * p.subs] for k in range(at_hand)]
        out, column, ring, ring_sems, rest_sem = refs[-5:]
        sub = t[p.o_sub]
        diag = t[p.o_diag] == 1
        dead = t[p.o_dead] == 1

        def strip_of(shift, chunk, place):
            return sources[chunk][shift][:, place].reshape(p.strip, p.order)

        def gather_column(j, chunk, place):
            strips = [strip_of(shift, chunk, place) for shift in range(p.subs)]
            for at in range(p.subs):
                strip = strips[0]
                for shift in range(1, p.subs):
                    here = lax.rem(sub + shift, p.subs) == at
                    strip = jnp.where(here, strips[shift], strip)
                if j == 0:
                    strip = jnp.where(dead, jnp.zeros_like(strip), strip)
                column[j, at * p.strip : (at + 1) * p.strip] = strip

        def scale(members):
            strips = [strip_of(0, *p.place_of(member)) for member in members]
            product = lax.dot_general(
                jnp.concatenate(strips, axis=0),
                inv[...],
                (((1,), (0,)), ((), ())),
                preferred_element_type=jnp.float32,
            )
            return product.astype(jnp.bfloat16)

        def times(left, j):
            return lax.dot_general(
                left, column[j], (((1,), (1,)), ((), ())), preferred_element_type=jnp.float32
            )

        class Writer:
            def __init__(self):
                self.copies = []

            def put(self, slot, product):
                n = len(self.copies)
                if n >= ring_size:
                    self.copies[n - ring_size].wait()
                ring[n % ring_size] = tiles[slot] + product
                copy = pltpu.make_async_copy(
                    ring.at[n % ring_size], out.at[slot], ring_sems.at[n % ring_size]
                )
                copy.start()
                self.copies.append(copy)

            def finish(self):
                for copy in self.copies[-ring_size:]:
                    copy.wait()

        @pl.when(diag)
        def _():
            writer = Writer()
            known = set()

            def column_at(j):
                if j not in known:
                    known.add(j)
                    gather_column(j, *p.place_of(j))

            for i in range(0, p.per_group, 2):
                columns = [j for j in range(i + 2) if mine(i, j)]
                if not columns:
                    continue
                left = scale([i, i + 1])
                for j in columns:
                    column_at(j)
                    if j <= i:
                        product = times(left, j)
                        for r in range(2):
                            slot = (i + r) * (i + r + 1) // 2 + j
                            writer.put(slot, product[r * p.strip : (r + 1) * p.strip])
                    else:
                        slot = (i + 1) * (i + 2) // 2 + j
                        writer.put(slot, times(left[p.strip :], j))
            writer.finish()

        @pl.when(jnp.logical_not(diag))
        def _():
            empty = p.slots - rows_in_box if early else 0
            if empty:
                at = pl.ds(rows_in_box, empty)
                rest = pltpu.make_async_copy(tiles.at[at], out.at[at], rest_sem)
                rest.start()
            writer = Writer()
            known = set()
            for i in range(0, p.per_group, 2):
                columns = [j for j in range(p.half_group) if mine(i, j)]
                if not columns:
                    continue
                left = scale([i, i + 1])
                for j in columns:
                    if j not in known:
                        known.add(j)
                        gather_column(j, *p.column_of(j))
                    product = times(left, j)
                    for r in range(2):
                        slot = (i + r) * p.half_group + j
                        writer.put(slot, product[r * p.strip : (r + 1) * p.strip])
            writer.finish()
            if empty:
                rest.wait()

    hbm = pl.BlockSpec(memory_space=pltpu.HBM)
    delivered = [in_vmem(ref) for chunk in arrived for ref in chunk]
    specs = [IN_VMEM] * (2 + len(delivered))
    return pl.pallas_call(
        kernel,
        out_shape=jax.ShapeDtypeStruct(held.shape, jnp.float32),
        grid_spec=pltpu.PrefetchScalarGridSpec(
            num_scalar_prefetch=1,
            grid=(),
            in_specs=specs if early else specs + [hbm],
            out_specs=hbm,
            scratch_shapes=[
                pltpu.VMEM((p.per_group, p.order, p.order), jnp.bfloat16),
                pltpu.VMEM((ring_size, p.strip, p.order), jnp.float32),
                pltpu.SemaphoreType.DMA((ring_size,)),
                pltpu.SemaphoreType.DMA,
            ],
        ),
        input_output_aliases={} if early else {3 + len(delivered): 0},
        compiler_params=limit(20),
        name="begin" if early else "finish",
    )(
        table,
        in_vmem(held),
        in_vmem(inverse),
        *delivered,
        *([] if early else [before]),
    )


def planned(p, stored_tiles, cell_owner):
    current = stored_tiles[0]
    halves = [list(range(h * p.half_tri, (h + 1) * p.half_tri)) for h in range(2)]
    swap = [(i, (i + p.half_tri) % p.tri) for i in range(p.tri)]
    chunks = len(p.wides)

    def send(pieces):
        arrived = {0: pieces[0]}
        for n in reversed(range(1, p.half_tri)):
            pairs = [(i, i ^ n) for i in range(p.tri)]
            arrived[n] = lax.ppermute(pieces[n], "tri", pairs)
        return [arrived[n] for n in range(p.half_tri)]

    def arrivals(x):
        return [x] + [
            lax.ppermute(x, "sub", [((i + shift) % p.subs, i) for i in range(p.subs)])
            for shift in range(1, p.subs)
        ]

    table = table_call(p, cell_owner)
    near, far, arrived = [], [], []
    for number, members in enumerate(p.spreads):
        tiles = [tile for chunk in members for tile in p.tiles_of(chunk)]
        pieces = extract_call(p, cell_owner, current, tiles, number > 0)
        if number == 0:
            spread = [
                lax.all_to_all(
                    pieces[0],
                    "tri",
                    split_axis=0,
                    concat_axis=0,
                    tiled=True,
                    axis_index_groups=halves,
                )
            ]
        else:
            spread = send(pieces)
        near.extend(pick_call(p, table, spread, members))
    for chunk in range(chunks):
        far.append(lax.ppermute(near[chunk], "tri", swap))
    for chunk in range(chunks):
        built = build_call(p, table, near[chunk], far[chunk], p.wides[chunk], chunk == 0)
        pieces = send(built)
        packed = pack_call(p, table, pieces)
        arrived.append(arrivals(packed))
    inverse, held = inverse_call(p, table, arrived[0], current)
    begun = update_call(p, table, held, arrived[:-1], inverse, None)
    return update_call(p, table, held, arrived, inverse, begun)[None]


def shards(stored_tiles, cell_owner):
    p = Plan(
        lax.axis_size("tri"),
        lax.axis_size("sub"),
        stored_tiles.shape[1],
        stored_tiles.shape[2],
        stored_tiles.shape[3],
    )
    if p.tiled():
        return planned(p, stored_tiles, cell_owner)
    return untiled(stored_tiles, cell_owner)


def solution(mesh):
    placed = (P("tri", None, "sub", None), P())
    return jax.shard_map(
        shards, mesh=mesh, in_specs=placed, out_specs=P("tri", None, "sub", None), check_vma=False
    )
```

```python
import math

import jax
import jax.numpy as jnp
import numpy as np
from jax import lax
from jax.experimental import pallas as pl
from jax.experimental.pallas import tpu as pltpu
from jax.sharding import PartitionSpec as P


NB = 32


def shortened(x):

    def short(part):
        return part.astype(jnp.bfloat16) if part.dtype == jnp.float32 else part

    return jax.tree.map(short, x)


def layout(groups, per_group):
    half_group = per_group // 2
    slot_count = per_group * (per_group + 1) // 2
    row_table = np.full((groups * groups, slot_count), -1, np.int32)
    col_table = np.full((groups * groups, slot_count), -1, np.int32)
    for first_group in range(groups):
        for second_group in range(groups):
            cell_index = first_group * groups + second_group
            for inner_row in range(per_group):
                if first_group == second_group:
                    for inner_column in range(inner_row + 1):
                        slot_index = inner_row * (inner_row + 1) // 2 + inner_column
                        row_table[cell_index, slot_index] = first_group * per_group + inner_row
                        col_table[cell_index, slot_index] = first_group * per_group + inner_column
                else:
                    for inner_column in range(half_group):
                        slot_index = inner_row * half_group + inner_column
                        if first_group > second_group:
                            row_table[cell_index, slot_index] = first_group * per_group + inner_row
                            col_table[cell_index, slot_index] = (
                                second_group * per_group + inner_column
                            )
                        else:
                            row_table[cell_index, slot_index] = second_group * per_group + inner_row
                            col_table[cell_index, slot_index] = (
                                first_group * per_group + half_group + inner_column
                            )
    return (row_table, col_table)


def untiled(stored_tiles, cell_owner):
    tri_count = lax.axis_size("tri")
    groups = math.isqrt(tri_count)
    per_group = NB // groups
    half_group = per_group // 2
    strip_rows = stored_tiles.shape[2]
    block_order = stored_tiles.shape[3]
    row_table, col_table = layout(groups, per_group)
    position = lax.axis_index("tri")
    my_cell = jnp.sum(jnp.where(cell_owner == position, jnp.arange(tri_count, dtype=jnp.int32), 0))
    cell_down = my_cell // groups
    cell_across = my_cell % groups
    row_group = jnp.maximum(cell_down, cell_across)
    col_group = jnp.minimum(cell_down, cell_across)
    my_rows = jnp.asarray(row_table)[my_cell]
    my_cols = jnp.asarray(col_table)[my_cell]
    row_local = jnp.clip(my_rows - row_group * per_group, 0, per_group - 1)
    col_local = jnp.clip(my_cols - col_group * per_group, 0, per_group - 1)
    holders = cell_owner[jnp.arange(groups) * groups]
    highest = lax.Precision.HIGHEST
    current = stored_tiles[0]
    lower_slots = np.array([member * half_group for member in range(per_group)], np.int32)
    first_slots = np.array(
        [member * (member + 1) // 2 if member > 0 else 0 for member in range(per_group)], np.int32
    )
    keep_first = np.array([1.0 if member > 0 else 0.0 for member in range(per_group)], np.float32)
    from_lower = current[lower_slots]
    from_first = current[first_slots] * keep_first[:, None, None]
    holder_part = jnp.where(cell_down > 0, from_lower, from_first)
    holder_part = jnp.where(cell_across == 0, holder_part, 0.0).astype(jnp.bfloat16)
    pivot_slot = 0 // 2
    pivot_part = jnp.where(my_cell == 0, current[pivot_slot], 0.0)
    piece_size = holder_part.size // tri_count
    pivot_piece = pivot_part.size // tri_count
    spread_panel = lax.all_to_all(
        holder_part.reshape(tri_count, piece_size), "tri", split_axis=0, concat_axis=0, tiled=True
    )
    spread_pivot = lax.all_to_all(
        pivot_part.reshape(tri_count, pivot_piece).astype(jnp.bfloat16),
        "tri",
        split_axis=0,
        concat_axis=0,
        tiled=True,
    ).astype(jnp.float32)
    picked_panel = spread_panel[holders][:, None, :]
    picked_pivot = spread_pivot[holders[0]][None, :]
    whole_panel = lax.all_gather(picked_panel, "tri", axis=1, tiled=True)
    whole_pivot = lax.all_gather(
        picked_pivot.astype(jnp.bfloat16), "tri", axis=0, tiled=True
    ).astype(picked_pivot.dtype)
    panels = whole_panel.reshape(groups, per_group, strip_rows, block_order)
    pivot_strip = whole_pivot.reshape(strip_rows, block_order)
    own_strips = panels[row_group]
    other_strips = panels[col_group]
    pivot_block = lax.all_gather(
        pivot_strip.astype(jnp.bfloat16), "sub", axis=0, tiled=True
    ).astype(pivot_strip.dtype)
    partner = lax.all_gather(other_strips, "sub", axis=1, tiled=True)
    gram_matrix = jnp.dot(pivot_block.T, pivot_block, precision=highest)
    factor = jnp.linalg.cholesky(gram_matrix)
    column_count = block_order // lax.axis_size("sub")
    first_column = lax.axis_index("sub") * column_count
    columns = lax.dynamic_slice_in_dim(pivot_block.T, first_column, column_count, 1)
    column_part = jax.scipy.linalg.cho_solve((factor, True), columns)
    inverse = lax.all_gather(shortened(column_part), "sub", axis=1, tiled=True).astype(
        column_part.dtype
    )
    scaled = jnp.einsum(
        "irk,kc->irc", own_strips.astype(jnp.float32), inverse, precision=highest
    ).astype(jnp.bfloat16)
    left_slots = scaled[row_local]
    right_slots = partner[col_local]
    update = jnp.einsum("qrk,qck->qrc", left_slots, right_slots, preferred_element_type=jnp.float32)
    live_slots = (my_rows > 0) & (my_cols > 0)
    current = current + jnp.where(live_slots[:, None, None], update, 0.0)
    return current[None]


class Plan:
    def __init__(self, tri, subs, slots, strip, order):
        self.tri, self.subs, self.slots, self.strip, self.order = tri, subs, slots, strip, order
        self.groups = math.isqrt(tri)
        self.per_group = NB // self.groups
        self.half_group = self.per_group // 2
        self.half_tri = tri // 2
        self.piece = strip // self.half_tri
        self.quarter = self.half_group // 4
        self.spreads = [[0, 1], [2, 3]]
        self.deliveries = [[0], [1, 2], [3]]
        self.o_sub = 0
        self.o_diag = 1
        self.o_me = 2
        self.o_dead = 3
        self.o_src = 8
        self.o_here = self.o_src + self.groups
        self.o_rg = self.o_here + self.groups
        self.o_cg = self.o_rg + self.half_tri
        self.o_hf = self.o_cg + self.half_tri
        self.size = self.o_hf + self.half_tri

    def tiled(self):
        return (
            self.piece % 16 == 0
            and self.order % 128 == 0
            and self.half_group % 4 == 0
            and self.groups * self.groups == self.tri
            and self.half_tri & (self.half_tri - 1) == 0
            and self.subs * self.strip == self.order
            and self.slots == self.per_group * (self.per_group + 1) // 2
        )

    def tiles_of(self, unit):
        inner = range(unit * self.quarter, (unit + 1) * self.quarter)
        return [half * self.half_group + n for half in range(2) for n in inner]

    def unit_of(self, inner):
        unit, rest = divmod(inner, self.quarter)
        for chunk, units in enumerate(self.deliveries):
            if unit in units:
                return chunk, 3 * self.quarter * units.index(unit), rest
        raise ValueError(inner)

    def place_of(self, member):
        half, inner = divmod(member, self.half_group)
        chunk, first, rest = self.unit_of(inner)
        return chunk, first + half * self.quarter + rest

    def column_of(self, inner):
        chunk, first, rest = self.unit_of(inner)
        return chunk, first + 2 * self.quarter + rest


def table_call(p, cell_owner):
    def kernel(owner, out, cell_of):
        position = lax.axis_index("tri")
        for cell in range(p.tri):
            cell_of[owner[cell]] = cell

        def split(cell):
            down = cell // p.groups
            across = cell - down * p.groups
            return down, across

        down, across = split(cell_of[position])
        col_group = jnp.minimum(down, across)
        diag = down == across
        my_half = position // p.half_tri
        out[p.o_sub] = lax.axis_index("sub")
        out[p.o_me] = position - my_half * p.half_tri
        out[p.o_diag] = jnp.where(diag, 1, 0)
        for group in range(p.groups):
            holder = owner[group * p.groups]
            half = holder // p.half_tri
            out[p.o_src + group] = holder - half * p.half_tri
            out[p.o_here + group] = jnp.where(half == my_half, 1, 0)
        for end in range(p.half_tri):
            there_down, there_across = split(cell_of[my_half * p.half_tri + end])
            out[p.o_rg + end] = jnp.maximum(there_down, there_across)
            out[p.o_cg + end] = jnp.minimum(there_down, there_across)
            out[p.o_hf + end] = jnp.where(there_down < there_across, 1, 0)
        out[p.o_dead] = jnp.where((col_group == 0) & (down >= across), 1, 0)

    return pl.pallas_call(
        kernel,
        out_shape=jax.ShapeDtypeStruct((p.size,), jnp.int32),
        in_specs=[pl.BlockSpec(memory_space=pltpu.SMEM)],
        out_specs=pl.BlockSpec(memory_space=pltpu.SMEM),
        scratch_shapes=[pltpu.SMEM((p.tri,), jnp.int32)],
        name="table",
    )(cell_owner)


IN_VMEM = pl.BlockSpec(memory_space=pltpu.VMEM)


def in_vmem(x):
    return pltpu.with_memory_space_constraint(x, pltpu.VMEM)


def limit(mib):
    return pltpu.CompilerParams(vmem_limit_bytes=mib * 2**20)


def in_hbm(x):
    return pltpu.with_memory_space_constraint(x, pltpu.HBM)


def in_hbm(x):
    return pltpu.with_memory_space_constraint(x, pltpu.HBM)


def extract_call(p, cell_owner, current, members, apart):
    one = (len(members), p.piece, p.order)

    def kernel(owner, tiles, *refs):
        outs, (wide, sems) = refs[:-2], refs[-2:]
        position = lax.axis_index("tri")
        me = lax.rem(position, p.half_tri)
        cell = jnp.int32(0)
        for n in range(1, p.tri):
            cell = jnp.where(owner[n] == position, n, cell)
        down = cell // p.groups
        copies = []
        for place, member in enumerate(members):
            slot = jnp.where(down > 0, member * p.half_group, member * (member + 1) // 2)
            copies.append(
                pltpu.make_async_copy(tiles.at[slot], wide.at[place], sems.at[place])
            )
        for copy in copies:
            copy.start()
        for place, copy in enumerate(copies):
            copy.wait()
            if apart:
                for n, out in enumerate(outs):
                    at = pl.multiple_of((me ^ n) * p.piece, p.piece)
                    out[place] = wide[place, pl.ds(at, p.piece)].astype(jnp.bfloat16)
            else:
                rounded = wide[place].astype(jnp.bfloat16)
                outs[0][:, place] = rounded.reshape(p.half_tri, p.piece, p.order)

    if apart:
        out_shape = [pltpu.VMEM(one, jnp.bfloat16)] * p.half_tri
    else:
        out_shape = [pltpu.VMEM((p.half_tri,) + one, jnp.bfloat16)]
    return pl.pallas_call(
        kernel,
        out_shape=out_shape,
        in_specs=[
            pl.BlockSpec(memory_space=pltpu.SMEM),
            pl.BlockSpec(memory_space=pltpu.HBM),
        ],
        out_specs=[IN_VMEM] * len(out_shape),
        scratch_shapes=[
            pltpu.VMEM((len(members), p.strip, p.order), jnp.float32),
            pltpu.SemaphoreType.DMA((len(members),)),
        ],
        compiler_params=limit(8),
        name="extract",
    )(cell_owner, in_hbm(current))


def pick_call(p, table, spread, units):
    def kernel(t, *refs):
        sources, outs = refs[: len(spread)], refs[len(spread) :]
        for g in range(p.groups):
            first = 0
            for out in outs:
                count = out.shape[1]
                part = slice(first, first + count)
                first += count
                if len(sources) == 1:
                    out[g] = sources[0][t[p.o_src + g], part]
                    continue
                for n, source in enumerate(sources):

                    @pl.when(t[p.o_src + g] == t[p.o_me] ^ n)
                    def _():
                        out[g] = source[part]

    return pl.pallas_call(
        kernel,
        out_shape=[
            pltpu.VMEM((p.groups, 2 * p.quarter, p.piece, p.order), jnp.bfloat16) for _ in units
        ],
        grid_spec=pltpu.PrefetchScalarGridSpec(
            num_scalar_prefetch=1,
            grid=(),
            in_specs=[IN_VMEM] * len(spread),
            out_specs=[IN_VMEM] * len(units),
        ),
        compiler_params=limit(8),
        name="pick",
    )(table, *[in_vmem(x) for x in spread])


def build_call(p, table, near, far, with_pivot):
    wide = p.quarter
    rows = 3 * wide * len(near) + (1 if with_pivot else 0)

    def kernel(t, *refs):
        near_refs, far_refs = refs[: len(near)], refs[len(near) : 2 * len(near)]
        outs = refs[2 * len(near) :]

        def part(unit, group, first, count, out, place):
            here = t[p.o_here + group] == 1

            @pl.when(here)
            def _():
                out[place : place + count] = near_refs[unit][group, pl.ds(first, count)]

            @pl.when(jnp.logical_not(here))
            def _():
                out[place : place + count] = far_refs[unit][group, pl.ds(first, count)]

        for n, out in enumerate(outs):
            end = t[p.o_me] ^ n
            for unit in range(len(near)):
                at = 3 * wide * unit
                part(unit, t[p.o_rg + end], 0, 2 * wide, out, at)
                part(unit, t[p.o_cg + end], t[p.o_hf + end] * wide, wide, out, at + 2 * wide)
            if with_pivot:
                part(0, 0, 0, 1, out, rows - 1)

    return pl.pallas_call(
        kernel,
        out_shape=[pltpu.VMEM((rows, p.piece, p.order), jnp.bfloat16)] * p.half_tri,
        grid_spec=pltpu.PrefetchScalarGridSpec(
            num_scalar_prefetch=1,
            grid=(),
            in_specs=[IN_VMEM] * (2 * len(near)),
            out_specs=[IN_VMEM] * p.half_tri,
        ),
        compiler_params=limit(8),
        name="build",
    )(table, *[in_vmem(x) for x in near], *[in_vmem(x) for x in far])


def pack_call(p, table, pieces):
    def kernel(t, *refs):
        out = refs[-1]
        for n in range(p.half_tri):
            out[t[p.o_me] ^ n] = refs[n][...]

    return pl.pallas_call(
        kernel,
        out_shape=pltpu.VMEM((p.half_tri,) + pieces[0].shape, jnp.bfloat16),
        grid_spec=pltpu.PrefetchScalarGridSpec(
            num_scalar_prefetch=1,
            grid=(),
            in_specs=[IN_VMEM] * p.half_tri,
            out_specs=IN_VMEM,
        ),
        compiler_params=limit(8),
        name="pack",
    )(table, *[in_vmem(x) for x in pieces])


def inverse_call(p, table, arrived, current):
    loads = next(n for n in (6, 5, 4, 3, 2, 1) if p.slots % n == 0)
    each = p.slots // loads
    place = 3 * p.quarter * len(p.deliveries[0])
    order = p.order

    def kernel(t, *refs):
        sources = refs[: p.subs]
        tiles, high, held, pivot, x_wide, x_half, e_ref, sems = refs[p.subs :]
        copies = [
            pltpu.make_async_copy(
                tiles.at[pl.ds(n * each, each)], held.at[pl.ds(n * each, each)], sems.at[n]
            )
            for n in range(loads)
        ]
        for copy in copies:
            copy.start()
        for shift in range(p.subs):
            strip = lax.rem(t[p.o_sub] + shift, p.subs) * p.strip
            at = pl.multiple_of(strip, p.strip)
            pivot[pl.ds(at, p.strip)] = sources[shift][:, place].reshape(p.strip, order)

        def dot(a, b):
            return lax.dot_general(
                a, b, (((1,), (0,)), ((), ())), preferred_element_type=jnp.float32
            )

        def eye():
            r = lax.broadcasted_iota(jnp.int32, (order, order), 0)
            c = lax.broadcasted_iota(jnp.int32, (order, order), 1)
            return jnp.where(r == c, 1.0, 0.0)

        square = -dot(pivot[...], pivot[...])
        factor = 1.9 / jnp.max(jnp.sum(jnp.abs(square), axis=1))
        residual = eye() - factor * square
        e_ref[...] = residual.astype(jnp.bfloat16)
        wide = -factor * (pivot[...].astype(jnp.float32) + dot(pivot[...], e_ref[...]))
        x_wide[...] = wide
        x_half[...] = wide.astype(jnp.bfloat16)

        def coarse_on(carry):
            step, error, before, noise = carry
            stuck = (before < 1.0) & (error > 0.5 * before)
            return (step < 60) & (error > 3e-3) & (noise < 0.1) & jnp.logical_not(stuck)

        def coarse(carry):
            step, before, _, _ = carry
            x = x_half[...]
            residual = eye() - dot(pivot[...], x)
            e_ref[...] = residual.astype(jnp.bfloat16)
            error = jnp.sum(residual * residual)
            new = x.astype(jnp.float32) + dot(x, e_ref[...])
            x_wide[...] = new
            x_half[...] = new.astype(jnp.bfloat16)
            noise = jnp.sum(new * new) / factor * 2.0**-18
            return step + 1, error, before, noise

        big = jnp.float32(1e30)
        _, reached, _, _ = lax.while_loop(
            coarse_on, coarse, (jnp.int32(0), big, big, jnp.float32(0.0))
        )

        def fine_on(carry):
            step, error, before = carry
            stuck = (before < 0.5) & (error > 0.5 * before)
            return (step < 100) & (error > 1e-4) & jnp.logical_not(stuck)

        def fine(carry):
            step, before, _ = carry
            x = x_wide[...]
            x_high = x.astype(jnp.bfloat16)
            x_low = (x - x_high.astype(jnp.float32)).astype(jnp.bfloat16)
            residual = eye() - (dot(pivot[...], x_high) + dot(pivot[...], x_low))
            error = jnp.sum(residual * residual)
            e_high = residual.astype(jnp.bfloat16)
            e_low = (residual - e_high.astype(jnp.float32)).astype(jnp.bfloat16)
            x_wide[...] = x + (dot(x_high, e_high) + (dot(x_high, e_low) + dot(x_low, e_high)))
            return step + 1, error, before

        @pl.when(jnp.logical_not(reached <= 3e-3))
        def _():
            lax.while_loop(fine_on, fine, (jnp.int32(0), big, big))

        high[...] = x_wide[...].astype(jnp.bfloat16)
        for copy in copies:
            copy.wait()

    square_shape = pltpu.VMEM((order, order), jnp.bfloat16)
    return pl.pallas_call(
        kernel,
        out_shape=(square_shape, pltpu.VMEM(current.shape, jnp.float32)),
        grid_spec=pltpu.PrefetchScalarGridSpec(
            num_scalar_prefetch=1,
            grid=(),
            in_specs=[IN_VMEM] * p.subs + [pl.BlockSpec(memory_space=pltpu.HBM)],
            out_specs=(IN_VMEM, IN_VMEM),
            scratch_shapes=[
                pltpu.VMEM((order, order), jnp.bfloat16),
                pltpu.VMEM((order, order), jnp.float32),
                pltpu.VMEM((order, order), jnp.bfloat16),
                pltpu.VMEM((order, order), jnp.bfloat16),
                pltpu.SemaphoreType.DMA((loads,)),
            ],
        ),
        compiler_params=limit(12),
        cost_estimate=pl.CostEstimate(
            flops=60 * 2 * order**3, bytes_accessed=4 * order**2, transcendentals=0
        ),
        name="inverse",
    )(table, *[in_vmem(x) for x in arrived], in_hbm(current))


def update_call(p, table, held, arrived, inverse, before):
    ring_size = 8
    chunks = len(p.deliveries)
    early = before is None
    rows_in_box = p.per_group * p.half_group

    members = range(p.per_group)
    known_first = [i for i in members if p.place_of(i)[0] < chunks - 1]
    known_last = [i for i in members if i not in known_first]
    row_sets = [some[n : n + 2] for some in (known_first, known_last) for n in range(0, len(some), 2)]

    def mine(i, j):
        first = max(p.place_of(i)[0], p.place_of(j)[0]) < chunks - 1
        return first == early

    def kernel(t, tiles, inv, *refs):
        at_hand = len(arrived)
        sources = [refs[k * p.subs : (k + 1) * p.subs] for k in range(at_hand)]
        out, column, ring, ring_sems, rest_sem = refs[-5:]
        sub = t[p.o_sub]
        diag = t[p.o_diag] == 1
        dead = t[p.o_dead] == 1

        def strip_of(shift, chunk, place):
            return sources[chunk][shift][:, place].reshape(p.strip, p.order)

        def gather_column(j, chunk, place):
            strips = [strip_of(shift, chunk, place) for shift in range(p.subs)]
            for at in range(p.subs):
                strip = strips[0]
                for shift in range(1, p.subs):
                    here = lax.rem(sub + shift, p.subs) == at
                    strip = jnp.where(here, strips[shift], strip)
                if j == 0:
                    strip = jnp.where(dead, jnp.zeros_like(strip), strip)
                column[j, at * p.strip : (at + 1) * p.strip] = strip

        def scale(members):
            strips = [strip_of(0, *p.place_of(member)) for member in members]
            product = lax.dot_general(
                jnp.concatenate(strips, axis=0),
                inv[...],
                (((1,), (0,)), ((), ())),
                preferred_element_type=jnp.float32,
            )
            return product.astype(jnp.bfloat16)

        def times(left, j):
            return lax.dot_general(
                left, column[j], (((1,), (1,)), ((), ())), preferred_element_type=jnp.float32
            )

        class Writer:
            def __init__(self):
                self.copies = []

            def put(self, slot, product):
                n = len(self.copies)
                if n >= ring_size:
                    self.copies[n - ring_size].wait()
                ring[n % ring_size] = tiles[slot] + product
                copy = pltpu.make_async_copy(
                    ring.at[n % ring_size], out.at[slot], ring_sems.at[n % ring_size]
                )
                copy.start()
                self.copies.append(copy)

            def finish(self):
                for copy in self.copies[-ring_size:]:
                    copy.wait()

        @pl.when(diag)
        def _():
            writer = Writer()
            known = set()

            def column_at(j):
                if j not in known:
                    known.add(j)
                    gather_column(j, *p.place_of(j))

            for rows in row_sets:
                columns = [j for j in range(rows[-1] + 1) if mine(rows[0], j)]
                if not columns:
                    continue
                left = scale(rows)
                for j in columns:
                    column_at(j)
                    live = [row for row in rows if j <= row]
                    product = times(left[(len(rows) - len(live)) * p.strip :], j)
                    for r, row in enumerate(live):
                        slot = row * (row + 1) // 2 + j
                        writer.put(slot, product[r * p.strip : (r + 1) * p.strip])
            writer.finish()

        @pl.when(jnp.logical_not(diag))
        def _():
            empty = p.slots - rows_in_box if early else 0
            if empty:
                at = pl.ds(rows_in_box, empty)
                rest = pltpu.make_async_copy(tiles.at[at], out.at[at], rest_sem)
                rest.start()
            writer = Writer()
            known = set()
            for rows in row_sets:
                columns = [j for j in range(p.half_group) if mine(rows[0], j)]
                if not columns:
                    continue
                left = scale(rows)
                for j in columns:
                    if j not in known:
                        known.add(j)
                        gather_column(j, *p.column_of(j))
                    product = times(left, j)
                    for r, row in enumerate(rows):
                        slot = row * p.half_group + j
                        writer.put(slot, product[r * p.strip : (r + 1) * p.strip])
            writer.finish()
            if empty:
                rest.wait()

    hbm = pl.BlockSpec(memory_space=pltpu.HBM)
    delivered = [in_vmem(ref) for chunk in arrived for ref in chunk]
    specs = [IN_VMEM] * (2 + len(delivered))
    return pl.pallas_call(
        kernel,
        out_shape=jax.ShapeDtypeStruct(held.shape, jnp.float32),
        grid_spec=pltpu.PrefetchScalarGridSpec(
            num_scalar_prefetch=1,
            grid=(),
            in_specs=specs if early else specs + [hbm],
            out_specs=hbm,
            scratch_shapes=[
                pltpu.VMEM((p.per_group, p.order, p.order), jnp.bfloat16),
                pltpu.VMEM((ring_size, p.strip, p.order), jnp.float32),
                pltpu.SemaphoreType.DMA((ring_size,)),
                pltpu.SemaphoreType.DMA,
            ],
        ),
        input_output_aliases={} if early else {3 + len(delivered): 0},
        compiler_params=limit(20),
        name="begin" if early else "finish",
    )(
        table,
        in_vmem(held),
        in_vmem(inverse),
        *delivered,
        *([] if early else [before]),
    )


def planned(p, stored_tiles, cell_owner):
    current = stored_tiles[0]
    halves = [list(range(h * p.half_tri, (h + 1) * p.half_tri)) for h in range(2)]
    swap = [(i, (i + p.half_tri) % p.tri) for i in range(p.tri)]

    def send(pieces):
        arrived = {0: pieces[0]}
        for n in reversed(range(1, p.half_tri)):
            pairs = [(i, i ^ n) for i in range(p.tri)]
            arrived[n] = lax.ppermute(pieces[n], "tri", pairs)
        return [arrived[n] for n in range(p.half_tri)]

    def arrivals(x):
        return [x] + [
            lax.ppermute(x, "sub", [((i + shift) % p.subs, i) for i in range(p.subs)])
            for shift in range(1, p.subs)
        ]

    table = table_call(p, cell_owner)
    near, far, arrived = [], [], []
    for number, members in enumerate(p.spreads):
        tiles = [tile for unit in members for tile in p.tiles_of(unit)]
        pieces = extract_call(p, cell_owner, current, tiles, number > 0)
        if number == 0:
            spread = [
                lax.all_to_all(
                    pieces[0],
                    "tri",
                    split_axis=0,
                    concat_axis=0,
                    tiled=True,
                    axis_index_groups=halves,
                )
            ]
        else:
            spread = send(pieces)
        near.extend(pick_call(p, table, spread, members))
    for x in near:
        far.append(lax.ppermute(x, "tri", swap))
    for chunk, units in enumerate(p.deliveries):
        built = build_call(p, table, [near[u] for u in units], [far[u] for u in units], chunk == 0)
        pieces = send(built)
        packed = pack_call(p, table, pieces)
        arrived.append(arrivals(packed))
    inverse, held = inverse_call(p, table, arrived[0], current)
    begun = update_call(p, table, held, arrived[:-1], inverse, None)
    return update_call(p, table, held, arrived, inverse, begun)[None]


def shards(stored_tiles, cell_owner):
    p = Plan(
        lax.axis_size("tri"),
        lax.axis_size("sub"),
        stored_tiles.shape[1],
        stored_tiles.shape[2],
        stored_tiles.shape[3],
    )
    if p.tiled():
        return planned(p, stored_tiles, cell_owner)
    return untiled(stored_tiles, cell_owner)


def solution(mesh):
    placed = (P("tri", None, "sub", None), P())
    return jax.shard_map(
        shards, mesh=mesh, in_specs=placed, out_specs=P("tri", None, "sub", None), check_vma=False
    )
```
